32 devices in a mesh: mem: 8 (over z, x), rep: 4 (over y, core).
Axes of the slice: x: 2, y: 2, z: 4, core: 2. Of those that a mesh axis runs over, the one named last changes fastest.
Arguments:
- memory: float32 [8192, 172], P('mem'), may hold values from -6 to 6
- node_slot: int32 [8192], replicated, may hold values from 0 to 8191, as said below
- event_nodes: int32 [2, 4096, 33], P(None, ('mem', 'rep')), may hold values from 0 to 8191, as said below
- event_times: int32 [2, 4096], P(None, ('mem', 'rep')), may hold values from 0 to 999
- valid_mask: int32 [2, 4096], P(None, ('mem', 'rep')), may hold values 0 or 1
- time_freq: float32 [100], replicated, may hold values from 0.001 to 1
- time_phase: float32 [100], replicated, may hold values from -3.140625 to 3.140625
- gru_input: bfloat16 [444, 516], replicated, may hold values from -0.25 to 0.25
- gru_hidden: bfloat16 [172, 516], replicated, may hold values from -0.4375 to 0.4375
- gru_in_bias: float32 [516], replicated, may hold values from -3 to 3
- gru_hid_bias: float32 [516], replicated, may hold values from -3 to 3
- w_self: float32 [172, 100], replicated, may hold values from -0.4375 to 0.4375
- w_nbr: float32 [172, 100], replicated, may hold values from -0.4375 to 0.4375
- b_embed: float32 [100], replicated, may hold values from -3 to 3
- w_dec1: float32 [200, 100], replicated, may hold values from -0.4375 to 0.4375
- b_dec1: float32 [100], replicated, may hold values from -3 to 3
- w_dec2: float32 [100], replicated, may hold values from -0.625 to 0.625
- b_dec2: float32 [1], replicated, may hold values from -3 to 3
Outputs:
- memory_out: float32 [8192, 172], P('mem')
- batch_losses: float32 [2], replicated
- w_self_out: float32 [172, 100], replicated
- w_nbr_out: float32 [172, 100], replicated
- b_embed_out: float32 [100], replicated
- w_dec1_out: float32 [200, 100], replicated
- b_dec1_out: float32 [100], replicated
- w_dec2_out: float32 [100], replicated
- b_dec2_out: float32 [1], replicated
The draws below stay inside these ranges and needn't reach their ends.
Inputs may be any that keep to these rules, and one draw needn't show every extreme that they name: A permutation: node n's memory is row node_slot[n] of memory. `event_nodes`: columns 0, 1, 2 of an event are its source, destination and negative node; column 3 + r * 10 + k is neighbour k of column r. Among one device's events of one batch, the nodes of columns 0 and 1 whose slots lie in one block of 1024 slots are at most 64, and those of the other columns at most 620; in every such group of events one block of slots receives exactly 64 and 620.
All inputs are finite; a program needn't handle non-finite values. No bound on the sum of `valid_mask` on one device may be relied on, other than what follows from the above.
Results may differ from the reference program's by a relative error of at most 0.002.
Values may be sent and summed in bfloat16 or wider, within the bound.
A program may use at most 128 MiB of HBM per device.

```python
import math
import jax
import jax.numpy as jnp
from jax import lax

DM = 172
DE = 100
DT = 100
K = 10
BATCHES = 2
NODE_DEV = 1024
EV_DEV = 128
MSGW = 444
NODES = 8192
EVENTS = 4096
CAP2 = 64
CAP_R = 620


def slot_table(key):
    return jax.random.permutation(jax.random.fold_in(key, 11), NODES).astype(jnp.int32)


def owner_pick(key, how_many, bound, owners, favored):
    total = owners * bound
    owner_pool = jnp.arange(total, dtype=jnp.int32) % owners
    scores = jax.random.permutation(key, total).astype(jnp.int32)
    scores = jnp.where(owner_pool == favored, scores - total, scores)
    ranking = jnp.argsort(scores, stable=True)
    chosen = owner_pool[ranking[:how_many]]
    return jax.random.permutation(jax.random.fold_in(key, 3), chosen)


def event_block(key, inverse):
    owners = NODES // NODE_DEV
    favored = jax.random.randint(jax.random.fold_in(key, 1), (), 0, owners).astype(jnp.int32)
    paired = owner_pick(jax.random.fold_in(key, 2), 2 * EV_DEV, CAP2, owners, favored)
    others = owner_pick(jax.random.fold_in(key, 4), (3 * K + 1) * EV_DEV, CAP_R, owners, favored)
    holder = jnp.concatenate([paired.reshape(EV_DEV, 2), others.reshape(EV_DEV, 3 * K + 1)], 1)
    offsets = jax.random.randint(jax.random.fold_in(key, 5), (EV_DEV, 3 * K + 3), 0, NODE_DEV).astype(jnp.int32)
    return inverse[holder * NODE_DEV + offsets]


def draw_node_slot(key, part):
    return slot_table(key)


def draw_event_nodes(key, part):
    inverse = jnp.argsort(slot_table(key)).astype(jnp.int32)
    blocks = BATCHES * (EVENTS // EV_DEV)
    keys = jax.random.split(jax.random.fold_in(key, 12), blocks)
    result = jax.vmap(lambda block_key: event_block(block_key, inverse))(keys)
    return result.reshape(BATCHES, EVENTS, 3 * K + 3).astype(jnp.int32)


def place_ends(drawn, stream_key, smallest, top_value):
    index_at = [jax.random.randint(jax.random.fold_in(stream_key, axis), (), 0, length) for axis, length in enumerate(drawn.shape)]
    main_axis = drawn.shape.index(max(drawn.shape))
    next_to = index_at[:main_axis] + [(index_at[main_axis] + 1) % drawn.shape[main_axis]] + index_at[main_axis + 1:]
    return drawn.at[tuple(index_at)].set(smallest).at[tuple(next_to)].set(top_value)


def block_levels(own_key, extent, cuts, least, top_value):
    level = 1.0
    for axis_at, blocks in cuts:
        heights = jax.random.uniform(jax.random.fold_in(jax.random.fold_in(own_key, 6), axis_at), (blocks,), jnp.float32, least / len(cuts), top_value / len(cuts))
        level = level * jnp.repeat(jnp.exp(heights), extent[axis_at] // blocks).reshape((-1,) + (1,) * (len(extent) - 1 - axis_at))
    return level


def noise(stream_key, dims, width, limit, shards=(), held_as=jnp.bfloat16):
    level = block_levels(stream_key, dims, shards, -0.22, 0.18) if shards else 1.0
    values = jax.random.normal(stream_key, dims, jnp.float32) * width * level
    return jnp.minimum(jnp.maximum(values, -limit), limit).astype(held_as)


def setup_inputs(seed: int = 0) -> dict:
    seeds = jax.random.split(jax.random.key(seed), 19)
    return {
        "memory": noise(seeds[0], (NODES, DM), 1.0, 6.0, ((0, 8),), jnp.float32),
        "node_slot": draw_node_slot(jax.random.fold_in(seeds[18], 71), 0),
        "event_nodes": draw_event_nodes(jax.random.fold_in(seeds[18], 71), 0),
        "event_times": place_ends(jax.random.randint(seeds[3], (BATCHES, EVENTS), 0, 1000), jax.random.fold_in(seeds[3], 1), 0, 999).astype(jnp.int32),
        "valid_mask": place_ends((jax.random.randint(seeds[4], (BATCHES, EVENTS), 0, 4) < 3).astype(jnp.int32), jax.random.fold_in(seeds[4], 1), 0, 1),
        "time_freq": jnp.clip(jnp.exp(jax.random.uniform(seeds[5], (DT,), jnp.float32, math.log(0.001), math.log(1.0))), 0.001, 1.0),
        "time_phase": jnp.clip(jax.random.uniform(seeds[6], (DT,), jnp.float32, -3.140625, 3.140625), -3.140625, 3.140625),
        "gru_input": noise(seeds[7], (MSGW, 3 * DM), MSGW ** -0.5, 0.25),
        "gru_hidden": noise(seeds[8], (DM, 3 * DM), DM ** -0.5, 0.4375),
        "gru_in_bias": noise(seeds[9], (3 * DM,), 0.5, 3.0, (), jnp.float32),
        "gru_hid_bias": noise(seeds[10], (3 * DM,), 0.5, 3.0, (), jnp.float32),
        "w_self": noise(seeds[11], (DM, DE), DM ** -0.5, 0.4375, (), jnp.float32),
        "w_nbr": noise(seeds[12], (DM, DE), DM ** -0.5, 0.4375, (), jnp.float32),
        "b_embed": noise(seeds[13], (DE,), 0.5, 3.0, (), jnp.float32),
        "w_dec1": noise(seeds[14], (2 * DE, DE), (2 * DE) ** -0.5, 0.4375, (), jnp.float32),
        "b_dec1": noise(seeds[15], (DE,), 0.5, 3.0, (), jnp.float32),
        "w_dec2": noise(seeds[16], (DE,), DE ** -0.5, 0.625, (), jnp.float32),
        "b_dec2": noise(seeds[17], (1,), 0.5, 3.0, (), jnp.float32),
    }


step_size = 4.0

def block_loss(current, fetched, valid_part):
    w_self, w_nbr, b_embed, w_dec1, b_dec1, w_dec2, b_dec2 = current
    num_events = fetched.shape[0]
    row_width = fetched.shape[2]
    neighbours = (fetched.shape[1] - 3) // 3
    embed_width = w_self.shape[1]
    own_rows = fetched[:, :3].reshape(num_events * 3, row_width)
    beside_all = fetched[:, 3:].reshape(num_events * 3 * neighbours, row_width)
    direct = jnp.dot(own_rows, w_self.astype(jnp.bfloat16), preferred_element_type=jnp.float32).reshape(num_events, 3, embed_width)
    spread = jnp.dot(beside_all, w_nbr.astype(jnp.bfloat16), preferred_element_type=jnp.float32).reshape(num_events, 3, neighbours, embed_width)
    hidden = jnp.tanh(direct + lax.optimization_barrier(jnp.mean(spread, 2)) + b_embed).astype(jnp.bfloat16)
    paired = jnp.concatenate([jnp.concatenate([hidden[:, 0], hidden[:, 1]], 1), jnp.concatenate([hidden[:, 0], hidden[:, 2]], 1)], 0)
    inner_act = jax.nn.relu(jnp.dot(paired, w_dec1.astype(jnp.bfloat16), preferred_element_type=jnp.float32) + b_dec1)
    logits = lax.optimization_barrier(jnp.sum(inner_act * w_dec2, 1)) + b_dec2[0]
    weights = valid_part.astype(jnp.float32)
    sign_flip = jnp.concatenate([-jnp.ones((num_events,), jnp.float32), jnp.ones((num_events,), jnp.float32)])
    return jnp.sum(jax.nn.softplus(sign_flip * logits) * jnp.concatenate([weights, weights]))

def normalized_step(params, gradients):
    total = jnp.zeros((), jnp.float32)
    for grad_part in gradients:
        total = total + jnp.sum(grad_part * grad_part)
    factor = step_size / (jnp.sqrt(total) + 1e-06)
    return tuple((value - factor * grad_part for value, grad_part in zip(params, gradients)))

def memory_update(mean_bf, state_bf, old_state, gru_input, gru_hidden, gru_in_bias, gru_hid_bias):
    row_width = old_state.shape[1]
    from_input = jnp.dot(mean_bf, gru_input, preferred_element_type=jnp.float32) + gru_in_bias
    from_state = jnp.dot(state_bf, gru_hidden, preferred_element_type=jnp.float32) + gru_hid_bias
    reset = jax.nn.sigmoid(from_input[:, :row_width] + from_state[:, :row_width])
    update = jax.nn.sigmoid(from_input[:, row_width:2 * row_width] + from_state[:, row_width:2 * row_width])
    candidate = jnp.tanh(from_input[:, 2 * row_width:] + reset * from_state[:, 2 * row_width:])
    return (1.0 - update) * candidate + update * old_state

def reference(memory, node_slot, event_nodes, event_times, valid_mask, time_freq, time_phase, gru_input, gru_hidden, gru_in_bias, gru_hid_bias, w_self, w_nbr, b_embed, w_dec1, b_dec1, w_dec2, b_dec2):
    params = (w_self, w_nbr, b_embed, w_dec1, b_dec1, w_dec2, b_dec2)
    losses = []
    blocks = EVENTS // EV_DEV
    columns = 3 * K + 3
    for batch_index in range(BATCHES):
        slot_ids = node_slot[event_nodes[batch_index]]
        memory_bf = memory.astype(jnp.bfloat16)

        def one_block(pieces):
            block_slots, block_valid = pieces
            fetched = memory_bf[block_slots]
            loss_part, pullback = jax.vjp(lambda current: block_loss(current, fetched, block_valid), params)
            return (loss_part, pullback(jnp.ones_like(loss_part))[0])
        loss_parts, grad_parts = lax.map(one_block, (slot_ids.reshape(blocks, EV_DEV, columns), valid_mask[batch_index].reshape(blocks, EV_DEV)))
        gradients = tuple((lax.optimization_barrier(jnp.sum(grad_part, 0)) for grad_part in grad_parts))
        loss_total = jnp.sum(loss_parts)
        count_total = jnp.sum(valid_mask[batch_index].astype(jnp.float32))
        losses.append(loss_total / jnp.maximum(count_total, 1.0))
        params = normalized_step(params, gradients)
        time_code = jnp.cos(event_times[batch_index].astype(jnp.float32)[:, None] * time_freq + time_phase).astype(jnp.bfloat16)
        source = memory_bf[slot_ids[:, 0]]
        target_rows = memory_bf[slot_ids[:, 1]]
        letters = jnp.stack([jnp.concatenate([source, target_rows, time_code], 1), jnp.concatenate([target_rows, source, time_code], 1)], 1).reshape(2 * EVENTS, -1)
        aims = slot_ids[:, :2].reshape(-1)
        summed = jax.ops.segment_sum(letters.astype(jnp.float32), aims, num_segments=NODES)
        counts = jax.ops.segment_sum(jnp.ones((2 * EVENTS,), jnp.float32), aims, num_segments=NODES)
        mean_bf = (summed / jnp.maximum(counts, 1.0)[:, None]).astype(jnp.bfloat16)
        fresh = memory_update(mean_bf, memory_bf, memory, gru_input, gru_hidden, gru_in_bias, gru_hid_bias)
        memory = jnp.where(counts[:, None] > 0, fresh, memory)
    return (memory, jnp.stack(losses), params[0], params[1], params[2], params[3], params[4], params[5], params[6])
```

```python
import functools

import jax
import jax.numpy as jnp
from jax import lax
from jax.experimental import pallas as pl
from jax.experimental.pallas import tpu as pltpu
from jax.sharding import PartitionSpec as P

step_size = 4.0
LANES = 128
TIMES = 1000
MESH_ID = pl.DeviceIdType.MESH
BF = jnp.bfloat16
F32 = jnp.float32
HI = lax.Precision.HIGHEST


def vmem(count):
    return [pl.BlockSpec(memory_space=pltpu.VMEM)] * count


def dot(a, b, precision=None):
    return lax.dot_general(
        a, b, (((1,), (0,)), ((), ())), precision=precision, preferred_element_type=F32
    )


def dot_tn(a, b, precision=None):
    return lax.dot_general(
        a, b, (((0,), (0,)), ((), ())), precision=precision, preferred_element_type=F32
    )


def dot_nt(a, b, precision=None):
    return lax.dot_general(
        a, b, (((1,), (1,)), ((), ())), precision=precision, preferred_element_type=F32
    )


def iota(shape, axis):
    return lax.broadcasted_iota(jnp.int32, shape, axis)


def pad_lanes(x):
    return jnp.concatenate([x, jnp.zeros((x.shape[0], LANES - x.shape[1]), x.dtype)], 1)


def pad_rows(x, rows):
    return jnp.concatenate([x, jnp.zeros((rows - x.shape[0], x.shape[1]), x.dtype)], 0)


def lists_kernel(owners, node_dev, cap, width, slot_ref, pair_ref, time_ref, freq_ref, phase_ref, lists_ref, codes_ref):
    groups = slot_ref.shape[0]
    ids = pair_ref[...]
    letters = ids.shape[1]
    per_batch = letters // 2
    grid = slot_ref[...]
    digits = jnp.concatenate([grid >> 8, grid & 255], 1).astype(F32).astype(BF)
    group_hot = jnp.where(iota((groups, letters), 0) == (ids >> 7), 1.0, 0.0).astype(BF)
    found = dot_tn(digits, group_hot)
    here = iota((LANES, letters), 0) == (ids & 127)
    slots_f = jnp.sum(jnp.where(here, found[:LANES] * 256.0 + found[LANES:], 0.0), 0, keepdims=True)
    slots = slots_f.astype(jnp.int32)
    events = per_batch // 2
    partners = jnp.concatenate(
        [
            slots[:, events : 2 * events],
            slots[:, :events],
            slots[:, 3 * events :],
            slots[:, 2 * events : 3 * events],
        ],
        1,
    )
    owner = slots // node_dev
    offset = slots - owner * node_dev
    owner_hot = jnp.where(iota((owners, letters), 0) == owner, 1.0, 0.0)
    earlier = jnp.where(
        iota((per_batch, per_batch), 0) < iota((per_batch, per_batch), 1), 1.0, 0.0
    ).astype(BF)
    hot_bf = owner_hot.astype(BF)
    before = jnp.concatenate(
        [dot(hot_bf[:, :per_batch], earlier), dot(hot_bf[:, per_batch:], earlier)], 1
    )
    rank = jnp.sum(before * owner_hot, 0, keepdims=True).astype(jnp.int32)
    batch = iota((1, letters), 1) // per_batch
    seat = owner * (2 * cap) + batch * cap + rank
    times = time_ref[...]
    values = jnp.concatenate(
        [
            offset >> 8, offset & 255, partners >> 8, partners & 255,
            times >> 8, times & 255, jnp.ones_like(times), jnp.zeros_like(times),
        ],
        0,
    ).astype(F32).astype(BF)
    for o in range(owners):
        seats = jnp.where(iota((2 * cap, letters), 0) + o * 2 * cap == seat, 1.0, 0.0).astype(BF)
        placed = dot_nt(values, seats)
        taken = placed[6:7] > 0.5
        rows = [
            jnp.where(taken, placed[0:1] * 256.0 + placed[1:2], float(node_dev)),
            placed[2:3] * 256.0 + placed[3:4],
            placed[4:5] * 256.0 + placed[5:6],
        ]
        lists_ref[o] = jnp.concatenate(rows + [jnp.zeros((5, 2 * cap), F32)], 0).astype(jnp.int32)
    stamps = iota(codes_ref.shape, 0).astype(F32)
    code = jnp.cos(stamps * freq_ref[...] + phase_ref[...])
    lane = iota(codes_ref.shape, 1)
    code = jnp.where(lane < width, code, jnp.where(lane == width, 1.0, 0.0))
    codes_ref[...] = code.astype(BF)


def peer(index, reps):
    return (index // reps, lax.rem(index, reps))


def enter(devices, reps, me):
    barrier = pltpu.get_barrier_semaphore()

    def greet(k, carry):
        pl.semaphore_signal(
            barrier, inc=1, device_id=peer(lax.rem(me + k, devices), reps), device_id_type=MESH_ID
        )
        return carry

    lax.fori_loop(1, devices, greet, 0)
    pl.semaphore_wait(barrier, devices - 1)


class Gather:
    def __init__(self, owners, own_ref, table_ref, send_sem, recv_sem, local_sem):
        self.outer = owners // 2
        mem = lax.axis_index("mem")
        rep = lax.axis_index("rep")
        self.a, self.b = mem // 2, lax.rem(mem, 2)
        self.u, self.c = rep // 2, lax.rem(rep, 2)
        self.mem, self.rep = mem, rep
        self.own, self.table = own_ref, table_ref
        self.send_sem, self.recv_sem = send_sem, recv_sem
        self.local = pltpu.make_async_copy(own_ref, table_ref.at[mem], local_sem)
        self.sent = []

    def push(self, shard, block, target, from_own=False):
        src = self.own.at[block] if from_own else self.table.at[shard, block]
        copy = pltpu.make_async_remote_copy(
            src_ref=src,
            dst_ref=self.table.at[shard, block],
            send_sem=self.send_sem.at[len(self.sent)],
            recv_sem=self.recv_sem.at[shard, block],
            device_id=target,
            device_id_type=MESH_ID,
        )
        copy.start()
        self.sent.append(copy)

    def arrived(self, shard, block):
        pltpu.make_async_copy(
            self.table.at[shard, block], self.table.at[shard, block], self.recv_sem.at[shard, block]
        ).wait()

    def begin(self):
        self.local.start()
        a, b, u, c, rep = self.a, self.b, self.u, self.c, self.rep
        mine = (3 * c + u, 3 * c + 2)
        self.mine = mine
        for block in mine:
            self.push(self.mem, block, (2 * a + 1 - b, rep), True)
            for d in range(1, self.outer):
                self.push(self.mem, block, (2 * lax.rem(a + d, self.outer) + b, rep), True)

    def steps(self):
        a, b, u, c, rep, mem = self.a, self.b, self.u, self.c, self.rep, self.mem
        beside_x = (2 * a + 1 - b, rep)
        beside_y = (mem, 2 * (1 - u) + c)
        beside_core = (mem, 2 * u + 1 - c)
        order = [(0, 1)]
        for d in range(1, self.outer):
            order.append((d, 0))
        for d in range(1, self.outer):
            order.append((d, 1))
        shards = []
        for d, other in order:
            shards.append((2 * lax.rem(a + d, self.outer) + (1 - b if other else b), other))
        for shard, other in shards:
            for k, block in enumerate(self.mine):
                self.arrived(shard, block)
                if not other:
                    self.push(shard, block, beside_x)
                if k == 0:
                    self.push(shard, block, beside_y)
                self.push(shard, block, beside_core)
                yield
        for shard, _ in shards:
            block = 3 * c + 1 - u
            self.arrived(shard, block)
            self.push(shard, block, beside_core)
            yield
        for shard, _ in shards:
            for k in range(3):
                self.arrived(shard, 3 * (1 - c) + k)
            yield

    def finish(self):
        for copy in self.sent:
            copy.wait_send()
        self.local.wait()


def gather_sends(owners):
    outer = owners // 2
    return 2 * outer + 2 * (outer - 1) + 4 * (owners - 1)


class Exchange:
    def __init__(self, devices, reps, me, source, target, send_sem, recv_sem):
        self.devices, self.reps, self.me = devices, reps, me
        self.source, self.target = source, target
        self.send_sem, self.recv_sem = send_sem, recv_sem

    def copy(self, k):
        to = lax.rem(self.me + k, self.devices)
        return pltpu.make_async_remote_copy(
            src_ref=self.source(to),
            dst_ref=self.target(self.me),
            send_sem=self.send_sem.at[k],
            recv_sem=self.recv_sem.at[k],
            device_id=peer(to, self.reps),
            device_id_type=MESH_ID,
        )

    def start(self):
        def one(k, carry):
            self.copy(k).start()
            return carry

        lax.fori_loop(1, self.devices, one, 0)

    def wait_recv(self):
        def one(k, carry):
            come = lax.rem(self.me + self.devices - k, self.devices)
            ref = self.target(come)
            pltpu.make_async_copy(ref, ref, self.recv_sem.at[k]).wait()
            return carry

        lax.fori_loop(1, self.devices, one, 0)

    def wait_send(self):
        def one(k, carry):
            self.copy(k).wait_send()
            return carry

        lax.fori_loop(1, self.devices, one, 0)


def first_kernel(owners, reps, own_ref, lists_ref, table_ref, all_lists_ref, send_sem, recv_sem, local_sem, ls, lr):
    me = lax.axis_index("mem") * reps + lax.axis_index("rep")
    devices = owners * reps
    enter(devices, reps, me)
    gather = Gather(owners, own_ref, table_ref, send_sem, recv_sem, local_sem.at[0])
    lists = Exchange(
        devices, reps, me,
        lambda to: lists_ref.at[to // reps], lambda come: all_lists_ref.at[come], ls, lr,
    )
    mine = pltpu.make_async_copy(
        lists_ref.at[lax.axis_index("mem")], all_lists_ref.at[me], local_sem.at[1]
    )
    lists.start()
    mine.start()
    gather.begin()
    for _ in gather.steps():
        pass
    lists.wait_recv()
    lists.wait_send()
    mine.wait()
    gather.finish()


def reduce_parts(devices, reps, me, grads_ref, parts_ref, sum_ref, total_ref, sems, between=None):
    scatter = Exchange(
        devices, reps, me, lambda to: grads_ref.at[to], lambda come: parts_ref.at[come],
        sems[0], sems[1],
    )
    share = Exchange(
        devices, reps, me, lambda to: sum_ref, lambda come: total_ref.at[come], sems[2], sems[3]
    )
    return scatter, share


def reduce_middle(me, grads_ref, parts_ref, sum_ref, total_ref):
    parts_ref[me] = grads_ref[me]
    total = jnp.sum(parts_ref[...].astype(F32), 0)
    sum_ref[...] = total
    total_ref[me] = total


def second_kernel(owners, reps, own_ref, grads_ref, table_ref, total_ref, send_sem, recv_sem, local_sem, parts_ref, sum_ref, s0, s1, s2, s3):
    me = lax.axis_index("mem") * reps + lax.axis_index("rep")
    devices = owners * reps
    enter(devices, reps, me)
    gather = Gather(owners, own_ref, table_ref, send_sem, recv_sem, local_sem.at[0])
    scatter, share = reduce_parts(devices, reps, me, grads_ref, parts_ref, sum_ref, total_ref, (s0, s1, s2, s3))
    scatter.start()
    gather.begin()
    for step, _ in enumerate(gather.steps()):
        if step == 2:
            scatter.wait_recv()
            reduce_middle(me, grads_ref, parts_ref, sum_ref, total_ref)
            share.start()
    share.wait_recv()
    scatter.wait_send()
    share.wait_send()
    gather.finish()


def third_kernel(owners, reps, grads_ref, total_ref, parts_ref, sum_ref, s0, s1, s2, s3):
    me = lax.axis_index("mem") * reps + lax.axis_index("rep")
    devices = owners * reps
    enter(devices, reps, me)
    scatter, share = reduce_parts(devices, reps, me, grads_ref, parts_ref, sum_ref, total_ref, (s0, s1, s2, s3))
    scatter.start()
    scatter.wait_recv()
    reduce_middle(me, grads_ref, parts_ref, sum_ref, total_ref)
    share.start()
    share.wait_recv()
    scatter.wait_send()
    share.wait_send()


def up8(n):
    return -(-n // 8) * 8


class Pack:
    def __init__(self, width, embed, devices):
        self.width, self.embed, self.devices = width, embed, devices
        self.high = up8(width - LANES)
        self.side = up8(embed)
        self.main = 16 * devices
        self.nbr = 2 * LANES
        self.top = 4 * LANES
        self.bottom = 5 * LANES
        self.vectors = 6 * LANES
        self.rows = 6 * LANES + 8
        self.at_top = 2 * LANES + 2 * self.high
        self.at_bottom = self.at_top + self.side
        self.extra = self.at_bottom + self.side - self.main
        self.spare = LANES - embed
        self.chunks = -(-embed // self.spare) if self.spare > 0 else 0

    def fits(self):
        return (
            self.spare > 0
            and 0 <= self.extra < self.side
            and self.chunks * (self.extra + 8) <= self.main
        )


def pack_params(pack, refs, out_ref):
    w_self, w_nbr, b_embed, w_dec1, b_dec1, w_dec2, b_dec2 = refs
    width, embed = pack.width, pack.embed
    out_ref[...] = jnp.zeros_like(out_ref)
    out_ref[0:width, 0:embed] = w_self[...]
    out_ref[pack.nbr : pack.nbr + width, 0:embed] = w_nbr[...]
    out_ref[pack.top : pack.top + embed, 0:embed] = w_dec1[0:embed, :]
    out_ref[pack.bottom : pack.bottom + embed, 0:embed] = w_dec1[embed : 2 * embed, :]
    v = pack.vectors
    out_ref[v : v + 1, 0:embed] = b_embed[...]
    out_ref[v + 1 : v + 2, 0:embed] = b_dec1[...]
    out_ref[v + 2 : v + 3, 0:embed] = w_dec2[...]
    out_ref[v + 3 : v + 4, 0:1] = b_dec2[...]


def pack_grads(pack, grads, small, table_ref, out_ref):
    s_lo, s_hi, n_lo, n_hi, top, bottom = grads
    high, side, extra = pack.high, pack.side, pack.extra
    table_ref[0:LANES] = s_lo
    table_ref[LANES : 2 * LANES] = n_lo
    table_ref[2 * LANES : 2 * LANES + high] = s_hi[:high]
    table_ref[2 * LANES + high : pack.at_top] = n_hi[:high]
    table_ref[pack.at_top : pack.at_bottom] = top[:side]
    table_ref[pack.at_bottom : pack.main] = bottom[: side - extra]
    coarse = small.astype(BF).astype(F32)
    pieces = [(0, bottom[side - extra : side])] if extra else []
    pieces.append((pack.chunks * extra, jnp.concatenate([coarse, small - coarse], 0)))
    for start, piece in pieces:
        size = piece.shape[0]
        lane = iota((size, LANES), 1)
        for k in range(pack.chunks):
            moved = pltpu.roll(piece, (pack.embed - k * pack.spare) % LANES, 1)
            rows = slice(start + k * size, start + (k + 1) * size)
            table_ref[rows] = jnp.where(lane >= pack.embed, moved, table_ref[rows])
    out_ref[...] = table_ref[...].reshape(out_ref.shape).astype(BF)


def update_params(pack, total_ref, old_ref, new_ref):
    high, side, extra = pack.high, pack.side, pack.extra
    table = total_ref[...].reshape(pack.main, LANES)

    def clean(x):
        return jnp.where(iota(x.shape, 1) < pack.embed, x, 0.0)

    def collect(start, size):
        out = jnp.zeros((size, LANES), F32)
        lane = iota((size, LANES), 1)
        for k in range(pack.chunks):
            part = table[start + k * size : start + (k + 1) * size]
            part = jnp.where(lane >= pack.embed, part, 0.0)
            out = out + pltpu.roll(part, (k * pack.spare - pack.embed) % LANES, 1)
        return out

    small = collect(pack.chunks * extra, 8)
    small = small[0:4] + small[4:8]
    lane4 = iota((4, LANES), 1)
    row4 = iota((4, LANES), 0)
    loss = jnp.sum(jnp.where((row4 == 3) & (lane4 == 1), small, 0.0))
    count = jnp.sum(jnp.where((row4 == 3) & (lane4 == 2), small, 0.0))
    small = jnp.where((row4 < 3) | (lane4 == 0), small, 0.0)
    parts = [
        (0, clean(table[0:LANES])),
        (LANES, clean(table[2 * LANES : 2 * LANES + high])),
        (pack.nbr, clean(table[LANES : 2 * LANES])),
        (pack.nbr + LANES, clean(table[2 * LANES + high : pack.at_top])),
        (pack.top, clean(table[pack.at_top : pack.at_bottom])),
        (pack.bottom, clean(table[pack.at_bottom : pack.main])),
    ]
    if extra:
        parts.append((pack.bottom + side - extra, collect(0, extra)))
    total = jnp.sum(small * small)
    for _, part in parts:
        total = total + jnp.sum(part * part)
    total = jnp.zeros((1, LANES), F32) + total
    factor = step_size / (jnp.sqrt(total) + 1e-06)
    new_ref[...] = old_ref[...]
    for start, part in parts:
        rows = slice(start, start + part.shape[0])
        new_ref[rows] = old_ref[rows] - factor * part
    rows = slice(pack.vectors, pack.vectors + 4)
    new_ref[rows] = old_ref[rows] - factor * small
    return loss / jnp.maximum(jnp.zeros((1, LANES), F32) + count, 1.0)


def unpack_params(pack, packed_ref, refs):
    w_self, w_nbr, b_embed, w_dec1, b_dec1, w_dec2, b_dec2 = refs
    width, embed = pack.width, pack.embed
    w_self[...] = packed_ref[0:width, 0:embed]
    w_nbr[...] = packed_ref[pack.nbr : pack.nbr + width, 0:embed]
    w_dec1[0:embed, :] = packed_ref[pack.top : pack.top + embed, 0:embed]
    w_dec1[embed : 2 * embed, :] = packed_ref[pack.bottom : pack.bottom + embed, 0:embed]
    v = pack.vectors
    b_embed[...] = packed_ref[v : v + 1, 0:embed]
    b_dec1[...] = packed_ref[v + 1 : v + 2, 0:embed]
    w_dec2[...] = packed_ref[v + 2 : v + 3, 0:embed]
    b_dec2[...] = packed_ref[v + 3 : v + 4, 0:1]


def expand(table_ref, low_ref, high_ref, shard, quarter):
    base = shard * 4 * quarter
    lane = iota((quarter, LANES), 1)
    for c in range(2):
        for u in range(2):
            at = pl.multiple_of(base + (2 * c + u) * quarter, quarter)
            low_ref[pl.ds(at, quarter), :] = table_ref[shard, 3 * c + u].astype(F32)
        both = table_ref[shard, 3 * c + 2].astype(F32)
        at = pl.multiple_of(base + 2 * c * quarter, quarter)
        high_ref[pl.ds(at, quarter), :] = jnp.where(lane < LANES // 2, both, 0.0)
        at = pl.multiple_of(base + (2 * c + 1) * quarter, quarter)
        high_ref[pl.ds(at, quarter), :] = jnp.where(
            lane < LANES // 2, pltpu.roll(both, LANES // 2, 1), 0.0
        )


def partner_rows(batch, cap, lists_smem, low_ref, high_ref, out_low, out_high):
    def one(d, carry):
        for j in range(cap):
            p = lists_smem[d, 1, batch * cap + j]
            at = d * cap + j
            out_low[pl.ds(at, 1), :] = low_ref[pl.ds(p, 1), :]
            out_high[pl.ds(at, 1), :] = high_ref[pl.ds(p, 1), :]
        return carry

    lax.fori_loop(0, lists_smem.shape[0], one, 0)


def event_rows(batch, nodes_smem, slot_smem, low_ref, high_ref, own_low, own_high, nbr_low, nbr_high):
    _, events, columns = nodes_smem.shape
    neighbours = (columns - 3) // 3

    def one(e, carry):
        def row(col):
            slot = slot_smem[nodes_smem[batch, e, col]]
            return low_ref[pl.ds(slot, 1), :], high_ref[pl.ds(slot, 1), :]

        for r in range(3):
            at = pl.ds(r * events + e, 1)
            low, high = row(r)
            own_low[at, :] = low
            own_high[at, :] = high
            low, high = row(3 + r * neighbours)
            for k in range(1, neighbours):
                more, rest = row(3 + r * neighbours + k)
                low, high = low + more, high + rest
            nbr_low[at, :] = low
            nbr_high[at, :] = high
        return carry

    lax.fori_loop(0, events, one, 0)


def pair_row(batch, cap, lists_ref, i, row):
    first, second = lists_ref[2 * i], lists_ref[2 * i + 1]
    lane = iota(first.shape, 1)
    if batch == 0:
        both = jnp.where(lane < cap, first, pltpu.roll(second, cap, 1))
    else:
        both = jnp.where(lane < cap, pltpu.roll(first, cap, 1), second)
    return both[row : row + 1]


def letter_codes(batch, cap, lists_ref, codes_ref, letters_ref):
    times = codes_ref.shape[0]
    codes = codes_ref[...]
    for i in range(lists_ref.shape[0] // 2):
        stamp = pair_row(batch, cap, lists_ref, i, 2)
        hot = jnp.where(iota((times, LANES), 0) == stamp, 1.0, 0.0).astype(BF)
        letters_ref[i * LANES : (i + 1) * LANES, 2 * LANES :] = dot_tn(hot, codes).astype(BF)


def split2(x):
    coarse = x.astype(BF)
    return coarse, (x - coarse.astype(F32)).astype(BF)


def memory_step(batch, cap, width, code, lists_ref, letters_ref, memory_ref, gi_ref, gh_ref, bias_ref, hot_ref, out_ref, blocks_ref):
    slots = memory_ref.shape[0]
    quarter = slots // 4
    pairs = lists_ref.shape[0] // 2
    lane = iota((quarter, LANES), 1)
    rest = width - LANES
    held = None
    for q in range(4):
        rows = slice(q * quarter, (q + 1) * quarter)
        for i in range(pairs):
            target = pair_row(batch, cap, lists_ref, i, 0)
            hot = jnp.where(iota((quarter, LANES), 0) + q * quarter == target, 1.0, 0.0)
            hot_ref[:, i * LANES : (i + 1) * LANES] = hot.astype(BF)
        summed = dot(hot_ref[...], letters_ref[...])
        counts = jnp.sum(
            jnp.where(lane == code, summed[:, 2 * LANES :], 0.0), 1, keepdims=True
        )
        mean = (summed / jnp.maximum(counts, 1.0)).astype(BF)
        low = memory_ref[rows, 0:LANES]
        high = pad_lanes(memory_ref[rows, LANES:width])
        old = jnp.concatenate([low, high], 1)
        state = old.astype(BF)
        joined = jnp.concatenate([state, mean], 1)
        inner = [dot(joined, gi_ref[j]) + bias_ref[j : j + 1] for j in range(3)]
        outer = [dot(state, gh_ref[j]) + bias_ref[j + 3 : j + 4] for j in range(3)]
        reset = jax.nn.sigmoid(inner[0] + outer[0])
        update = jax.nn.sigmoid(inner[1] + outer[1])
        candidate = jnp.tanh(inner[2] + reset * outer[2])
        fresh = (1.0 - update) * candidate + update * old
        new = jnp.where(counts > 0.5, fresh, old)
        new_low, new_high = new[:, :LANES], new[:, LANES:]
        out_ref[rows, 0:LANES] = new_low
        out_ref[rows, LANES:width] = new_high[:, :rest]
        if blocks_ref is not None:
            c, u = q // 2, q % 2
            blocks_ref[3 * c + u] = new_low.astype(BF)
            masked = jnp.where(lane < rest, new_high, 0.0)
            if u == 0:
                held = masked
            else:
                blocks_ref[3 * c + 2] = (held + pltpu.roll(masked, LANES // 2, 1)).astype(BF)


def loss_step(pack, batch, neighbours, params_ref, valid_ref, own_low, own_high, nbr_low, nbr_high, table_ref, out_ref):
    events = valid_ref.shape[1]
    v = pack.vectors

    def weight(start):
        return params_ref[start : start + LANES].astype(BF)

    b_embed = params_ref[v : v + 1]
    b_dec1 = params_ref[v + 1 : v + 2]
    w_dec2 = params_ref[v + 2 : v + 3]
    b_dec2 = jnp.sum(params_ref[v + 3 : v + 4])
    x_low, x_high = own_low[...].astype(BF), own_high[...].astype(BF)
    n_low, n_high = split2(nbr_low[...]), split2(nbr_high[...])
    direct = dot(x_low, weight(0)) + dot(x_high, weight(LANES))
    w_low, w_high = weight(pack.nbr), weight(pack.nbr + LANES)
    spread = (
        dot(n_low[0], w_low) + dot(n_low[1], w_low) + dot(n_high[0], w_high) + dot(n_high[1], w_high)
    )
    act = jnp.tanh(direct + spread * (1.0 / neighbours) + b_embed)
    hidden = act.astype(BF)
    h0, h1, h2 = (hidden[r * events : (r + 1) * events] for r in range(3))
    top, bottom = weight(pack.top), weight(pack.bottom)
    shared = dot(h0, top)
    pre = [shared + dot(h, bottom) + b_dec1 for h in (h1, h2)]
    eye = iota((events, events), 0) == iota((events, events), 1)
    valid = jnp.where(eye, valid_ref[batch : batch + 1].astype(F32), 0.0)
    valid = jnp.sum(valid, 1, keepdims=True)
    loss = jnp.zeros((1, 1), F32)
    d_pre, g_dec2, g_out = [], jnp.zeros((1, LANES), F32), jnp.zeros((1, 1), F32)
    for z, sign in zip(pre, (-1.0, 1.0)):
        inner = jnp.maximum(z, 0.0)
        logit = (jnp.sum(inner * w_dec2, 1, keepdims=True) + b_dec2) * sign
        soft = jnp.maximum(logit, 0.0) + jnp.log1p(jnp.exp(-jnp.abs(logit)))
        loss = loss + jnp.sum(soft * valid, 0, keepdims=True)
        d_logit = jax.nn.sigmoid(logit) * valid * sign
        g_dec2 = g_dec2 + jnp.sum(d_logit * inner, 0, keepdims=True)
        g_out = g_out + jnp.sum(d_logit, 0, keepdims=True)
        d_pre.append(jnp.where(z > 0.0, d_logit * w_dec2, 0.0))
    g_dec1 = jnp.sum(d_pre[0] + d_pre[1], 0, keepdims=True)
    both = split2(d_pre[0] + d_pre[1])
    parts = [split2(d) for d in d_pre]
    g_top = dot_tn(h0, both[0]) + dot_tn(h0, both[1])
    g_bottom = (
        dot_tn(h1, parts[0][0]) + dot_tn(h1, parts[0][1])
        + dot_tn(h2, parts[1][0]) + dot_tn(h2, parts[1][1])
    )
    back = []
    for w in (top, bottom):
        back.append([(dot_nt(p[0], w) + dot_nt(p[1], w)).astype(BF) for p in parts])
    d0 = (back[0][0].astype(F32) + back[0][1].astype(F32)).astype(BF)
    d_hidden = jnp.concatenate([d0, back[1][0], back[1][1]], 0).astype(F32)
    d_act = d_hidden * (1.0 - act * act)
    g_embed = jnp.sum(d_act, 0, keepdims=True)
    d_own = split2(d_act)
    d_nbr = split2(d_act * (1.0 / neighbours))
    g_s = [dot_tn(x, d_own[0]) + dot_tn(x, d_own[1]) for x in (x_low, x_high)]
    g_n = [
        dot_tn(n[0], d_nbr[0]) + dot_tn(n[0], d_nbr[1]) + dot_tn(n[1], d_nbr[0])
        for n in (n_low, n_high)
    ]
    count = jnp.sum(valid, 0, keepdims=True)
    lane = iota((1, LANES), 1)
    scalars = jnp.where(lane == 0, g_out, jnp.where(lane == 1, loss, jnp.where(lane == 2, count, 0.0)))
    small = jnp.concatenate([g_embed, g_dec1, g_dec2, scalars], 0)
    pack_grads(pack, (g_s[0], g_s[1], g_n[0], g_n[1], g_top, g_bottom), small, table_ref, out_ref)


def start_kernel(owners, node_dev, cap, code, pack, slot_ref, pair_ref, time_ref, freq_ref, phase_ref, memory_ref, *refs):
    params, (lists_ref, codes_ref, packed_ref, blocks_ref) = refs[:7], refs[7:]
    lists_kernel(owners, node_dev, cap, code, slot_ref, pair_ref, time_ref, freq_ref, phase_ref, lists_ref, codes_ref)
    pack_params(pack, params, packed_ref)
    width = memory_ref.shape[1]
    quarter = node_dev // 4
    for c in range(2):
        for u in range(2):
            rows = slice((2 * c + u) * quarter, (2 * c + u + 1) * quarter)
            blocks_ref[3 * c + u] = memory_ref[rows, 0:LANES].astype(BF)
        first = slice(2 * c * quarter, (2 * c + 1) * quarter)
        second = slice((2 * c + 1) * quarter, (2 * c + 2) * quarter)
        blocks_ref[3 * c + 2] = (
            pad_lanes(memory_ref[first, LANES:width])
            + pltpu.roll(pad_lanes(memory_ref[second, LANES:width]), LANES // 2, 1)
        ).astype(BF)


def batch_kernel(batch, last, cap, code, pack, nodes_smem, slot_smem, lists_smem, table_ref, lists_ref, codes_ref, memory_ref, valid_ref, gi_ref, gh_ref, bias_ref, params_ref, *refs):
    if last:
        (out_ref, grads_ref), rest = refs[:2], refs[2:]
        blocks_ref = None
    else:
        (out_ref, blocks_ref, grads_ref), rest = refs[:3], refs[3:]
    low, high, p_low, p_high, letters, hot, own_low, own_high, nbr_low, nbr_high, flat = rest
    owners = table_ref.shape[0]
    quarter = memory_ref.shape[0] // 4
    neighbours = (nodes_smem.shape[2] - 3) // 3

    def spread(s, carry):
        expand(table_ref, low, high, s, quarter)
        return carry

    lax.fori_loop(0, owners, spread, 0)
    partner_rows(batch, cap, lists_smem, low, high, p_low, p_high)
    letters[:, 0:LANES] = p_low[...].astype(BF)
    letters[:, LANES : 2 * LANES] = p_high[...].astype(BF)
    letter_codes(batch, cap, lists_ref, codes_ref, letters)
    memory_step(batch, cap, pack.width, code, lists_ref, letters, memory_ref, gi_ref, gh_ref, bias_ref, hot, out_ref, blocks_ref)
    event_rows(batch, nodes_smem, slot_smem, low, high, own_low, own_high, nbr_low, nbr_high)
    loss_step(pack, batch, neighbours, params_ref, valid_ref, own_low, own_high, nbr_low, nbr_high, flat, grads_ref)


def update_kernel(pack, total_ref, old_ref, new_ref, loss_ref):
    loss_ref[...] = update_params(pack, total_ref, old_ref, new_ref)


def final_kernel(pack, total_ref, old_ref, *refs):
    loss_ref, outs, new_ref = refs[0], refs[1:8], refs[8]
    loss_ref[...] = update_params(pack, total_ref, old_ref, new_ref)
    unpack_params(pack, new_ref, outs)


def quick_body(owners, reps, cap, memory, node_slot, event_nodes, event_times, valid_mask, time_freq, time_phase, gru_input, gru_hidden, gru_in_bias, gru_hid_bias, *params):
    node_dev, width = memory.shape
    batches, events, columns = event_nodes.shape
    code = time_freq.shape[0]
    embed = params[0].shape[1]
    devices = owners * reps
    pack = Pack(width, embed, devices)
    quarter = node_dev // 4
    sds = jax.ShapeDtypeStruct
    pairs = event_nodes[:, :, :2].transpose(0, 2, 1).reshape(1, -1)
    times = jnp.broadcast_to(event_times[:, None, :], (batches, 2, events)).reshape(1, -1)
    freq = jnp.pad(time_freq, (0, LANES - code))[None, :]
    phase = jnp.pad(time_phase, (0, LANES - code))[None, :]
    rows = [p[None, :] if p.ndim == 1 else p for p in params]
    stamps = -(-TIMES // LANES) * LANES
    lists, codes, packed, blocks = pl.pallas_call(
        functools.partial(start_kernel, owners, node_dev, cap, code, pack),
        out_shape=(
            sds((owners, 8, 2 * cap), jnp.int32),
            sds((stamps, LANES), BF),
            sds((pack.rows, LANES), F32),
            sds((6, quarter, LANES), BF),
        ),
        in_specs=vmem(13),
        out_specs=tuple(vmem(4)),
        name="start",
    )(node_slot.reshape(-1, LANES), pairs, times, freq, phase, memory, *rows)

    pad_w = 2 * LANES - width
    gi = gru_input.reshape(-1, 3, width).transpose(1, 0, 2)
    gi = jnp.concatenate(
        [
            jnp.pad(gi[:, :width], ((0, 0), (0, pad_w), (0, pad_w))),
            jnp.pad(gi[:, width : 2 * width], ((0, 0), (0, pad_w), (0, pad_w))),
            jnp.pad(gi[:, 2 * width :], ((0, 0), (0, LANES - code), (0, pad_w))),
        ],
        1,
    )
    gh = jnp.pad(gru_hidden.reshape(width, 3, width).transpose(1, 0, 2), ((0, 0), (0, pad_w), (0, pad_w)))
    bias = jnp.pad(
        jnp.concatenate([gru_in_bias.reshape(3, width), gru_hid_bias.reshape(3, width)], 0),
        ((0, 2), (0, pad_w)),
    )

    dma = pltpu.SemaphoreType.DMA
    sends = gather_sends(owners)
    gather_sems = [dma((sends,)), dma((owners, 6)), dma((2,))]
    reduce_scratch = [
        pltpu.VMEM((devices, 16, LANES), BF),
        pltpu.VMEM((16, LANES), F32),
        dma((devices,)),
        dma((devices,)),
        dma((devices,)),
        dma((devices,)),
    ]
    table_shape = sds((owners, 6, quarter, LANES), BF)
    total_shape = sds((devices, 16, LANES), F32)
    table, all_lists = pl.pallas_call(
        functools.partial(first_kernel, owners, reps),
        out_shape=(table_shape, sds((devices, 8, 2 * cap), jnp.int32)),
        in_specs=vmem(2),
        out_specs=tuple(vmem(2)),
        scratch_shapes=gather_sems + [dma((devices,)), dma((devices,))],
        compiler_params=pltpu.CompilerParams(collective_id=0, has_side_effects=True),
        name="first",
    )(blocks, lists)

    losses = []
    for batch in range(batches):
        last = batch == batches - 1
        outs = [sds((node_dev, width), F32)]
        if not last:
            outs.append(sds((6, quarter, LANES), BF))
        outs.append(sds((devices, 16, LANES), BF))
        letters = devices * cap
        slots = node_slot.shape[0]
        made = pl.pallas_call(
            functools.partial(batch_kernel, batch, last, cap, code, pack),
            out_shape=tuple(outs),
            in_specs=[pl.BlockSpec(memory_space=pltpu.SMEM)] * 3 + vmem(9),
            out_specs=tuple(vmem(len(outs))),
            scratch_shapes=[
                pltpu.VMEM((slots, LANES), F32),
                pltpu.VMEM((slots, LANES), F32),
                pltpu.VMEM((letters, LANES), F32),
                pltpu.VMEM((letters, LANES), F32),
                pltpu.VMEM((letters, 3 * LANES), BF),
                pltpu.VMEM((quarter, letters), BF),
                pltpu.VMEM((3 * events, LANES), F32),
                pltpu.VMEM((3 * events, LANES), F32),
                pltpu.VMEM((3 * events, LANES), F32),
                pltpu.VMEM((3 * events, LANES), F32),
                pltpu.VMEM((pack.main, LANES), F32),
            ],
            compiler_params=pltpu.CompilerParams(vmem_limit_bytes=48 * 1024 * 1024),
            name="batch" + str(batch),
        )(event_nodes, node_slot, all_lists, table, all_lists, codes, memory, valid_mask, gi, gh, bias, packed)
        if last:
            memory, grads = made
            total = pl.pallas_call(
                functools.partial(third_kernel, owners, reps),
                out_shape=total_shape,
                in_specs=vmem(1),
                out_specs=vmem(1)[0],
                scratch_shapes=reduce_scratch,
                compiler_params=pltpu.CompilerParams(collective_id=2, has_side_effects=True),
                name="third",
            )(grads)
            outs = pl.pallas_call(
                functools.partial(final_kernel, pack),
                out_shape=(sds((1, LANES), F32),) + tuple(sds(p.shape, F32) for p in rows),
                in_specs=vmem(2),
                out_specs=tuple(vmem(8)),
                scratch_shapes=[pltpu.VMEM((pack.rows, LANES), F32)],
                name="final",
            )(total, packed)
            losses.append(outs[0])
            params = [o.reshape(p.shape) for o, p in zip(outs[1:], params)]
        else:
            memory, blocks, grads = made
            table, total = pl.pallas_call(
                functools.partial(second_kernel, owners, reps),
                out_shape=(table_shape, total_shape),
                in_specs=vmem(2),
                out_specs=tuple(vmem(2)),
                scratch_shapes=gather_sems + reduce_scratch,
                compiler_params=pltpu.CompilerParams(collective_id=1, has_side_effects=True),
                name="second",
            )(blocks, grads)
            packed, loss = pl.pallas_call(
                functools.partial(update_kernel, pack),
                out_shape=(sds((pack.rows, LANES), F32), sds((1, LANES), F32)),
                in_specs=vmem(2),
                out_specs=tuple(vmem(2)),
                name="update",
            )(total, packed)
            losses.append(loss)
    losses = jnp.concatenate([loss[:, 0] for loss in losses])
    return (memory, losses, *params)


def block_loss(current, own_rows, beside_sum, neighbours, valid_part):
    w_self, w_nbr, b_embed, w_dec1, b_dec1, w_dec2, b_dec2 = current
    num_events = own_rows.shape[0] // 3
    direct = jnp.dot(own_rows, w_self.astype(jnp.bfloat16), preferred_element_type=jnp.float32)
    spread = jnp.dot(
        beside_sum,
        w_nbr.astype(jnp.bfloat16).astype(jnp.float32),
        precision=lax.Precision.HIGHEST,
    )
    hidden = jnp.tanh(direct + spread * (1.0 / neighbours) + b_embed).astype(jnp.bfloat16)
    first = hidden[:num_events]
    paired = jnp.concatenate(
        [jnp.concatenate([first, first], 0), hidden[num_events:]],
        1,
    )
    inner_act = jax.nn.relu(
        jnp.dot(paired, w_dec1.astype(jnp.bfloat16), preferred_element_type=jnp.float32) + b_dec1
    )
    logits = jnp.sum(inner_act * w_dec2, 1) + b_dec2[0]
    weights = valid_part.astype(jnp.float32)
    sign_flip = jnp.concatenate(
        [-jnp.ones((num_events,), jnp.float32), jnp.ones((num_events,), jnp.float32)]
    )
    return jnp.sum(jax.nn.softplus(sign_flip * logits) * jnp.concatenate([weights, weights]))


def normalized_step(params, gradients):
    total = jnp.zeros((), jnp.float32)
    for grad_part in gradients:
        total = total + jnp.sum(grad_part * grad_part)
    factor = step_size / (jnp.sqrt(total) + 1e-06)
    return tuple((value - factor * grad_part for value, grad_part in zip(params, gradients)))


def memory_update(
    mean_rest, state_bf, old_state, gru_input, gru_hidden, gru_in_bias, gru_hid_bias
):
    row_width = old_state.shape[1]
    from_input = (
        jnp.dot(state_bf, gru_input[:row_width], preferred_element_type=jnp.float32)
        + jnp.dot(mean_rest, gru_input[row_width:], preferred_element_type=jnp.float32)
        + gru_in_bias
    )
    from_state = jnp.dot(state_bf, gru_hidden, preferred_element_type=jnp.float32) + gru_hid_bias
    reset = jax.nn.sigmoid(from_input[:, :row_width] + from_state[:, :row_width])
    update = jax.nn.sigmoid(
        from_input[:, row_width : 2 * row_width] + from_state[:, row_width : 2 * row_width]
    )
    candidate = jnp.tanh(from_input[:, 2 * row_width :] + reset * from_state[:, 2 * row_width :])
    return (1.0 - update) * candidate + update * old_state


def look_up(table, ids):
    width = 128
    groups = table.shape[0] // width
    grid = table.reshape(groups, width)
    digits = jnp.concatenate([grid >> 8, grid & 255], 1).astype(jnp.bfloat16)
    pick = ((ids // width)[..., None] == jnp.arange(groups, dtype=jnp.int32)).astype(jnp.bfloat16)
    rows = jnp.dot(pick, digits, preferred_element_type=jnp.float32)
    here = (ids % width)[..., None] == jnp.arange(width, dtype=jnp.int32)
    both = jnp.where(here, rows[..., :width] * 256.0 + rows[..., width:], 0.0)
    return jnp.sum(both, -1).astype(jnp.int32)


def sum_everywhere(gradients, loss_local, count_local, devices):
    g_self, g_nbr, g_embed, g_dec1, g_bias1, g_dec2, g_bias2 = gradients
    width = g_self.shape[1]
    scalars = jnp.concatenate([g_bias2, loss_local[None], count_local[None]])
    scalars = jnp.pad(scalars, (0, width - scalars.shape[0]))
    table = jnp.concatenate(
        [g_self, g_nbr, g_dec1, jnp.stack([g_embed, g_bias1, g_dec2, scalars])], 0
    )
    used = table.shape[0]
    share = -(-used // (devices * 8)) * 8
    table = jnp.pad(table, ((0, share * devices - used), (0, 0))).reshape(devices, share, width)
    parts = lax.all_to_all(table, ("mem", "rep"), split_axis=0, concat_axis=0, tiled=True)
    total = lax.all_gather(jnp.sum(parts, 0), ("mem", "rep"), axis=0, tiled=True)
    n_self, n_nbr, n_dec1 = g_self.shape[0], g_nbr.shape[0], g_dec1.shape[0]
    at = n_self + n_nbr + n_dec1
    return (
        (
            total[:n_self],
            total[n_self : n_self + n_nbr],
            total[at],
            total[n_self + n_nbr : at],
            total[at + 1],
            total[at + 2],
            total[at + 3, :1],
        ),
        total[at + 3, 1],
        total[at + 3, 2],
    )


def place_rows(owner_ids, owners, stride, offset):
    length = owner_ids.shape[0]
    width = 128
    groups = -(-length // width)
    padded_ids = owner_ids.reshape(groups, width)
    one_hot = (padded_ids[:, :, None] == jnp.arange(owners, dtype=jnp.int32)[None, None, :]).astype(
        jnp.float32
    )
    lower = (
        jnp.arange(width, dtype=jnp.int32)[:, None] > jnp.arange(width, dtype=jnp.int32)[None, :]
    ).astype(jnp.float32)
    within = jnp.einsum("ij,gjo->gio", lower, one_hot, precision=lax.Precision.HIGHEST)
    totals = jnp.sum(one_hot, 1)
    starts = jnp.cumsum(totals, 0) - totals
    before = jnp.sum((within + starts[:, None, :]) * one_hot, 2).reshape(-1)
    return owner_ids * stride + offset + before.astype(jnp.int32)


def body(
    memory,
    node_slot,
    event_nodes,
    event_times,
    valid_mask,
    time_freq,
    time_phase,
    gru_input,
    gru_hidden,
    gru_in_bias,
    gru_hid_bias,
    w_self,
    w_nbr,
    b_embed,
    w_dec1,
    b_dec1,
    w_dec2,
    b_dec2,
):
    owners = lax.axis_size("mem")
    devices = owners * lax.axis_size("rep")
    node_dev, row_width = memory.shape
    batches, events, columns = event_nodes.shape
    neighbours = (columns - 3) // 3
    cap_pair = 2 * events // owners * 2
    params = (w_self, w_nbr, b_embed, w_dec1, b_dec1, w_dec2, b_dec2)
    losses = []
    all_slots = look_up(node_slot, event_nodes.transpose(0, 2, 1))
    for batch_index in range(batches):
        slot_ids = all_slots[batch_index]
        memory_bf = memory.astype(jnp.bfloat16)
        whole_bf = lax.all_gather(memory_bf, "mem", axis=0, tiled=True)
        fetched = jnp.take(whole_bf, slot_ids.reshape(-1), axis=0, mode="clip")
        own_rows = fetched[: 3 * events]
        beside = fetched[3 * events :].reshape(3, neighbours, events, row_width)
        beside_sum = jnp.sum(beside.astype(jnp.float32), 1).reshape(3 * events, row_width)

        pair_slots = slot_ids[:2].reshape(-1)
        pair_at = place_rows(pair_slots // node_dev, owners, cap_pair, 0)
        offsets = (pair_slots % node_dev).astype(jnp.int32)
        time_code = jnp.cos(
            event_times[batch_index].astype(jnp.float32)[:, None] * time_freq + time_phase
        ).astype(jnp.bfloat16)
        marks = jnp.stack([jnp.ones_like(offsets), offsets // 128, offsets % 128], 1)
        partners = jnp.concatenate([own_rows[events : 2 * events], own_rows[:events]], 0)
        letters = jnp.concatenate(
            [partners, jnp.concatenate([time_code, time_code], 0), marks.astype(jnp.bfloat16)], 1
        )
        seats = jnp.arange(owners * cap_pair, dtype=jnp.int32)[:, None] == pair_at[None, :]
        parcel = jnp.dot(
            seats.astype(jnp.bfloat16), letters, preferred_element_type=jnp.float32
        ).astype(jnp.bfloat16)
        parcel = parcel.reshape(owners, cap_pair, letters.shape[1])
        parcel = lax.all_to_all(parcel, "mem", split_axis=0, concat_axis=0, tiled=True)
        every_parcel = lax.all_gather(parcel, "rep", axis=0, tiled=True)
        every_parcel = every_parcel.reshape(-1, letters.shape[1])
        digits = every_parcel[:, -2:].astype(jnp.int32)
        target = digits[:, 0] * 128 + digits[:, 1]
        matches = jnp.arange(node_dev, dtype=jnp.int32)[:, None] == target[None, :]
        summed = jnp.dot(
            matches.astype(jnp.bfloat16), every_parcel, preferred_element_type=jnp.float32
        )
        counts = summed[:, -3:-2]
        mean_rest = (summed[:, :-3] / jnp.maximum(counts, 1.0)).astype(jnp.bfloat16)
        fresh = memory_update(
            mean_rest, memory_bf, memory, gru_input, gru_hidden, gru_in_bias, gru_hid_bias
        )
        memory = jnp.where(counts > 0, fresh, memory)

        valid_part = valid_mask[batch_index]
        loss_local, pullback = jax.vjp(
            lambda current: block_loss(current, own_rows, beside_sum, neighbours, valid_part),
            params,
        )
        gradients = pullback(jnp.ones_like(loss_local))[0]
        count_local = jnp.sum(valid_part.astype(jnp.float32))
        gradients, loss_total, count_total = sum_everywhere(
            gradients, loss_local, count_local, devices
        )
        params = normalized_step(params, gradients)
        losses.append(loss_total / jnp.maximum(count_total, 1.0))
    return (
        memory,
        jnp.stack(losses),
        params[0],
        params[1],
        params[2],
        params[3],
        params[4],
        params[5],
        params[6],
    )


def solution(mesh):
    owners, reps = mesh.shape["mem"], mesh.shape["rep"]
    in_specs = (
        P("mem", None),
        P(),
        P(None, ("mem", "rep"), None),
        P(None, ("mem", "rep")),
        P(None, ("mem", "rep")),
    ) + (P(),) * 13
    out_specs = (P("mem", None),) + (P(),) * 8

    def choose(*args):
        memory, node_slot, event_nodes = args[:3]
        node_dev, width = memory.shape
        batches, events, _ = event_nodes.shape
        cap = 2 * events // owners * 2
        pack = Pack(width, args[11].shape[1], owners * reps)
        small = node_slot.shape[0] * 2 * LANES * 4 <= 16 * 1024 * 1024
        shaped = (
            reps == 4
            and owners % 2 == 0
            and batches == 2
            and 2 * cap == LANES
            and events == LANES
            and node_dev % (4 * LANES) == 0
            and LANES < width <= LANES + LANES // 2
            and args[5].shape[0] < LANES
            and pack.fits()
        )
        if small and shaped:
            return quick_body(owners, reps, cap, *args)
        return body(*args)

    return jax.shard_map(choose, mesh=mesh, in_specs=in_specs, out_specs=out_specs, check_vma=False)
```

```python
import functools

import jax
import jax.numpy as jnp
from jax import lax
from jax.experimental import pallas as pl
from jax.experimental.pallas import tpu as pltpu
from jax.sharding import PartitionSpec as P

step_size = 4.0
LANES = 128
TIMES = 1000
MESH_ID = pl.DeviceIdType.MESH
BF = jnp.bfloat16
F32 = jnp.float32
HI = lax.Precision.HIGHEST


def vmem(count):
    return [pl.BlockSpec(memory_space=pltpu.VMEM)] * count


def dot(a, b, precision=None):
    return lax.dot_general(
        a, b, (((1,), (0,)), ((), ())), precision=precision, preferred_element_type=F32
    )


def dot_tn(a, b, precision=None):
    return lax.dot_general(
        a, b, (((0,), (0,)), ((), ())), precision=precision, preferred_element_type=F32
    )


def dot_nt(a, b, precision=None):
    return lax.dot_general(
        a, b, (((1,), (1,)), ((), ())), precision=precision, preferred_element_type=F32
    )


def iota(shape, axis):
    return lax.broadcasted_iota(jnp.int32, shape, axis)


def pad_lanes(x):
    return jnp.concatenate([x, jnp.zeros((x.shape[0], LANES - x.shape[1]), x.dtype)], 1)


def pad_rows(x, rows):
    return jnp.concatenate([x, jnp.zeros((rows - x.shape[0], x.shape[1]), x.dtype)], 0)


def lists_kernel(owners, node_dev, cap, width, slot_ref, pair_ref, time_ref, freq_ref, phase_ref, lists_ref, codes_ref):
    groups = slot_ref.shape[0]
    ids = pair_ref[...]
    letters = ids.shape[1]
    per_batch = letters // 2
    grid = slot_ref[...]
    digits = jnp.concatenate([grid >> 8, grid & 255], 1).astype(F32).astype(BF)
    group_hot = jnp.where(iota((groups, letters), 0) == (ids >> 7), 1.0, 0.0).astype(BF)
    found = dot_tn(digits, group_hot)
    here = iota((LANES, letters), 0) == (ids & 127)
    slots_f = jnp.sum(jnp.where(here, found[:LANES] * 256.0 + found[LANES:], 0.0), 0, keepdims=True)
    slots = slots_f.astype(jnp.int32)
    events = per_batch // 2
    partners = jnp.concatenate(
        [
            slots[:, events : 2 * events],
            slots[:, :events],
            slots[:, 3 * events :],
            slots[:, 2 * events : 3 * events],
        ],
        1,
    )
    owner = slots // node_dev
    offset = slots - owner * node_dev
    owner_hot = jnp.where(iota((owners, letters), 0) == owner, 1.0, 0.0)
    earlier = jnp.where(
        iota((per_batch, per_batch), 0) < iota((per_batch, per_batch), 1), 1.0, 0.0
    ).astype(BF)
    hot_bf = owner_hot.astype(BF)
    before = jnp.concatenate(
        [dot(hot_bf[:, :per_batch], earlier), dot(hot_bf[:, per_batch:], earlier)], 1
    )
    rank = jnp.sum(before * owner_hot, 0, keepdims=True).astype(jnp.int32)
    batch = iota((1, letters), 1) // per_batch
    seat = owner * (2 * cap) + batch * cap + rank
    times = time_ref[...]
    values = jnp.concatenate(
        [
            offset >> 8, offset & 255, partners >> 8, partners & 255,
            times >> 8, times & 255, jnp.ones_like(times), jnp.zeros_like(times),
        ],
        0,
    ).astype(F32).astype(BF)
    for o in range(owners):
        seats = jnp.where(iota((2 * cap, letters), 0) + o * 2 * cap == seat, 1.0, 0.0).astype(BF)
        placed = dot_nt(values, seats)
        taken = placed[6:7] > 0.5
        rows = [
            jnp.where(taken, placed[0:1] * 256.0 + placed[1:2], float(node_dev)),
            placed[2:3] * 256.0 + placed[3:4],
            placed[4:5] * 256.0 + placed[5:6],
        ]
        lists_ref[o] = jnp.concatenate(rows + [jnp.zeros((5, 2 * cap), F32)], 0).astype(jnp.int32)
    stamps = iota(codes_ref.shape, 0).astype(F32)
    code = jnp.cos(stamps * freq_ref[...] + phase_ref[...])
    lane = iota(codes_ref.shape, 1)
    code = jnp.where(lane < width, code, jnp.where(lane == width, 1.0, 0.0))
    codes_ref[...] = code.astype(BF)


def peer(index, reps):
    return (index // reps, lax.rem(index, reps))


def enter(devices, reps, me):
    barrier = pltpu.get_barrier_semaphore()

    def greet(k, carry):
        pl.semaphore_signal(
            barrier, inc=1, device_id=peer(lax.rem(me + k, devices), reps), device_id_type=MESH_ID
        )
        return carry

    lax.fori_loop(1, devices, greet, 0)
    pl.semaphore_wait(barrier, devices - 1)


BLOCKS = 6


class Gather:
    def __init__(self, owners, own_ref, table_ref, send_sem, recv_sem, local_sem):
        self.outer = owners // 2
        mem = lax.axis_index("mem")
        rep = lax.axis_index("rep")
        self.a, self.b = mem // 2, lax.rem(mem, 2)
        self.u, self.c = rep // 2, lax.rem(rep, 2)
        self.mem, self.rep = mem, rep
        self.own, self.table = own_ref, table_ref
        self.send_sem, self.recv_sem = send_sem, recv_sem
        self.local = pltpu.make_async_copy(own_ref, table_ref.at[mem], local_sem)
        self.sent = 0
        base = BLOCKS * self.c
        self.line_first = [base + 2 * self.u, base + 2 * self.u + 1, base + 4]
        self.pair_first = base + 5
        self.planes = [base + 2 * (1 - self.u), base + 2 * (1 - self.u) + 1]
        self.ahead = (jnp.minimum(mem + 2, owners - 1), rep)
        self.behind = (jnp.maximum(mem - 2, 0), rep)
        self.beside = (2 * self.a + 1 - self.b, rep)
        self.plane = (mem, 2 * (1 - self.u) + self.c)
        self.core = (mem, 2 * self.u + 1 - self.c)
        self.checks = []

    def push(self, shard, block, target, from_own=False, when=None):
        index = self.sent
        self.sent += 1
        src = self.own.at[block] if from_own else self.table.at[shard, block]

        def go():
            pltpu.make_async_remote_copy(
                src_ref=src,
                dst_ref=self.table.at[shard, block],
                send_sem=self.send_sem.at[index],
                recv_sem=self.recv_sem.at[shard, block],
                device_id=target,
                device_id_type=MESH_ID,
            ).start()

        self.guard(when, go)
        self.checks.append((index, when))

    def guard(self, when, go):
        if when is None:
            go()
        else:
            pl.when(when)(go)

    def arrived(self, shard, block):
        ref = self.table.at[shard, block]
        pltpu.make_async_copy(ref, ref, self.recv_sem.at[shard, block]).wait()

    def along(self, shard, block, from_own=False):
        self.push(shard, block, self.ahead, from_own, self.a < self.outer - 1)
        self.push(shard, block, self.behind, from_own, self.a > 0)

    def begin(self):
        self.local.start()
        self.push(self.mem, self.pair_first, self.beside, True)
        for block in self.line_first:
            self.along(self.mem, block, True)
            self.push(self.mem, block, self.beside, True)
        self.along(self.mem, self.pair_first, True)

    def shard(self, t, other):
        at = jnp.clip(self.a + t, 0, self.outer - 1)
        return 2 * at + (1 - self.b if other else self.b)

    def take(self, t, other, k):
        shard = self.shard(t, other)
        block = self.line_first[k] if k < 3 else self.pair_first
        onward = (t != 0) and not (other and k < 3)

        there = None
        if t < 0:
            there = self.a >= -t
        if t > 0:
            there = self.a < self.outer - t

        def also(extra):
            return extra if there is None else there & extra

        self.guard(there, lambda: self.arrived(shard, block))
        if t == 0 and k == 3:
            self.along(shard, block)
        if onward and t < 0:
            self.push(shard, block, self.ahead, when=also(self.a < self.outer - 1))
        if onward and t > 0:
            self.push(shard, block, self.behind, when=also(self.a > 0))
        if not other and k < 3:
            self.push(shard, block, self.beside, when=there)
        if k < 2:
            self.push(shard, block, self.plane, when=there)
        self.push(shard, block, self.core, when=there)

    def from_plane(self, t, other, k):
        shard, block = self.shard(t, other), self.planes[k]
        there = None
        if t < 0:
            there = self.a >= -t
        if t > 0:
            there = self.a < self.outer - t
        self.guard(there, lambda: self.arrived(shard, block))
        self.push(shard, block, self.core, when=there)

    def from_core(self, t, other):
        shard = self.shard(t, other)
        there = None
        if t < 0:
            there = self.a >= -t
        if t > 0:
            there = self.a < self.outer - t

        def go():
            for k in range(BLOCKS):
                self.arrived(shard, BLOCKS * (1 - self.c) + k)

        self.guard(there, go)

    def steps(self):
        far = self.outer - 1
        self.take(0, True, 3)
        for k in range(3):
            for t in (-1, 1):
                self.take(t, False, k)
            self.take(0, True, k)
            yield
        for t in range(1, far + 1):
            for k in range(3):
                for s in (-t, t):
                    self.take(s, True, k)
                    if t < far:
                        self.take(s + (1 if s > 0 else -1), False, k)
                yield
            for s in (-t, t):
                self.take(s, False, 3)
                self.take(s, True, 3)
            if t == 1:
                self.from_plane(0, True, 0)
                self.from_plane(0, True, 1)
            yield
            for s in (-t, t):
                for k in range(2):
                    self.from_plane(s, False, k)
                    self.from_plane(s, True, k)
            yield
        self.from_core(0, True)
        for t in range(1, far + 1):
            for s in (-t, t):
                self.from_core(s, False)
                self.from_core(s, True)

    def finish(self):
        for index, when in self.checks:
            ref = self.own.at[0]
            copy = pltpu.make_async_copy(ref, ref, self.send_sem.at[index])
            self.guard(when, copy.wait)
        self.local.wait()


def gather_sends(owners):
    outer = owners // 2
    return 12 + 16 * outer + 4 * BLOCKS * owners


class Exchange:
    def __init__(self, devices, reps, me, source, target, send_sem, recv_sem):
        self.devices, self.reps, self.me = devices, reps, me
        self.source, self.target = source, target
        self.send_sem, self.recv_sem = send_sem, recv_sem

    def copy(self, k):
        to = lax.rem(self.me + k, self.devices)
        return pltpu.make_async_remote_copy(
            src_ref=self.source(to),
            dst_ref=self.target(self.me),
            send_sem=self.send_sem.at[k],
            recv_sem=self.recv_sem.at[k],
            device_id=peer(to, self.reps),
            device_id_type=MESH_ID,
        )

    def start(self):
        def one(k, carry):
            self.copy(k).start()
            return carry

        lax.fori_loop(1, self.devices, one, 0)

    def wait_recv(self):
        def one(k, carry):
            come = lax.rem(self.me + self.devices - k, self.devices)
            ref = self.target(come)
            pltpu.make_async_copy(ref, ref, self.recv_sem.at[k]).wait()
            return carry

        lax.fori_loop(1, self.devices, one, 0)

    def wait_send(self):
        def one(k, carry):
            self.copy(k).wait_send()
            return carry

        lax.fori_loop(1, self.devices, one, 0)


def first_kernel(owners, reps, own_ref, lists_ref, table_ref, all_lists_ref, send_sem, recv_sem, local_sem, ls, lr):
    me = lax.axis_index("mem") * reps + lax.axis_index("rep")
    devices = owners * reps
    enter(devices, reps, me)
    gather = Gather(owners, own_ref, table_ref, send_sem, recv_sem, local_sem.at[0])
    lists = Exchange(
        devices, reps, me,
        lambda to: lists_ref.at[to // reps], lambda come: all_lists_ref.at[come], ls, lr,
    )
    mine = pltpu.make_async_copy(
        lists_ref.at[lax.axis_index("mem")], all_lists_ref.at[me], local_sem.at[1]
    )
    lists.start()
    mine.start()
    gather.begin()
    for _ in gather.steps():
        pass
    lists.wait_recv()
    lists.wait_send()
    mine.wait()
    gather.finish()


def reduce_parts(devices, reps, me, grads_ref, parts_ref, sum_ref, total_ref, sems, between=None):
    scatter = Exchange(
        devices, reps, me, lambda to: grads_ref.at[to], lambda come: parts_ref.at[come],
        sems[0], sems[1],
    )
    share = Exchange(
        devices, reps, me, lambda to: sum_ref, lambda come: total_ref.at[come], sems[2], sems[3]
    )
    return scatter, share


def reduce_middle(me, grads_ref, parts_ref, sum_ref, total_ref):
    parts_ref[me] = grads_ref[me]
    total = jnp.sum(parts_ref[...].astype(F32), 0)
    sum_ref[...] = total
    total_ref[me] = total


def second_kernel(owners, reps, own_ref, grads_ref, table_ref, total_ref, send_sem, recv_sem, local_sem, parts_ref, sum_ref, s0, s1, s2, s3):
    me = lax.axis_index("mem") * reps + lax.axis_index("rep")
    devices = owners * reps
    enter(devices, reps, me)
    gather = Gather(owners, own_ref, table_ref, send_sem, recv_sem, local_sem.at[0])
    scatter, share = reduce_parts(devices, reps, me, grads_ref, parts_ref, sum_ref, total_ref, (s0, s1, s2, s3))
    scatter.start()
    gather.begin()
    for step, _ in enumerate(gather.steps()):
        if step == 2:
            scatter.wait_recv()
            reduce_middle(me, grads_ref, parts_ref, sum_ref, total_ref)
            share.start()
    share.wait_recv()
    scatter.wait_send()
    share.wait_send()
    gather.finish()


def third_kernel(owners, reps, grads_ref, total_ref, parts_ref, sum_ref, s0, s1, s2, s3):
    me = lax.axis_index("mem") * reps + lax.axis_index("rep")
    devices = owners * reps
    enter(devices, reps, me)
    scatter, share = reduce_parts(devices, reps, me, grads_ref, parts_ref, sum_ref, total_ref, (s0, s1, s2, s3))
    scatter.start()
    scatter.wait_recv()
    reduce_middle(me, grads_ref, parts_ref, sum_ref, total_ref)
    share.start()
    share.wait_recv()
    scatter.wait_send()
    share.wait_send()


def up8(n):
    return -(-n // 8) * 8


class Pack:
    def __init__(self, width, embed, devices):
        self.width, self.embed, self.devices = width, embed, devices
        self.high = up8(width - LANES)
        self.side = up8(embed)
        self.main = 16 * devices
        self.nbr = 2 * LANES
        self.top = 4 * LANES
        self.bottom = 5 * LANES
        self.vectors = 6 * LANES
        self.rows = 6 * LANES + 8
        self.at_top = 2 * LANES + 2 * self.high
        self.at_bottom = self.at_top + self.side
        self.extra = self.at_bottom + self.side - self.main
        self.spare = LANES - embed
        self.chunks = -(-embed // self.spare) if self.spare > 0 else 0

    def fits(self):
        return (
            self.spare > 0
            and 0 <= self.extra < self.side
            and self.chunks * (self.extra + 8) <= self.main
        )


def pack_params(pack, refs, out_ref):
    w_self, w_nbr, b_embed, w_dec1, b_dec1, w_dec2, b_dec2 = refs
    width, embed = pack.width, pack.embed
    out_ref[...] = jnp.zeros_like(out_ref)
    out_ref[0:width, 0:embed] = w_self[...]
    out_ref[pack.nbr : pack.nbr + width, 0:embed] = w_nbr[...]
    out_ref[pack.top : pack.top + embed, 0:embed] = w_dec1[0:embed, :]
    out_ref[pack.bottom : pack.bottom + embed, 0:embed] = w_dec1[embed : 2 * embed, :]
    v = pack.vectors
    out_ref[v : v + 1, 0:embed] = b_embed[...]
    out_ref[v + 1 : v + 2, 0:embed] = b_dec1[...]
    out_ref[v + 2 : v + 3, 0:embed] = w_dec2[...]
    out_ref[v + 3 : v + 4, 0:1] = b_dec2[...]


def pack_grads(pack, grads, small, table_ref, out_ref):
    s_lo, s_hi, n_lo, n_hi, top, bottom = grads
    high, side, extra = pack.high, pack.side, pack.extra
    table_ref[0:LANES] = s_lo
    table_ref[LANES : 2 * LANES] = n_lo
    table_ref[2 * LANES : 2 * LANES + high] = s_hi[:high]
    table_ref[2 * LANES + high : pack.at_top] = n_hi[:high]
    table_ref[pack.at_top : pack.at_bottom] = top[:side]
    table_ref[pack.at_bottom : pack.main] = bottom[: side - extra]
    coarse = small.astype(BF).astype(F32)
    pieces = [(0, bottom[side - extra : side])] if extra else []
    pieces.append((pack.chunks * extra, jnp.concatenate([coarse, small - coarse], 0)))
    for start, piece in pieces:
        size = piece.shape[0]
        lane = iota((size, LANES), 1)
        for k in range(pack.chunks):
            moved = pltpu.roll(piece, (pack.embed - k * pack.spare) % LANES, 1)
            rows = slice(start + k * size, start + (k + 1) * size)
            table_ref[rows] = jnp.where(lane >= pack.embed, moved, table_ref[rows])
    out_ref[...] = table_ref[...].reshape(out_ref.shape).astype(BF)


def update_params(pack, total_ref, old_ref, new_ref):
    high, side, extra = pack.high, pack.side, pack.extra
    table = total_ref[...].reshape(pack.main, LANES)

    def clean(x):
        return jnp.where(iota(x.shape, 1) < pack.embed, x, 0.0)

    def collect(start, size):
        out = jnp.zeros((size, LANES), F32)
        lane = iota((size, LANES), 1)
        for k in range(pack.chunks):
            part = table[start + k * size : start + (k + 1) * size]
            part = jnp.where(lane >= pack.embed, part, 0.0)
            out = out + pltpu.roll(part, (k * pack.spare - pack.embed) % LANES, 1)
        return out

    small = collect(pack.chunks * extra, 8)
    small = small[0:4] + small[4:8]
    lane4 = iota((4, LANES), 1)
    row4 = iota((4, LANES), 0)
    loss = jnp.sum(jnp.where((row4 == 3) & (lane4 == 1), small, 0.0))
    count = jnp.sum(jnp.where((row4 == 3) & (lane4 == 2), small, 0.0))
    small = jnp.where((row4 < 3) | (lane4 == 0), small, 0.0)
    parts = [
        (0, clean(table[0:LANES])),
        (LANES, clean(table[2 * LANES : 2 * LANES + high])),
        (pack.nbr, clean(table[LANES : 2 * LANES])),
        (pack.nbr + LANES, clean(table[2 * LANES + high : pack.at_top])),
        (pack.top, clean(table[pack.at_top : pack.at_bottom])),
        (pack.bottom, clean(table[pack.at_bottom : pack.main])),
    ]
    if extra:
        parts.append((pack.bottom + side - extra, collect(0, extra)))
    total = jnp.sum(small * small)
    for _, part in parts:
        total = total + jnp.sum(part * part)
    total = jnp.zeros((1, LANES), F32) + total
    factor = step_size / (jnp.sqrt(total) + 1e-06)
    new_ref[...] = old_ref[...]
    for start, part in parts:
        rows = slice(start, start + part.shape[0])
        new_ref[rows] = old_ref[rows] - factor * part
    rows = slice(pack.vectors, pack.vectors + 4)
    new_ref[rows] = old_ref[rows] - factor * small
    return loss / jnp.maximum(jnp.zeros((1, LANES), F32) + count, 1.0)


def unpack_params(pack, packed_ref, refs):
    w_self, w_nbr, b_embed, w_dec1, b_dec1, w_dec2, b_dec2 = refs
    width, embed = pack.width, pack.embed
    w_self[...] = packed_ref[0:width, 0:embed]
    w_nbr[...] = packed_ref[pack.nbr : pack.nbr + width, 0:embed]
    w_dec1[0:embed, :] = packed_ref[pack.top : pack.top + embed, 0:embed]
    w_dec1[embed : 2 * embed, :] = packed_ref[pack.bottom : pack.bottom + embed, 0:embed]
    v = pack.vectors
    b_embed[...] = packed_ref[v : v + 1, 0:embed]
    b_dec1[...] = packed_ref[v + 1 : v + 2, 0:embed]
    w_dec2[...] = packed_ref[v + 2 : v + 3, 0:embed]
    b_dec2[...] = packed_ref[v + 3 : v + 4, 0:1]


def expand(table_ref, low_ref, high_ref, shard, quarter):
    base = shard * 4 * quarter
    lane = iota((quarter, LANES), 1)
    for c in range(2):
        at = pl.multiple_of(base + 2 * c * quarter, quarter)
        low = table_ref[shard, BLOCKS * c : BLOCKS * c + 4].astype(F32)
        low_ref[pl.ds(at, 2 * quarter), :] = low.reshape(2 * quarter, LANES)
        both = table_ref[shard, BLOCKS * c + 4 : BLOCKS * c + 6].astype(F32).reshape(quarter, LANES)
        at = pl.multiple_of(base + 2 * c * quarter, quarter)
        high_ref[pl.ds(at, quarter), :] = jnp.where(lane < LANES // 2, both, 0.0)
        at = pl.multiple_of(base + (2 * c + 1) * quarter, quarter)
        high_ref[pl.ds(at, quarter), :] = jnp.where(
            lane < LANES // 2, pltpu.roll(both, LANES // 2, 1), 0.0
        )


def partner_rows(batch, cap, lists_smem, low_ref, high_ref, out_low, out_high):
    def one(d, carry):
        for j in range(cap):
            p = lists_smem[d, 1, batch * cap + j]
            at = d * cap + j
            out_low[pl.ds(at, 1), :] = low_ref[pl.ds(p, 1), :]
            out_high[pl.ds(at, 1), :] = high_ref[pl.ds(p, 1), :]
        return carry

    lax.fori_loop(0, lists_smem.shape[0], one, 0)


def event_rows(batch, nodes_smem, slot_smem, low_ref, high_ref, own_low, own_high, nbr_low, nbr_high):
    _, events, columns = nodes_smem.shape
    neighbours = (columns - 3) // 3

    def one(e, carry):
        def row(col):
            slot = slot_smem[nodes_smem[batch, e, col]]
            return low_ref[pl.ds(slot, 1), :], high_ref[pl.ds(slot, 1), :]

        for r in range(3):
            at = pl.ds(r * events + e, 1)
            low, high = row(r)
            own_low[at, :] = low
            own_high[at, :] = high
            low, high = row(3 + r * neighbours)
            for k in range(1, neighbours):
                more, rest = row(3 + r * neighbours + k)
                low, high = low + more, high + rest
            nbr_low[at, :] = low
            nbr_high[at, :] = high
        return carry

    lax.fori_loop(0, events, one, 0)


def pair_row(batch, cap, lists_ref, i, row):
    first, second = lists_ref[2 * i], lists_ref[2 * i + 1]
    lane = iota(first.shape, 1)
    if batch == 0:
        both = jnp.where(lane < cap, first, pltpu.roll(second, cap, 1))
    else:
        both = jnp.where(lane < cap, pltpu.roll(first, cap, 1), second)
    return both[row : row + 1]


def letter_codes(batch, cap, lists_ref, codes_ref, letters_ref):
    times = codes_ref.shape[0]
    codes = codes_ref[...]
    for i in range(lists_ref.shape[0] // 2):
        stamp = pair_row(batch, cap, lists_ref, i, 2)
        hot = jnp.where(iota((times, LANES), 0) == stamp, 1.0, 0.0).astype(BF)
        letters_ref[i * LANES : (i + 1) * LANES, 2 * LANES :] = dot_tn(hot, codes).astype(BF)


def split2(x):
    coarse = x.astype(BF)
    return coarse, (x - coarse.astype(F32)).astype(BF)


def memory_step(batch, cap, width, code, lists_ref, letters_ref, memory_ref, gi_ref, gh_ref, bias_ref, hot_ref, out_ref, blocks_ref):
    slots = memory_ref.shape[0]
    quarter = slots // 4
    pairs = lists_ref.shape[0] // 2
    lane = iota((quarter, LANES), 1)
    rest = width - LANES
    held = None
    for q in range(4):
        rows = slice(q * quarter, (q + 1) * quarter)
        for i in range(pairs):
            target = pair_row(batch, cap, lists_ref, i, 0)
            hot = jnp.where(iota((quarter, LANES), 0) + q * quarter == target, 1.0, 0.0)
            hot_ref[:, i * LANES : (i + 1) * LANES] = hot.astype(BF)
        summed = dot(hot_ref[...], letters_ref[...])
        counts = jnp.sum(
            jnp.where(lane == code, summed[:, 2 * LANES :], 0.0), 1, keepdims=True
        )
        mean = (summed / jnp.maximum(counts, 1.0)).astype(BF)
        low = memory_ref[rows, 0:LANES]
        high = pad_lanes(memory_ref[rows, LANES:width])
        old = jnp.concatenate([low, high], 1)
        state = old.astype(BF)
        joined = jnp.concatenate([state, mean], 1)
        inner = [dot(joined, gi_ref[j]) + bias_ref[j : j + 1] for j in range(3)]
        outer = [dot(state, gh_ref[j]) + bias_ref[j + 3 : j + 4] for j in range(3)]
        reset = jax.nn.sigmoid(inner[0] + outer[0])
        update = jax.nn.sigmoid(inner[1] + outer[1])
        candidate = jnp.tanh(inner[2] + reset * outer[2])
        fresh = (1.0 - update) * candidate + update * old
        new = jnp.where(counts > 0.5, fresh, old)
        new_low, new_high = new[:, :LANES], new[:, LANES:]
        out_ref[rows, 0:LANES] = new_low
        out_ref[rows, LANES:width] = new_high[:, :rest]
        if blocks_ref is not None:
            c, u = q // 2, q % 2
            at = BLOCKS * c + 2 * u
            blocks_ref[at : at + 2] = new_low.astype(BF).reshape(2, quarter // 2, LANES)
            masked = jnp.where(lane < rest, new_high, 0.0)
            if u == 0:
                held = masked
            else:
                both = (held + pltpu.roll(masked, LANES // 2, 1)).astype(BF)
                blocks_ref[BLOCKS * c + 4 : BLOCKS * c + 6] = both.reshape(2, quarter // 2, LANES)


def loss_step(pack, batch, neighbours, params_ref, valid_ref, own_low, own_high, nbr_low, nbr_high, table_ref, out_ref):
    events = valid_ref.shape[1]
    v = pack.vectors

    def weight(start):
        return params_ref[start : start + LANES].astype(BF)

    b_embed = params_ref[v : v + 1]
    b_dec1 = params_ref[v + 1 : v + 2]
    w_dec2 = params_ref[v + 2 : v + 3]
    b_dec2 = jnp.sum(params_ref[v + 3 : v + 4])
    x_low, x_high = own_low[...].astype(BF), own_high[...].astype(BF)
    n_low, n_high = split2(nbr_low[...]), split2(nbr_high[...])
    direct = dot(x_low, weight(0)) + dot(x_high, weight(LANES))
    w_low, w_high = weight(pack.nbr), weight(pack.nbr + LANES)
    spread = (
        dot(n_low[0], w_low) + dot(n_low[1], w_low) + dot(n_high[0], w_high) + dot(n_high[1], w_high)
    )
    act = jnp.tanh(direct + spread * (1.0 / neighbours) + b_embed)
    hidden = act.astype(BF)
    h0, h1, h2 = (hidden[r * events : (r + 1) * events] for r in range(3))
    top, bottom = weight(pack.top), weight(pack.bottom)
    shared = dot(h0, top)
    pre = [shared + dot(h, bottom) + b_dec1 for h in (h1, h2)]
    eye = iota((events, events), 0) == iota((events, events), 1)
    valid = jnp.where(eye, valid_ref[batch : batch + 1].astype(F32), 0.0)
    valid = jnp.sum(valid, 1, keepdims=True)
    loss = jnp.zeros((1, 1), F32)
    d_pre, g_dec2, g_out = [], jnp.zeros((1, LANES), F32), jnp.zeros((1, 1), F32)
    for z, sign in zip(pre, (-1.0, 1.0)):
        inner = jnp.maximum(z, 0.0)
        logit = (jnp.sum(inner * w_dec2, 1, keepdims=True) + b_dec2) * sign
        soft = jnp.maximum(logit, 0.0) + jnp.log1p(jnp.exp(-jnp.abs(logit)))
        loss = loss + jnp.sum(soft * valid, 0, keepdims=True)
        d_logit = jax.nn.sigmoid(logit) * valid * sign
        g_dec2 = g_dec2 + jnp.sum(d_logit * inner, 0, keepdims=True)
        g_out = g_out + jnp.sum(d_logit, 0, keepdims=True)
        d_pre.append(jnp.where(z > 0.0, d_logit * w_dec2, 0.0))
    g_dec1 = jnp.sum(d_pre[0] + d_pre[1], 0, keepdims=True)
    both = split2(d_pre[0] + d_pre[1])
    parts = [split2(d) for d in d_pre]
    g_top = dot_tn(h0, both[0]) + dot_tn(h0, both[1])
    g_bottom = (
        dot_tn(h1, parts[0][0]) + dot_tn(h1, parts[0][1])
        + dot_tn(h2, parts[1][0]) + dot_tn(h2, parts[1][1])
    )
    back = []
    for w in (top, bottom):
        back.append([(dot_nt(p[0], w) + dot_nt(p[1], w)).astype(BF) for p in parts])
    d0 = (back[0][0].astype(F32) + back[0][1].astype(F32)).astype(BF)
    d_hidden = jnp.concatenate([d0, back[1][0], back[1][1]], 0).astype(F32)
    d_act = d_hidden * (1.0 - act * act)
    g_embed = jnp.sum(d_act, 0, keepdims=True)
    d_own = split2(d_act)
    d_nbr = split2(d_act * (1.0 / neighbours))
    g_s = [dot_tn(x, d_own[0]) + dot_tn(x, d_own[1]) for x in (x_low, x_high)]
    g_n = [
        dot_tn(n[0], d_nbr[0]) + dot_tn(n[0], d_nbr[1]) + dot_tn(n[1], d_nbr[0])
        for n in (n_low, n_high)
    ]
    count = jnp.sum(valid, 0, keepdims=True)
    lane = iota((1, LANES), 1)
    scalars = jnp.where(lane == 0, g_out, jnp.where(lane == 1, loss, jnp.where(lane == 2, count, 0.0)))
    small = jnp.concatenate([g_embed, g_dec1, g_dec2, scalars], 0)
    pack_grads(pack, (g_s[0], g_s[1], g_n[0], g_n[1], g_top, g_bottom), small, table_ref, out_ref)


def start_kernel(owners, node_dev, cap, code, pack, slot_ref, pair_ref, time_ref, freq_ref, phase_ref, memory_ref, *refs):
    params, (lists_ref, codes_ref, packed_ref, blocks_ref) = refs[:7], refs[7:]
    lists_kernel(owners, node_dev, cap, code, slot_ref, pair_ref, time_ref, freq_ref, phase_ref, lists_ref, codes_ref)
    pack_params(pack, params, packed_ref)
    width = memory_ref.shape[1]
    quarter = node_dev // 4
    for c in range(2):
        for u in range(2):
            rows = slice((2 * c + u) * quarter, (2 * c + u + 1) * quarter)
            at = BLOCKS * c + 2 * u
            low = memory_ref[rows, 0:LANES].astype(BF)
            blocks_ref[at : at + 2] = low.reshape(2, quarter // 2, LANES)
        first = slice(2 * c * quarter, (2 * c + 1) * quarter)
        second = slice((2 * c + 1) * quarter, (2 * c + 2) * quarter)
        both = (
            pad_lanes(memory_ref[first, LANES:width])
            + pltpu.roll(pad_lanes(memory_ref[second, LANES:width]), LANES // 2, 1)
        ).astype(BF)
        blocks_ref[BLOCKS * c + 4 : BLOCKS * c + 6] = both.reshape(2, quarter // 2, LANES)


def batch_kernel(batch, last, cap, code, pack, nodes_smem, slot_smem, lists_smem, table_ref, lists_ref, codes_ref, memory_ref, valid_ref, gi_ref, gh_ref, bias_ref, params_ref, *refs):
    if last:
        (out_ref, grads_ref), rest = refs[:2], refs[2:]
        blocks_ref = None
    else:
        (out_ref, blocks_ref, grads_ref), rest = refs[:3], refs[3:]
    low, high, p_low, p_high, letters, hot, own_low, own_high, nbr_low, nbr_high, flat = rest
    owners = table_ref.shape[0]
    quarter = memory_ref.shape[0] // 4
    neighbours = (nodes_smem.shape[2] - 3) // 3

    def spread(s, carry):
        expand(table_ref, low, high, s, quarter)
        return carry

    lax.fori_loop(0, owners, spread, 0)
    partner_rows(batch, cap, lists_smem, low, high, p_low, p_high)
    letters[:, 0:LANES] = p_low[...].astype(BF)
    letters[:, LANES : 2 * LANES] = p_high[...].astype(BF)
    letter_codes(batch, cap, lists_ref, codes_ref, letters)
    memory_step(batch, cap, pack.width, code, lists_ref, letters, memory_ref, gi_ref, gh_ref, bias_ref, hot, out_ref, blocks_ref)
    event_rows(batch, nodes_smem, slot_smem, low, high, own_low, own_high, nbr_low, nbr_high)
    loss_step(pack, batch, neighbours, params_ref, valid_ref, own_low, own_high, nbr_low, nbr_high, flat, grads_ref)


def update_kernel(pack, total_ref, old_ref, new_ref, loss_ref):
    loss_ref[...] = update_params(pack, total_ref, old_ref, new_ref)


def final_kernel(pack, total_ref, old_ref, *refs):
    loss_ref, outs, new_ref = refs[0], refs[1:8], refs[8]
    loss_ref[...] = update_params(pack, total_ref, old_ref, new_ref)
    unpack_params(pack, new_ref, outs)


def quick_body(owners, reps, cap, memory, node_slot, event_nodes, event_times, valid_mask, time_freq, time_phase, gru_input, gru_hidden, gru_in_bias, gru_hid_bias, *params):
    node_dev, width = memory.shape
    batches, events, columns = event_nodes.shape
    code = time_freq.shape[0]
    embed = params[0].shape[1]
    devices = owners * reps
    pack = Pack(width, embed, devices)
    quarter = node_dev // 4
    sds = jax.ShapeDtypeStruct
    pairs = event_nodes[:, :, :2].transpose(0, 2, 1).reshape(1, -1)
    times = jnp.broadcast_to(event_times[:, None, :], (batches, 2, events)).reshape(1, -1)
    freq = jnp.pad(time_freq, (0, LANES - code))[None, :]
    phase = jnp.pad(time_phase, (0, LANES - code))[None, :]
    rows = [p[None, :] if p.ndim == 1 else p for p in params]
    stamps = -(-TIMES // LANES) * LANES
    lists, codes, packed, blocks = pl.pallas_call(
        functools.partial(start_kernel, owners, node_dev, cap, code, pack),
        out_shape=(
            sds((owners, 8, 2 * cap), jnp.int32),
            sds((stamps, LANES), BF),
            sds((pack.rows, LANES), F32),
            sds((2 * BLOCKS, quarter // 2, LANES), BF),
        ),
        in_specs=vmem(13),
        out_specs=tuple(vmem(4)),
        name="start",
    )(node_slot.reshape(-1, LANES), pairs, times, freq, phase, memory, *rows)

    pad_w = 2 * LANES - width
    gi = gru_input.reshape(-1, 3, width).transpose(1, 0, 2)
    gi = jnp.concatenate(
        [
            jnp.pad(gi[:, :width], ((0, 0), (0, pad_w), (0, pad_w))),
            jnp.pad(gi[:, width : 2 * width], ((0, 0), (0, pad_w), (0, pad_w))),
            jnp.pad(gi[:, 2 * width :], ((0, 0), (0, LANES - code), (0, pad_w))),
        ],
        1,
    )
    gh = jnp.pad(gru_hidden.reshape(width, 3, width).transpose(1, 0, 2), ((0, 0), (0, pad_w), (0, pad_w)))
    bias = jnp.pad(
        jnp.concatenate([gru_in_bias.reshape(3, width), gru_hid_bias.reshape(3, width)], 0),
        ((0, 2), (0, pad_w)),
    )

    dma = pltpu.SemaphoreType.DMA
    sends = gather_sends(owners)
    gather_sems = [dma((sends,)), dma((owners, 2 * BLOCKS)), dma((2,))]
    reduce_scratch = [
        pltpu.VMEM((devices, 16, LANES), BF),
        pltpu.VMEM((16, LANES), F32),
        dma((devices,)),
        dma((devices,)),
        dma((devices,)),
        dma((devices,)),
    ]
    table_shape = sds((owners, 2 * BLOCKS, quarter // 2, LANES), BF)
    total_shape = sds((devices, 16, LANES), F32)
    table, all_lists = pl.pallas_call(
        functools.partial(first_kernel, owners, reps),
        out_shape=(table_shape, sds((devices, 8, 2 * cap), jnp.int32)),
        in_specs=vmem(2),
        out_specs=tuple(vmem(2)),
        scratch_shapes=gather_sems + [dma((devices,)), dma((devices,))],
        compiler_params=pltpu.CompilerParams(collective_id=0, has_side_effects=True),
        name="first",
    )(blocks, lists)

    losses = []
    for batch in range(batches):
        last = batch == batches - 1
        outs = [sds((node_dev, width), F32)]
        if not last:
            outs.append(sds((2 * BLOCKS, quarter // 2, LANES), BF))
        outs.append(sds((devices, 16, LANES), BF))
        letters = devices * cap
        slots = node_slot.shape[0]
        made = pl.pallas_call(
            functools.partial(batch_kernel, batch, last, cap, code, pack),
            out_shape=tuple(outs),
            in_specs=[pl.BlockSpec(memory_space=pltpu.SMEM)] * 3 + vmem(9),
            out_specs=tuple(vmem(len(outs))),
            scratch_shapes=[
                pltpu.VMEM((slots, LANES), F32),
                pltpu.VMEM((slots, LANES), F32),
                pltpu.VMEM((letters, LANES), F32),
                pltpu.VMEM((letters, LANES), F32),
                pltpu.VMEM((letters, 3 * LANES), BF),
                pltpu.VMEM((quarter, letters), BF),
                pltpu.VMEM((3 * events, LANES), F32),
                pltpu.VMEM((3 * events, LANES), F32),
                pltpu.VMEM((3 * events, LANES), F32),
                pltpu.VMEM((3 * events, LANES), F32),
                pltpu.VMEM((pack.main, LANES), F32),
            ],
            compiler_params=pltpu.CompilerParams(vmem_limit_bytes=48 * 1024 * 1024),
            name="batch" + str(batch),
        )(event_nodes, node_slot, all_lists, table, all_lists, codes, memory, valid_mask, gi, gh, bias, packed)
        if last:
            memory, grads = made
            total = pl.pallas_call(
                functools.partial(third_kernel, owners, reps),
                out_shape=total_shape,
                in_specs=vmem(1),
                out_specs=vmem(1)[0],
                scratch_shapes=reduce_scratch,
                compiler_params=pltpu.CompilerParams(collective_id=2, has_side_effects=True),
                name="third",
            )(grads)
            outs = pl.pallas_call(
                functools.partial(final_kernel, pack),
                out_shape=(sds((1, LANES), F32),) + tuple(sds(p.shape, F32) for p in rows),
                in_specs=vmem(2),
                out_specs=tuple(vmem(8)),
                scratch_shapes=[pltpu.VMEM((pack.rows, LANES), F32)],
                name="final",
            )(total, packed)
            losses.append(outs[0])
            params = [o.reshape(p.shape) for o, p in zip(outs[1:], params)]
        else:
            memory, blocks, grads = made
            table, total = pl.pallas_call(
                functools.partial(second_kernel, owners, reps),
                out_shape=(table_shape, total_shape),
                in_specs=vmem(2),
                out_specs=tuple(vmem(2)),
                scratch_shapes=gather_sems + reduce_scratch,
                compiler_params=pltpu.CompilerParams(collective_id=1, has_side_effects=True),
                name="second",
            )(blocks, grads)
            packed, loss = pl.pallas_call(
                functools.partial(update_kernel, pack),
                out_shape=(sds((pack.rows, LANES), F32), sds((1, LANES), F32)),
                in_specs=vmem(2),
                out_specs=tuple(vmem(2)),
                name="update",
            )(total, packed)
            losses.append(loss)
    losses = jnp.concatenate([loss[:, 0] for loss in losses])
    return (memory, losses, *params)


def block_loss(current, own_rows, beside_sum, neighbours, valid_part):
    w_self, w_nbr, b_embed, w_dec1, b_dec1, w_dec2, b_dec2 = current
    num_events = own_rows.shape[0] // 3
    direct = jnp.dot(own_rows, w_self.astype(jnp.bfloat16), preferred_element_type=jnp.float32)
    spread = jnp.dot(
        beside_sum,
        w_nbr.astype(jnp.bfloat16).astype(jnp.float32),
        precision=lax.Precision.HIGHEST,
    )
    hidden = jnp.tanh(direct + spread * (1.0 / neighbours) + b_embed).astype(jnp.bfloat16)
    first = hidden[:num_events]
    paired = jnp.concatenate(
        [jnp.concatenate([first, first], 0), hidden[num_events:]],
        1,
    )
    inner_act = jax.nn.relu(
        jnp.dot(paired, w_dec1.astype(jnp.bfloat16), preferred_element_type=jnp.float32) + b_dec1
    )
    logits = jnp.sum(inner_act * w_dec2, 1) + b_dec2[0]
    weights = valid_part.astype(jnp.float32)
    sign_flip = jnp.concatenate(
        [-jnp.ones((num_events,), jnp.float32), jnp.ones((num_events,), jnp.float32)]
    )
    return jnp.sum(jax.nn.softplus(sign_flip * logits) * jnp.concatenate([weights, weights]))


def normalized_step(params, gradients):
    total = jnp.zeros((), jnp.float32)
    for grad_part in gradients:
        total = total + jnp.sum(grad_part * grad_part)
    factor = step_size / (jnp.sqrt(total) + 1e-06)
    return tuple((value - factor * grad_part for value, grad_part in zip(params, gradients)))


def memory_update(
    mean_rest, state_bf, old_state, gru_input, gru_hidden, gru_in_bias, gru_hid_bias
):
    row_width = old_state.shape[1]
    from_input = (
        jnp.dot(state_bf, gru_input[:row_width], preferred_element_type=jnp.float32)
        + jnp.dot(mean_rest, gru_input[row_width:], preferred_element_type=jnp.float32)
        + gru_in_bias
    )
    from_state = jnp.dot(state_bf, gru_hidden, preferred_element_type=jnp.float32) + gru_hid_bias
    reset = jax.nn.sigmoid(from_input[:, :row_width] + from_state[:, :row_width])
    update = jax.nn.sigmoid(
        from_input[:, row_width : 2 * row_width] + from_state[:, row_width : 2 * row_width]
    )
    candidate = jnp.tanh(from_input[:, 2 * row_width :] + reset * from_state[:, 2 * row_width :])
    return (1.0 - update) * candidate + update * old_state


def look_up(table, ids):
    width = 128
    groups = table.shape[0] // width
    grid = table.reshape(groups, width)
    digits = jnp.concatenate([grid >> 8, grid & 255], 1).astype(jnp.bfloat16)
    pick = ((ids // width)[..., None] == jnp.arange(groups, dtype=jnp.int32)).astype(jnp.bfloat16)
    rows = jnp.dot(pick, digits, preferred_element_type=jnp.float32)
    here = (ids % width)[..., None] == jnp.arange(width, dtype=jnp.int32)
    both = jnp.where(here, rows[..., :width] * 256.0 + rows[..., width:], 0.0)
    return jnp.sum(both, -1).astype(jnp.int32)


def sum_everywhere(gradients, loss_local, count_local, devices):
    g_self, g_nbr, g_embed, g_dec1, g_bias1, g_dec2, g_bias2 = gradients
    width = g_self.shape[1]
    scalars = jnp.concatenate([g_bias2, loss_local[None], count_local[None]])
    scalars = jnp.pad(scalars, (0, width - scalars.shape[0]))
    table = jnp.concatenate(
        [g_self, g_nbr, g_dec1, jnp.stack([g_embed, g_bias1, g_dec2, scalars])], 0
    )
    used = table.shape[0]
    share = -(-used // (devices * 8)) * 8
    table = jnp.pad(table, ((0, share * devices - used), (0, 0))).reshape(devices, share, width)
    parts = lax.all_to_all(table, ("mem", "rep"), split_axis=0, concat_axis=0, tiled=True)
    total = lax.all_gather(jnp.sum(parts, 0), ("mem", "rep"), axis=0, tiled=True)
    n_self, n_nbr, n_dec1 = g_self.shape[0], g_nbr.shape[0], g_dec1.shape[0]
    at = n_self + n_nbr + n_dec1
    return (
        (
            total[:n_self],
            total[n_self : n_self + n_nbr],
            total[at],
            total[n_self + n_nbr : at],
            total[at + 1],
            total[at + 2],
            total[at + 3, :1],
        ),
        total[at + 3, 1],
        total[at + 3, 2],
    )


def place_rows(owner_ids, owners, stride, offset):
    length = owner_ids.shape[0]
    width = 128
    groups = -(-length // width)
    padded_ids = owner_ids.reshape(groups, width)
    one_hot = (padded_ids[:, :, None] == jnp.arange(owners, dtype=jnp.int32)[None, None, :]).astype(
        jnp.float32
    )
    lower = (
        jnp.arange(width, dtype=jnp.int32)[:, None] > jnp.arange(width, dtype=jnp.int32)[None, :]
    ).astype(jnp.float32)
    within = jnp.einsum("ij,gjo->gio", lower, one_hot, precision=lax.Precision.HIGHEST)
    totals = jnp.sum(one_hot, 1)
    starts = jnp.cumsum(totals, 0) - totals
    before = jnp.sum((within + starts[:, None, :]) * one_hot, 2).reshape(-1)
    return owner_ids * stride + offset + before.astype(jnp.int32)


def body(
    memory,
    node_slot,
    event_nodes,
    event_times,
    valid_mask,
    time_freq,
    time_phase,
    gru_input,
    gru_hidden,
    gru_in_bias,
    gru_hid_bias,
    w_self,
    w_nbr,
    b_embed,
    w_dec1,
    b_dec1,
    w_dec2,
    b_dec2,
):
    owners = lax.axis_size("mem")
    devices = owners * lax.axis_size("rep")
    node_dev, row_width = memory.shape
    batches, events, columns = event_nodes.shape
    neighbours = (columns - 3) // 3
    cap_pair = 2 * events // owners * 2
    params = (w_self, w_nbr, b_embed, w_dec1, b_dec1, w_dec2, b_dec2)
    losses = []
    all_slots = look_up(node_slot, event_nodes.transpose(0, 2, 1))
    for batch_index in range(batches):
        slot_ids = all_slots[batch_index]
        memory_bf = memory.astype(jnp.bfloat16)
        whole_bf = lax.all_gather(memory_bf, "mem", axis=0, tiled=True)
        fetched = jnp.take(whole_bf, slot_ids.reshape(-1), axis=0, mode="clip")
        own_rows = fetched[: 3 * events]
        beside = fetched[3 * events :].reshape(3, neighbours, events, row_width)
        beside_sum = jnp.sum(beside.astype(jnp.float32), 1).reshape(3 * events, row_width)

        pair_slots = slot_ids[:2].reshape(-1)
        pair_at = place_rows(pair_slots // node_dev, owners, cap_pair, 0)
        offsets = (pair_slots % node_dev).astype(jnp.int32)
        time_code = jnp.cos(
            event_times[batch_index].astype(jnp.float32)[:, None] * time_freq + time_phase
        ).astype(jnp.bfloat16)
        marks = jnp.stack([jnp.ones_like(offsets), offsets // 128, offsets % 128], 1)
        partners = jnp.concatenate([own_rows[events : 2 * events], own_rows[:events]], 0)
        letters = jnp.concatenate(
            [partners, jnp.concatenate([time_code, time_code], 0), marks.astype(jnp.bfloat16)], 1
        )
        seats = jnp.arange(owners * cap_pair, dtype=jnp.int32)[:, None] == pair_at[None, :]
        parcel = jnp.dot(
            seats.astype(jnp.bfloat16), letters, preferred_element_type=jnp.float32
        ).astype(jnp.bfloat16)
        parcel = parcel.reshape(owners, cap_pair, letters.shape[1])
        parcel = lax.all_to_all(parcel, "mem", split_axis=0, concat_axis=0, tiled=True)
        every_parcel = lax.all_gather(parcel, "rep", axis=0, tiled=True)
        every_parcel = every_parcel.reshape(-1, letters.shape[1])
        digits = every_parcel[:, -2:].astype(jnp.int32)
        target = digits[:, 0] * 128 + digits[:, 1]
        matches = jnp.arange(node_dev, dtype=jnp.int32)[:, None] == target[None, :]
        summed = jnp.dot(
            matches.astype(jnp.bfloat16), every_parcel, preferred_element_type=jnp.float32
        )
        counts = summed[:, -3:-2]
        mean_rest = (summed[:, :-3] / jnp.maximum(counts, 1.0)).astype(jnp.bfloat16)
        fresh = memory_update(
            mean_rest, memory_bf, memory, gru_input, gru_hidden, gru_in_bias, gru_hid_bias
        )
        memory = jnp.where(counts > 0, fresh, memory)

        valid_part = valid_mask[batch_index]
        loss_local, pullback = jax.vjp(
            lambda current: block_loss(current, own_rows, beside_sum, neighbours, valid_part),
            params,
        )
        gradients = pullback(jnp.ones_like(loss_local))[0]
        count_local = jnp.sum(valid_part.astype(jnp.float32))
        gradients, loss_total, count_total = sum_everywhere(
            gradients, loss_local, count_local, devices
        )
        params = normalized_step(params, gradients)
        losses.append(loss_total / jnp.maximum(count_total, 1.0))
    return (
        memory,
        jnp.stack(losses),
        params[0],
        params[1],
        params[2],
        params[3],
        params[4],
        params[5],
        params[6],
    )


def solution(mesh):
    owners, reps = mesh.shape["mem"], mesh.shape["rep"]
    in_specs = (
        P("mem", None),
        P(),
        P(None, ("mem", "rep"), None),
        P(None, ("mem", "rep")),
        P(None, ("mem", "rep")),
    ) + (P(),) * 13
    out_specs = (P("mem", None),) + (P(),) * 8

    def choose(*args):
        memory, node_slot, event_nodes = args[:3]
        node_dev, width = memory.shape
        batches, events, _ = event_nodes.shape
        cap = 2 * events // owners * 2
        pack = Pack(width, args[11].shape[1], owners * reps)
        small = node_slot.shape[0] * 2 * LANES * 4 <= 16 * 1024 * 1024
        shaped = (
            reps == 4
            and owners % 2 == 0
            and owners > 4
            and batches == 2
            and 2 * cap == LANES
            and events == LANES
            and node_dev % (4 * LANES) == 0
            and LANES < width <= LANES + LANES // 2
            and args[5].shape[0] < LANES
            and pack.fits()
        )
        if small and shaped:
            return quick_body(owners, reps, cap, *args)
        return body(*args)

    return jax.shard_map(choose, mesh=mesh, in_specs=in_specs, out_specs=out_specs, check_vma=False)
```

```python
import functools

import jax
import jax.numpy as jnp
from jax import lax
from jax.experimental import pallas as pl
from jax.experimental.pallas import tpu as pltpu
from jax.sharding import PartitionSpec as P

step_size = 4.0
LANES = 128
TIMES = 1000
MESH_ID = pl.DeviceIdType.MESH
BF = jnp.bfloat16
F32 = jnp.float32
HI = lax.Precision.HIGHEST


def vmem(count):
    return [pl.BlockSpec(memory_space=pltpu.VMEM)] * count


def dot(a, b, precision=None):
    return lax.dot_general(
        a, b, (((1,), (0,)), ((), ())), precision=precision, preferred_element_type=F32
    )


def dot_tn(a, b, precision=None):
    return lax.dot_general(
        a, b, (((0,), (0,)), ((), ())), precision=precision, preferred_element_type=F32
    )


def dot_nt(a, b, precision=None):
    return lax.dot_general(
        a, b, (((1,), (1,)), ((), ())), precision=precision, preferred_element_type=F32
    )


def iota(shape, axis):
    return lax.broadcasted_iota(jnp.int32, shape, axis)


def pad_lanes(x):
    return jnp.concatenate([x, jnp.zeros((x.shape[0], LANES - x.shape[1]), x.dtype)], 1)


def pad_rows(x, rows):
    return jnp.concatenate([x, jnp.zeros((rows - x.shape[0], x.shape[1]), x.dtype)], 0)


def make_lists(owners, node_dev, cap, slot_ref, nodes_ref, time_ref, lists_ref):
    groups = slot_ref.shape[0]
    ids = []
    for b in range(2):
        ids += [nodes_ref[0, b : b + 1], nodes_ref[1, b : b + 1]]
    ids = jnp.concatenate(ids, 1)
    letters = ids.shape[1]
    per_batch = letters // 2
    grid = slot_ref[...]
    digits = jnp.concatenate([grid >> 8, grid & 255], 1).astype(F32).astype(BF)
    group_hot = jnp.where(iota((groups, letters), 0) == (ids >> 7), 1.0, 0.0).astype(BF)
    found = dot_tn(digits, group_hot)
    here = iota((LANES, letters), 0) == (ids & 127)
    slots_f = jnp.sum(jnp.where(here, found[:LANES] * 256.0 + found[LANES:], 0.0), 0, keepdims=True)
    slots = slots_f.astype(jnp.int32)
    events = per_batch // 2
    partners = jnp.concatenate(
        [
            slots[:, events : 2 * events],
            slots[:, :events],
            slots[:, 3 * events :],
            slots[:, 2 * events : 3 * events],
        ],
        1,
    )
    owner = slots // node_dev
    offset = slots - owner * node_dev
    owner_hot = jnp.where(iota((owners, letters), 0) == owner, 1.0, 0.0)
    earlier = jnp.where(
        iota((per_batch, per_batch), 0) < iota((per_batch, per_batch), 1), 1.0, 0.0
    ).astype(BF)
    hot_bf = owner_hot.astype(BF)
    before = jnp.concatenate(
        [dot(hot_bf[:, :per_batch], earlier), dot(hot_bf[:, per_batch:], earlier)], 1
    )
    rank = jnp.sum(before * owner_hot, 0, keepdims=True).astype(jnp.int32)
    batch = iota((1, letters), 1) // per_batch
    seat = owner * (2 * cap) + batch * cap + rank
    times = jnp.concatenate([time_ref[0:1], time_ref[0:1], time_ref[1:2], time_ref[1:2]], 1)
    values = jnp.concatenate(
        [
            offset >> 8, offset & 255, partners >> 8, partners & 255,
            times >> 8, times & 255, jnp.ones_like(times), jnp.zeros_like(times),
        ],
        0,
    ).astype(F32).astype(BF)
    for o in range(owners):
        seats = jnp.where(iota((2 * cap, letters), 0) + o * 2 * cap == seat, 1.0, 0.0).astype(BF)
        placed = dot_nt(values, seats)
        taken = placed[6:7] > 0.5
        rows = [
            jnp.where(taken, placed[0:1] * 256.0 + placed[1:2], float(node_dev)),
            placed[2:3] * 256.0 + placed[3:4],
            placed[4:5] * 256.0 + placed[5:6],
        ]
        lists_ref[o] = jnp.concatenate(rows + [jnp.zeros((5, 2 * cap), F32)], 0).astype(jnp.int32)


def make_codes(width, pad_ref, codes_ref):
    stamps = iota(codes_ref.shape, 0).astype(F32)
    lane = iota(codes_ref.shape, 1)
    code = jnp.cos(stamps * pad_ref[0:1] + pad_ref[1:2])
    code = jnp.where(lane < width, code, jnp.where(lane == width, 1.0, 0.0))
    codes_ref[...] = code.astype(BF)


def peer(index, reps):
    return (index // reps, lax.rem(index, reps))


BLOCKS = 6


class Gather:
    def __init__(self, owners, own_ref, table_ref, send_sem, recv_sem, local_sem):
        self.outer = owners // 2
        mem = lax.axis_index("mem")
        rep = lax.axis_index("rep")
        self.a, self.b = mem // 2, lax.rem(mem, 2)
        self.u, self.c = rep // 2, lax.rem(rep, 2)
        self.mem, self.rep = mem, rep
        self.own, self.table = own_ref, table_ref
        self.send_sem, self.recv_sem = send_sem, recv_sem
        self.local = pltpu.make_async_copy(own_ref, table_ref.at[mem], local_sem)
        self.sent = 0
        base = BLOCKS * self.c
        self.line_first = [base + 2 * self.u, base + 2 * self.u + 1, base + 4]
        self.pair_first = base + 5
        self.planes = [base + 2 * (1 - self.u), base + 2 * (1 - self.u) + 1]
        self.ahead = (jnp.minimum(mem + 2, owners - 1), rep)
        self.behind = (jnp.maximum(mem - 2, 0), rep)
        self.beside = (2 * self.a + 1 - self.b, rep)
        self.plane = (mem, 2 * (1 - self.u) + self.c)
        self.core = (mem, 2 * self.u + 1 - self.c)
        self.checks = []

    def push(self, shard, block, target, from_own=False, when=None):
        index = self.sent
        self.sent += 1
        src = self.own.at[block] if from_own else self.table.at[shard, block]

        def go():
            pltpu.make_async_remote_copy(
                src_ref=src,
                dst_ref=self.table.at[shard, block],
                send_sem=self.send_sem.at[index],
                recv_sem=self.recv_sem.at[shard, block],
                device_id=target,
                device_id_type=MESH_ID,
            ).start()

        self.guard(when, go)
        self.checks.append((index, when))

    def guard(self, when, go):
        if when is None:
            go()
        else:
            pl.when(when)(go)

    def arrived(self, shard, block):
        ref = self.table.at[shard, block]
        pltpu.make_async_copy(ref, ref, self.recv_sem.at[shard, block]).wait()

    def along(self, shard, block, from_own=False):
        self.push(shard, block, self.ahead, from_own, self.a < self.outer - 1)
        self.push(shard, block, self.behind, from_own, self.a > 0)

    def begin(self):
        self.local.start()
        self.push(self.mem, self.pair_first, self.beside, True)
        for block in self.line_first:
            self.along(self.mem, block, True)
            self.push(self.mem, block, self.beside, True)
        self.along(self.mem, self.pair_first, True)

    def shard(self, t, other):
        at = jnp.clip(self.a + t, 0, self.outer - 1)
        return 2 * at + (1 - self.b if other else self.b)

    def take(self, t, other, k):
        shard = self.shard(t, other)
        block = self.line_first[k] if k < 3 else self.pair_first
        onward = (t != 0) and not (other and k < 3)

        there = None
        if t < 0:
            there = self.a >= -t
        if t > 0:
            there = self.a < self.outer - t

        def also(extra):
            return extra if there is None else there & extra

        self.guard(there, lambda: self.arrived(shard, block))
        if t == 0 and k == 3:
            self.along(shard, block)
        if onward and t < 0:
            self.push(shard, block, self.ahead, when=also(self.a < self.outer - 1))
        if onward and t > 0:
            self.push(shard, block, self.behind, when=also(self.a > 0))
        if not other and k < 3:
            self.push(shard, block, self.beside, when=there)
        if k < 2:
            self.push(shard, block, self.plane, when=there)
        self.push(shard, block, self.core, when=there)

    def from_plane(self, t, other, k):
        shard, block = self.shard(t, other), self.planes[k]
        there = None
        if t < 0:
            there = self.a >= -t
        if t > 0:
            there = self.a < self.outer - t
        self.guard(there, lambda: self.arrived(shard, block))
        self.push(shard, block, self.core, when=there)

    def from_core(self, t, other):
        shard = self.shard(t, other)
        there = None
        if t < 0:
            there = self.a >= -t
        if t > 0:
            there = self.a < self.outer - t

        def go():
            for k in range(BLOCKS):
                self.arrived(shard, BLOCKS * (1 - self.c) + k)

        self.guard(there, go)

    def steps(self):
        far = self.outer - 1
        self.take(0, True, 3)
        for k in range(3):
            for t in (-1, 1):
                self.take(t, False, k)
            self.take(0, True, k)
            yield
        for t in range(1, far + 1):
            for k in range(3):
                for s in (-t, t):
                    self.take(s, True, k)
                    if t < far:
                        self.take(s + (1 if s > 0 else -1), False, k)
                yield
            for s in (-t, t):
                self.take(s, False, 3)
                self.take(s, True, 3)
            if t == 1:
                self.from_plane(0, True, 0)
                self.from_plane(0, True, 1)
            yield
            for s in (-t, t):
                for k in range(2):
                    self.from_plane(s, False, k)
                    self.from_plane(s, True, k)
            yield
        self.local.wait()
        self.from_core(0, True)
        for t in range(1, far + 1):
            for s in (-t, t):
                self.from_core(s, False)
                self.from_core(s, True)

    def finish(self):
        for index, when in self.checks:
            ref = self.own.at[0]
            copy = pltpu.make_async_copy(ref, ref, self.send_sem.at[index])
            self.guard(when, copy.wait)


def gather_sends(owners):
    outer = owners // 2
    return 12 + 16 * outer + 4 * BLOCKS * owners


class Exchange:
    def __init__(self, devices, reps, me, source, target, send_sem, recv_sem):
        self.devices, self.reps, self.me = devices, reps, me
        self.source, self.target = source, target
        self.send_sem, self.recv_sem = send_sem, recv_sem

    def copy(self, k):
        to = lax.rem(self.me + k, self.devices)
        return pltpu.make_async_remote_copy(
            src_ref=self.source(to),
            dst_ref=self.target(self.me),
            send_sem=self.send_sem.at[k],
            recv_sem=self.recv_sem.at[k],
            device_id=peer(to, self.reps),
            device_id_type=MESH_ID,
        )

    def start(self):
        def one(k, carry):
            self.copy(k).start()
            return carry

        lax.fori_loop(1, self.devices, one, 0)

    def wait_recv(self):
        def one(k, carry):
            come = lax.rem(self.me + self.devices - k, self.devices)
            ref = self.target(come)
            pltpu.make_async_copy(ref, ref, self.recv_sem.at[k]).wait()
            return carry

        lax.fori_loop(1, self.devices, one, 0)

    def wait_send(self):
        def one(k, carry):
            self.copy(k).wait_send()
            return carry

        lax.fori_loop(1, self.devices, one, 0)


def reduce_parts(devices, reps, me, grads_ref, parts_ref, sum_ref, total_ref, sems):
    scatter = Exchange(
        devices, reps, me, lambda to: grads_ref.at[to], lambda come: parts_ref.at[come],
        sems[0], sems[1],
    )
    share = Exchange(
        devices, reps, me, lambda to: sum_ref, lambda come: total_ref.at[come], sems[2], sems[3]
    )
    return scatter, share


def reduce_middle(me, grads_ref, parts_ref, sum_ref, total_ref):
    parts_ref[me] = grads_ref[me]
    total = jnp.sum(parts_ref[...].astype(F32), 0)
    sum_ref[...] = total
    total_ref[me] = total


def up8(n):
    return -(-n // 8) * 8


class Pack:
    def __init__(self, width, embed, devices):
        self.width, self.embed, self.devices = width, embed, devices
        self.high = up8(width - LANES)
        self.side = up8(embed)
        self.main = 16 * devices
        self.nbr = 2 * LANES
        self.top = 4 * LANES
        self.bottom = 5 * LANES
        self.vectors = 6 * LANES
        self.rows = 6 * LANES + 8
        self.at_top = 2 * LANES + 2 * self.high
        self.at_bottom = self.at_top + self.side
        self.extra = self.at_bottom + self.side - self.main
        self.spare = LANES - embed
        self.chunks = -(-embed // self.spare) if self.spare > 0 else 0

    def fits(self):
        return (
            self.spare > 0
            and 0 <= self.extra < self.side
            and self.chunks * (self.extra + 8) <= self.main
        )


def pack_params(pack, refs, out_ref):
    w_self, w_nbr, b_embed, w_dec1, b_dec1, w_dec2, b_dec2 = refs
    width, embed = pack.width, pack.embed
    out_ref[...] = jnp.zeros_like(out_ref)
    out_ref[0:width, 0:embed] = w_self[...]
    out_ref[pack.nbr : pack.nbr + width, 0:embed] = w_nbr[...]
    out_ref[pack.top : pack.top + embed, 0:embed] = w_dec1[0:embed, :]
    out_ref[pack.bottom : pack.bottom + embed, 0:embed] = w_dec1[embed : 2 * embed, :]
    v = pack.vectors
    out_ref[v : v + 1, 0:embed] = b_embed[...]
    out_ref[v + 1 : v + 2, 0:embed] = b_dec1[...]
    out_ref[v + 2 : v + 3, 0:embed] = w_dec2[...]
    out_ref[v + 3 : v + 4, 0:1] = b_dec2[...]


def pack_grads(pack, grads, small, table_ref, out_ref):
    s_lo, s_hi, n_lo, n_hi, top, bottom = grads
    high, side, extra = pack.high, pack.side, pack.extra
    table_ref[0:LANES] = s_lo
    table_ref[LANES : 2 * LANES] = n_lo
    table_ref[2 * LANES : 2 * LANES + high] = s_hi[:high]
    table_ref[2 * LANES + high : pack.at_top] = n_hi[:high]
    table_ref[pack.at_top : pack.at_bottom] = top[:side]
    table_ref[pack.at_bottom : pack.main] = bottom[: side - extra]
    coarse = small.astype(BF).astype(F32)
    pieces = [(0, bottom[side - extra : side])] if extra else []
    pieces.append((pack.chunks * extra, jnp.concatenate([coarse, small - coarse], 0)))
    for start, piece in pieces:
        size = piece.shape[0]
        lane = iota((size, LANES), 1)
        for k in range(pack.chunks):
            moved = pltpu.roll(piece, (pack.embed - k * pack.spare) % LANES, 1)
            rows = slice(start + k * size, start + (k + 1) * size)
            table_ref[rows] = jnp.where(lane >= pack.embed, moved, table_ref[rows])
    out_ref[...] = table_ref[...].reshape(out_ref.shape).astype(BF)


def update_params(pack, total_ref, old_ref, new_ref):
    high, side, extra = pack.high, pack.side, pack.extra
    table = total_ref[...].reshape(pack.main, LANES)

    def clean(x):
        return jnp.where(iota(x.shape, 1) < pack.embed, x, 0.0)

    def collect(start, size):
        out = jnp.zeros((size, LANES), F32)
        lane = iota((size, LANES), 1)
        for k in range(pack.chunks):
            part = table[start + k * size : start + (k + 1) * size]
            part = jnp.where(lane >= pack.embed, part, 0.0)
            out = out + pltpu.roll(part, (k * pack.spare - pack.embed) % LANES, 1)
        return out

    small = collect(pack.chunks * extra, 8)
    small = small[0:4] + small[4:8]
    lane4 = iota((4, LANES), 1)
    row4 = iota((4, LANES), 0)
    loss = jnp.sum(jnp.where((row4 == 3) & (lane4 == 1), small, 0.0))
    count = jnp.sum(jnp.where((row4 == 3) & (lane4 == 2), small, 0.0))
    small = jnp.where((row4 < 3) | (lane4 == 0), small, 0.0)
    parts = [
        (0, clean(table[0:LANES])),
        (LANES, clean(table[2 * LANES : 2 * LANES + high])),
        (pack.nbr, clean(table[LANES : 2 * LANES])),
        (pack.nbr + LANES, clean(table[2 * LANES + high : pack.at_top])),
        (pack.top, clean(table[pack.at_top : pack.at_bottom])),
        (pack.bottom, clean(table[pack.at_bottom : pack.main])),
    ]
    if extra:
        parts.append((pack.bottom + side - extra, collect(0, extra)))
    total = jnp.sum(small * small)
    for _, part in parts:
        total = total + jnp.sum(part * part)
    total = jnp.zeros((1, LANES), F32) + total
    factor = step_size / (jnp.sqrt(total) + 1e-06)
    new_ref[...] = old_ref[...]
    for start, part in parts:
        rows = slice(start, start + part.shape[0])
        new_ref[rows] = old_ref[rows] - factor * part
    rows = slice(pack.vectors, pack.vectors + 4)
    new_ref[rows] = old_ref[rows] - factor * small
    return loss / jnp.maximum(jnp.zeros((1, LANES), F32) + count, 1.0)


def unpack_params(pack, packed_ref, refs):
    w_self, w_nbr, b_embed, w_dec1, b_dec1, w_dec2, b_dec2 = refs
    width, embed = pack.width, pack.embed
    w_self[...] = packed_ref[0:width, 0:embed]
    w_nbr[...] = packed_ref[pack.nbr : pack.nbr + width, 0:embed]
    w_dec1[0:embed, :] = packed_ref[pack.top : pack.top + embed, 0:embed]
    w_dec1[embed : 2 * embed, :] = packed_ref[pack.bottom : pack.bottom + embed, 0:embed]
    v = pack.vectors
    b_embed[...] = packed_ref[v : v + 1, 0:embed]
    b_dec1[...] = packed_ref[v + 1 : v + 2, 0:embed]
    w_dec2[...] = packed_ref[v + 2 : v + 3, 0:embed]
    b_dec2[...] = packed_ref[v + 3 : v + 4, 0:1]


def expand(table_ref, low_ref, high_ref, shard, quarter):
    base = shard * 4 * quarter
    lane = iota((quarter, LANES), 1)
    for c in range(2):
        at = pl.multiple_of(base + 2 * c * quarter, quarter)
        low = table_ref[shard, BLOCKS * c : BLOCKS * c + 4].astype(F32)
        low_ref[pl.ds(at, 2 * quarter), :] = low.reshape(2 * quarter, LANES)
        both = table_ref[shard, BLOCKS * c + 4 : BLOCKS * c + 6].astype(F32).reshape(quarter, LANES)
        at = pl.multiple_of(base + 2 * c * quarter, quarter)
        high_ref[pl.ds(at, quarter), :] = jnp.where(lane < LANES // 2, both, 0.0)
        at = pl.multiple_of(base + (2 * c + 1) * quarter, quarter)
        high_ref[pl.ds(at, quarter), :] = jnp.where(
            lane < LANES // 2, pltpu.roll(both, LANES // 2, 1), 0.0
        )


def partner_rows(batch, cap, lists_smem, low_ref, high_ref, out_low, out_high):
    slots = low_ref.shape[0]

    def one(d, carry):
        for j in range(cap):
            p = lists_smem[d, 1, batch * cap + j]
            p = p & (slots - 1) if slots & (slots - 1) == 0 else jnp.clip(p, 0, slots - 1)
            at = d * cap + j
            out_low[pl.ds(at, 1), :] = low_ref[pl.ds(p, 1), :]
            out_high[pl.ds(at, 1), :] = high_ref[pl.ds(p, 1), :]
        return carry

    lax.fori_loop(0, lists_smem.shape[0], one, 0)


def event_rows(batch, first, count, nodes_smem, slot_smem, low_ref, high_ref, own_low, own_high, nbr_low, nbr_high):
    neighbours = (nodes_smem.shape[0] - 3) // 3
    events = nodes_smem.shape[2]

    def one(e, carry):
        def row(col):
            slot = slot_smem[nodes_smem[col, batch, e]]
            return low_ref[pl.ds(slot, 1), :], high_ref[pl.ds(slot, 1), :]

        for r in range(3):
            at = pl.ds(r * events + e, 1)
            low, high = row(r)
            own_low[at, :] = low
            own_high[at, :] = high
            low, high = row(3 + r * neighbours)
            for k in range(1, neighbours):
                more, rest = row(3 + r * neighbours + k)
                low, high = low + more, high + rest
            nbr_low[at, :] = low
            nbr_high[at, :] = high
        return carry

    lax.fori_loop(first, first + count, one, 0)


def pair_row(batch, cap, lists_ref, i, row):
    first, second = lists_ref[2 * i], lists_ref[2 * i + 1]
    lane = iota(first.shape, 1)
    if batch == 0:
        both = jnp.where(lane < cap, first, pltpu.roll(second, cap, 1))
    else:
        both = jnp.where(lane < cap, pltpu.roll(first, cap, 1), second)
    return both[row : row + 1]


def letter_codes(batch, cap, lists_ref, codes_ref, letters_ref):
    times = codes_ref.shape[0]
    codes = codes_ref[...]
    for i in range(lists_ref.shape[0] // 2):
        stamp = pair_row(batch, cap, lists_ref, i, 2)
        hot = jnp.where(iota((times, LANES), 0) == stamp, 1.0, 0.0).astype(BF)
        letters_ref[i * LANES : (i + 1) * LANES, 2 * LANES :] = dot_tn(hot, codes).astype(BF)


def split2(x):
    coarse = x.astype(BF)
    return coarse, (x - coarse.astype(F32)).astype(BF)


def memory_step(batch, cap, width, code, lists_ref, letters_ref, memory_ref, gi_ref, gh_ref, bias_ref, hot_ref, out_ref, blocks_ref):
    slots = memory_ref.shape[0]
    quarter = slots // 4
    pairs = lists_ref.shape[0] // 2
    lane = iota((quarter, LANES), 1)
    rest = width - LANES
    held = None
    for q in range(4):
        rows = slice(q * quarter, (q + 1) * quarter)
        for i in range(pairs):
            target = pair_row(batch, cap, lists_ref, i, 0)
            hot = jnp.where(iota((quarter, LANES), 0) + q * quarter == target, 1.0, 0.0)
            hot_ref[:, i * LANES : (i + 1) * LANES] = hot.astype(BF)
        summed = dot(hot_ref[...], letters_ref[...])
        counts = jnp.sum(
            jnp.where(lane == code, summed[:, 2 * LANES :], 0.0), 1, keepdims=True
        )
        mean = (summed / jnp.maximum(counts, 1.0)).astype(BF)
        low = memory_ref[rows, 0:LANES]
        high = memory_ref[rows, LANES : 2 * LANES]
        old = jnp.concatenate([low, high], 1)
        state = old.astype(BF)
        joined = jnp.concatenate([state, mean], 1)
        inner = [dot(joined, gi_ref[j]) + bias_ref[j : j + 1] for j in range(3)]
        outer = [dot(state, gh_ref[j]) + bias_ref[j + 3 : j + 4] for j in range(3)]
        reset = jax.nn.sigmoid(inner[0] + outer[0])
        update = jax.nn.sigmoid(inner[1] + outer[1])
        candidate = jnp.tanh(inner[2] + reset * outer[2])
        fresh = (1.0 - update) * candidate + update * old
        new = jnp.where(counts > 0.5, fresh, old)
        new_low, new_high = new[:, :LANES], new[:, LANES:]
        if blocks_ref is None:
            out_ref[0:LANES, rows] = new_low.T
            out_ref[LANES:width, rows] = new_high.T[:rest]
        else:
            out_ref[rows, 0:LANES] = new_low
            out_ref[rows, LANES : 2 * LANES] = new_high
            c, u = q // 2, q % 2
            at = BLOCKS * c + 2 * u
            blocks_ref[at : at + 2] = new_low.astype(BF).reshape(2, quarter // 2, LANES)
            masked = jnp.where(lane < rest, new_high, 0.0)
            if u == 0:
                held = masked
            else:
                both = (held + pltpu.roll(masked, LANES // 2, 1)).astype(BF)
                blocks_ref[BLOCKS * c + 4 : BLOCKS * c + 6] = both.reshape(2, quarter // 2, LANES)


def loss_step(pack, batch, neighbours, params_ref, valid_ref, own_low, own_high, nbr_low, nbr_high, table_ref, out_ref):
    events = valid_ref.shape[1]
    v = pack.vectors

    def weight(start):
        return params_ref[start : start + LANES].astype(BF)

    b_embed = params_ref[v : v + 1]
    b_dec1 = params_ref[v + 1 : v + 2]
    w_dec2 = params_ref[v + 2 : v + 3]
    b_dec2 = jnp.sum(params_ref[v + 3 : v + 4])
    x_low, x_high = own_low[...].astype(BF), own_high[...].astype(BF)
    n_low, n_high = split2(nbr_low[...]), split2(nbr_high[...])
    direct = dot(x_low, weight(0)) + dot(x_high, weight(LANES))
    w_low, w_high = weight(pack.nbr), weight(pack.nbr + LANES)
    spread = (
        dot(n_low[0], w_low) + dot(n_low[1], w_low) + dot(n_high[0], w_high) + dot(n_high[1], w_high)
    )
    act = jnp.tanh(direct + spread * (1.0 / neighbours) + b_embed)
    hidden = act.astype(BF)
    h0, h1, h2 = (hidden[r * events : (r + 1) * events] for r in range(3))
    top, bottom = weight(pack.top), weight(pack.bottom)
    shared = dot(h0, top)
    pre = [shared + dot(h, bottom) + b_dec1 for h in (h1, h2)]
    eye = iota((events, events), 0) == iota((events, events), 1)
    valid = jnp.where(eye, valid_ref[batch : batch + 1].astype(F32), 0.0)
    valid = jnp.sum(valid, 1, keepdims=True)
    loss = jnp.zeros((1, 1), F32)
    d_pre, g_dec2, g_out = [], jnp.zeros((1, LANES), F32), jnp.zeros((1, 1), F32)
    for z, sign in zip(pre, (-1.0, 1.0)):
        inner = jnp.maximum(z, 0.0)
        logit = (jnp.sum(inner * w_dec2, 1, keepdims=True) + b_dec2) * sign
        soft = jnp.maximum(logit, 0.0) + jnp.log1p(jnp.exp(-jnp.abs(logit)))
        loss = loss + jnp.sum(soft * valid, 0, keepdims=True)
        d_logit = jax.nn.sigmoid(logit) * valid * sign
        g_dec2 = g_dec2 + jnp.sum(d_logit * inner, 0, keepdims=True)
        g_out = g_out + jnp.sum(d_logit, 0, keepdims=True)
        d_pre.append(jnp.where(z > 0.0, d_logit * w_dec2, 0.0))
    g_dec1 = jnp.sum(d_pre[0] + d_pre[1], 0, keepdims=True)
    both = split2(d_pre[0] + d_pre[1])
    parts = [split2(d) for d in d_pre]
    g_top = dot_tn(h0, both[0]) + dot_tn(h0, both[1])
    g_bottom = (
        dot_tn(h1, parts[0][0]) + dot_tn(h1, parts[0][1])
        + dot_tn(h2, parts[1][0]) + dot_tn(h2, parts[1][1])
    )
    back = []
    for w in (top, bottom):
        back.append([(dot_nt(p[0], w) + dot_nt(p[1], w)).astype(BF) for p in parts])
    d0 = (back[0][0].astype(F32) + back[0][1].astype(F32)).astype(BF)
    d_hidden = jnp.concatenate([d0, back[1][0], back[1][1]], 0).astype(F32)
    d_act = d_hidden * (1.0 - act * act)
    g_embed = jnp.sum(d_act, 0, keepdims=True)
    d_own = split2(d_act)
    d_nbr = split2(d_act * (1.0 / neighbours))
    g_s = [dot_tn(x, d_own[0]) + dot_tn(x, d_own[1]) for x in (x_low, x_high)]
    g_n = [
        dot_tn(n[0], d_nbr[0]) + dot_tn(n[0], d_nbr[1]) + dot_tn(n[1], d_nbr[0])
        for n in (n_low, n_high)
    ]
    count = jnp.sum(valid, 0, keepdims=True)
    lane = iota((1, LANES), 1)
    scalars = jnp.where(lane == 0, g_out, jnp.where(lane == 1, loss, jnp.where(lane == 2, count, 0.0)))
    small = jnp.concatenate([g_embed, g_dec1, g_dec2, scalars], 0)
    pack_grads(pack, (g_s[0], g_s[1], g_n[0], g_n[1], g_top, g_bottom), small, table_ref, out_ref)


def turn_memory(turned_ref, memory_ref, blocks_ref):
    width, node_dev = turned_ref.shape
    quarter = node_dev // 4
    rest = width - LANES
    held = None
    for q in range(4):
        rows = slice(q * quarter, (q + 1) * quarter)
        c, u = q // 2, q % 2
        low = turned_ref[0:LANES, rows].T
        memory_ref[rows, 0:LANES] = low
        at = BLOCKS * c + 2 * u
        blocks_ref[at : at + 2] = low.astype(BF).reshape(2, quarter // 2, LANES)
        pad = jnp.zeros((LANES - up8(rest), quarter), F32)
        high = turned_ref[LANES:width, rows]
        if up8(rest) != rest:
            high = jnp.concatenate([high, jnp.zeros((up8(rest) - rest, quarter), F32)], 0)
        high = jnp.concatenate([high, pad], 0).T
        memory_ref[rows, LANES : 2 * LANES] = high
        if u == 0:
            held = high
        else:
            both = (held + pltpu.roll(high, LANES // 2, 1)).astype(BF)
            blocks_ref[BLOCKS * c + 4 : BLOCKS * c + 6] = both.reshape(2, quarter // 2, LANES)


def pack_turned(width, source_ref, spans, wide_ref, out_ref):
    rows, columns = source_ref.shape
    wide_ref[...] = jnp.zeros_like(wide_ref)
    wide_ref[0:rows, 0:columns] = source_ref[...].astype(F32)
    total = wide_ref.shape[1]
    keep = 2 * LANES
    for j in range(3):
        part = wide_ref[j * width : j * width + keep, :]
        for start, size, to in spans:
            span = -(-size // LANES) * LANES
            moved = part if start == 0 else pltpu.roll(part, total - start, 1)
            moved = moved[:, :span]
            inside = (iota(moved.shape, 1) < size) & (iota(moved.shape, 0) < width)
            out_ref[j, to : to + span, :] = jnp.where(inside, moved, 0.0).T.astype(BF)


def pack_gates(width, source_ref, spans, wide_ref, out_ref):
    rows, columns = source_ref.shape
    wide_ref[...] = jnp.zeros_like(wide_ref)
    wide_ref[0:rows, 0:columns] = source_ref[...].astype(F32)
    total = wide_ref.shape[1]
    out_ref[...] = jnp.zeros_like(out_ref)
    for start, size, to in spans:
        part = wide_ref[start : start + size, :]
        for j in range(3):
            moved = part if j == 0 else pltpu.roll(part, total - j * width, 1)
            moved = moved[:, : 2 * LANES]
            moved = jnp.where(iota(moved.shape, 1) < width, moved, 0.0)
            out_ref[j, to : to + size, :] = moved.astype(BF)


def pack_bias(width, in_ref, hid_ref, wide_ref, out_ref):
    total = wide_ref.shape[1]
    columns = in_ref.shape[0]
    wide_ref[0:8, :] = jnp.zeros((8, total), F32)
    wide_ref[0:1, 0:columns] = in_ref[...].reshape(1, columns)
    wide_ref[1:2, 0:columns] = hid_ref[...].reshape(1, columns)
    part = wide_ref[0:8, :]
    for j in range(3):
        moved = part if j == 0 else pltpu.roll(part, total - j * width, 1)
        moved = jnp.where(iota((8, 2 * LANES), 1) < width, moved[:, : 2 * LANES], 0.0)
        out_ref[j : j + 1] = moved[0:1]
        out_ref[j + 3 : j + 4] = moved[1:2]


def window_kernel(owners, reps, cap, code, pack, *refs):
    (
        nodes_smem, slot_smem, nodes_ref, slot_ref, time_ref, valid_ref, freq_ref, phase_ref,
        turned_ref, gru_in_ref, gru_hid_ref, in_bias_ref, hid_bias_ref,
    ) = refs[:13]
    params = refs[13:20]
    memory_out, loss_ref, packed_out = refs[20:23]
    (
        memory_ref, blocks, table, low, high, p_low, p_high, letters, hot, own_low, own_high, nbr_low, nbr_high,
        flat, middle, lists_ref, all_lists, lists_smem, codes, packed, gi, gh, bias, wide, pad_ref,
        grads, parts, sums, totals,
        send_sems, recv_sems, local_sem, list_sems, reduce_sems,
    ) = refs[23:]
    me = lax.axis_index("mem") * reps + lax.axis_index("rep")
    devices = owners * reps
    width, node_dev = turned_ref.shape
    quarter = node_dev // 4
    columns, _, events = nodes_ref.shape
    neighbours = (columns - 3) // 3

    barrier = pltpu.get_barrier_semaphore()

    def greet(k, carry):
        pl.semaphore_signal(
            barrier, inc=1, device_id=peer(lax.rem(me + k, devices), reps), device_id_type=MESH_ID
        )
        return carry

    lax.fori_loop(1, devices, greet, 0)
    turn_memory(turned_ref, memory_ref, blocks.at[0])
    pl.semaphore_wait(barrier, devices - 1)

    gathers = [
        Gather(owners, blocks.at[b], table.at[b], send_sems.at[b], recv_sems.at[b], local_sem.at[b])
        for b in range(2)
    ]
    exchange = Exchange(
        devices, reps, me,
        lambda to: lists_ref.at[to // reps], lambda come: all_lists.at[come],
        list_sems.at[0], list_sems.at[1],
    )
    mine = pltpu.make_async_copy(
        lists_ref.at[lax.axis_index("mem")], all_lists.at[me], local_sem.at[2]
    )
    to_smem = pltpu.make_async_copy(all_lists, lists_smem, local_sem.at[3])
    reduces = [
        reduce_parts(
            devices, reps, me, grads.at[b], parts.at[b], sums.at[b], totals.at[b],
            [reduce_sems.at[4 * b + i] for i in range(4)],
        )
        for b in range(2)
    ]

    gathers[0].begin()
    make_lists(owners, node_dev, cap, slot_ref, nodes_ref, time_ref, lists_ref)
    exchange.start()
    mine.start()

    def time_table():
        pad_ref[...] = jnp.zeros_like(pad_ref)
        pad_ref[0:1, 0:code] = freq_ref[...]
        pad_ref[1:2, 0:code] = phase_ref[...]
        make_codes(code, pad_ref, codes)

    def lists_in():
        exchange.wait_recv()
        mine.wait()
        to_smem.start()

    def codes_of(batch):
        return lambda: letter_codes(batch, cap, all_lists, codes, letters.at[batch])

    shadow = [
        lambda: pack_turned(
            width, gru_in_ref,
            [(0, width, 0), (width, width, 2 * LANES), (2 * width, code, 4 * LANES)],
            wide, gi,
        ),
        lambda: pack_gates(width, gru_hid_ref, [(0, width, 0)], wide, gh),
        lambda: pack_bias(width, in_bias_ref, hid_bias_ref, wide, bias),
        lambda: pack_params(pack, params, packed.at[0]),
        time_table,
        lists_in,
        codes_of(0),
        codes_of(1),
    ]
    for _ in gathers[0].steps():
        if shadow:
            shadow.pop(0)()
    for task in shadow:
        task()
    to_smem.wait()

    def spread(b):
        def one(s, carry):
            expand(table.at[b], low, high, s, quarter)
            return carry

        lax.fori_loop(0, owners, one, 0)

    def partners(b):
        partner_rows(b, cap, lists_smem, low, high, p_low, p_high)
        letters[b, :, 0:LANES] = p_low[...].astype(BF)
        letters[b, :, LANES : 2 * LANES] = p_high[...].astype(BF)

    def remember(b, old_ref, new_ref, blocks_ref):
        memory_step(
            b, cap, width, code, all_lists, letters.at[b], old_ref, gi, gh, bias, hot, new_ref, blocks_ref
        )

    def rows_of(b, first, count):
        event_rows(
            b, first, count, nodes_smem, slot_smem, low, high, own_low, own_high, nbr_low, nbr_high
        )

    def loss_of(b):
        loss_step(
            pack, b, neighbours, packed.at[b], valid_ref, own_low, own_high, nbr_low, nbr_high, flat,
            grads.at[b],
        )

    spread(0)
    partners(0)
    remember(0, memory_ref, middle, blocks.at[1])
    gathers[1].begin()
    pieces = 16
    size = events // pieces
    tasks = [functools.partial(rows_of, 0, i * size, size) for i in range(pieces)]

    def send_grads():
        loss_of(0)
        reduces[0][0].start()

    tasks.append(send_grads)
    for _ in gathers[1].steps():
        if tasks:
            tasks.pop(0)()
    for task in tasks:
        task()
    reduces[0][0].wait_recv()
    reduce_middle(me, grads.at[0], parts.at[0], sums.at[0], totals.at[0])
    reduces[0][1].start()

    spread(1)
    rows_of(1, 0, events)
    reduces[0][1].wait_recv()
    loss0 = update_params(pack, totals.at[0], packed.at[0], packed.at[1])
    loss_of(1)
    reduces[1][0].start()
    partners(1)
    reduces[1][0].wait_recv()
    reduce_middle(me, grads.at[1], parts.at[1], sums.at[1], totals.at[1])
    reduces[1][1].start()
    remember(1, middle, memory_out, None)
    reduces[1][1].wait_recv()
    loss1 = update_params(pack, totals.at[1], packed.at[1], packed_out)
    loss_ref[...] = jnp.where(iota((1, LANES), 1) == 0, loss0, loss1)

    exchange.wait_send()
    for scatter, share in reduces:
        scatter.wait_send()
        share.wait_send()
    for gather in gathers:
        gather.finish()


def final_kernel(pack, memory_ref, loss_ref, packed_ref, memory_out, loss_out, *outs):
    memory_out[...] = memory_ref[...]
    loss_out[...] = loss_ref[0, 0:2]
    unpack_params(pack, packed_ref, outs)


def quick_body(owners, reps, cap, memory, node_slot, event_nodes, event_times, valid_mask, time_freq, time_phase, gru_input, gru_hidden, gru_in_bias, gru_hid_bias, *params):
    node_dev, width = memory.shape
    batches, events, columns = event_nodes.shape
    code = time_freq.shape[0]
    devices = owners * reps
    pack = Pack(width, params[0].shape[1], devices)
    quarter = node_dev // 4
    slots = node_slot.shape[0]
    letters = devices * cap
    sends = gather_sends(owners)
    stamps = -(-TIMES // LANES) * LANES
    wide_rows = up8(2 * width + 2 * LANES)
    wide_lanes = -(-3 * width // LANES) * LANES + LANES
    sds = jax.ShapeDtypeStruct
    dma = pltpu.SemaphoreType.DMA
    rows = [p[None, :] if p.ndim == 1 else p for p in params]
    smem = [pl.BlockSpec(memory_space=pltpu.SMEM)]
    nodes = event_nodes.transpose(2, 0, 1)
    made = pl.pallas_call(
        functools.partial(window_kernel, owners, reps, cap, code, pack),
        out_shape=(sds((width, node_dev), F32), sds((1, LANES), F32), sds((pack.rows, LANES), F32)),
        in_specs=smem * 2 + vmem(18),
        out_specs=tuple(vmem(3)),
        scratch_shapes=[
            pltpu.VMEM((node_dev, 2 * LANES), F32),
            pltpu.VMEM((2, 2 * BLOCKS, quarter // 2, LANES), BF),
            pltpu.VMEM((2, owners, 2 * BLOCKS, quarter // 2, LANES), BF),
            pltpu.VMEM((slots, LANES), F32),
            pltpu.VMEM((slots, LANES), F32),
            pltpu.VMEM((letters, LANES), F32),
            pltpu.VMEM((letters, LANES), F32),
            pltpu.VMEM((2, letters, 3 * LANES), BF),
            pltpu.VMEM((quarter, letters), BF),
            pltpu.VMEM((3 * events, LANES), F32),
            pltpu.VMEM((3 * events, LANES), F32),
            pltpu.VMEM((3 * events, LANES), F32),
            pltpu.VMEM((3 * events, LANES), F32),
            pltpu.VMEM((pack.main, LANES), F32),
            pltpu.VMEM((node_dev, 2 * LANES), F32),
            pltpu.VMEM((owners, 8, 2 * cap), jnp.int32),
            pltpu.VMEM((devices, 8, 2 * cap), jnp.int32),
            pltpu.SMEM((devices, 8, 2 * cap), jnp.int32),
            pltpu.VMEM((stamps, LANES), BF),
            pltpu.VMEM((2, pack.rows, LANES), F32),
            pltpu.VMEM((3, 5 * LANES, 2 * LANES), BF),
            pltpu.VMEM((3, 2 * LANES, 2 * LANES), BF),
            pltpu.VMEM((8, 2 * LANES), F32),
            pltpu.VMEM((wide_rows, wide_lanes), F32),
            pltpu.VMEM((8, LANES), F32),
            pltpu.VMEM((2, devices, 16, LANES), BF),
            pltpu.VMEM((2, devices, 16, LANES), BF),
            pltpu.VMEM((2, 16, LANES), F32),
            pltpu.VMEM((2, devices, 16, LANES), F32),
            dma((2, sends)),
            dma((2, owners, 2 * BLOCKS)),
            dma((4,)),
            dma((2, devices)),
            dma((8, devices)),
        ],
        compiler_params=pltpu.CompilerParams(
            collective_id=0, has_side_effects=True, vmem_limit_bytes=56 * 1024 * 1024
        ),
        name="window",
    )(
        nodes, node_slot, nodes, node_slot.reshape(-1, LANES), event_times, valid_mask,
        time_freq[None, :], time_phase[None, :], memory.T, gru_input.T, gru_hidden,
        gru_in_bias, gru_hid_bias, *rows,
    )
    outs = pl.pallas_call(
        functools.partial(final_kernel, pack),
        out_shape=(sds((width, node_dev), F32), sds((batches,), F32))
        + tuple(sds(p.shape, F32) for p in rows),
        in_specs=vmem(3),
        out_specs=tuple(vmem(9)),
        name="final",
    )(*made)
    new = [o.reshape(p.shape) for o, p in zip(outs[2:], params)]
    return (outs[0].T, outs[1], *new)


def block_loss(current, own_rows, beside_sum, neighbours, valid_part):
    w_self, w_nbr, b_embed, w_dec1, b_dec1, w_dec2, b_dec2 = current
    num_events = own_rows.shape[0] // 3
    direct = jnp.dot(own_rows, w_self.astype(jnp.bfloat16), preferred_element_type=jnp.float32)
    spread = jnp.dot(
        beside_sum,
        w_nbr.astype(jnp.bfloat16).astype(jnp.float32),
        precision=lax.Precision.HIGHEST,
    )
    hidden = jnp.tanh(direct + spread * (1.0 / neighbours) + b_embed).astype(jnp.bfloat16)
    first = hidden[:num_events]
    paired = jnp.concatenate(
        [jnp.concatenate([first, first], 0), hidden[num_events:]],
        1,
    )
    inner_act = jax.nn.relu(
        jnp.dot(paired, w_dec1.astype(jnp.bfloat16), preferred_element_type=jnp.float32) + b_dec1
    )
    logits = jnp.sum(inner_act * w_dec2, 1) + b_dec2[0]
    weights = valid_part.astype(jnp.float32)
    sign_flip = jnp.concatenate(
        [-jnp.ones((num_events,), jnp.float32), jnp.ones((num_events,), jnp.float32)]
    )
    return jnp.sum(jax.nn.softplus(sign_flip * logits) * jnp.concatenate([weights, weights]))


def normalized_step(params, gradients):
    total = jnp.zeros((), jnp.float32)
    for grad_part in gradients:
        total = total + jnp.sum(grad_part * grad_part)
    factor = step_size / (jnp.sqrt(total) + 1e-06)
    return tuple((value - factor * grad_part for value, grad_part in zip(params, gradients)))


def memory_update(
    mean_rest, state_bf, old_state, gru_input, gru_hidden, gru_in_bias, gru_hid_bias
):
    row_width = old_state.shape[1]
    from_input = (
        jnp.dot(state_bf, gru_input[:row_width], preferred_element_type=jnp.float32)
        + jnp.dot(mean_rest, gru_input[row_width:], preferred_element_type=jnp.float32)
        + gru_in_bias
    )
    from_state = jnp.dot(state_bf, gru_hidden, preferred_element_type=jnp.float32) + gru_hid_bias
    reset = jax.nn.sigmoid(from_input[:, :row_width] + from_state[:, :row_width])
    update = jax.nn.sigmoid(
        from_input[:, row_width : 2 * row_width] + from_state[:, row_width : 2 * row_width]
    )
    candidate = jnp.tanh(from_input[:, 2 * row_width :] + reset * from_state[:, 2 * row_width :])
    return (1.0 - update) * candidate + update * old_state


def look_up(table, ids):
    width = 128
    groups = table.shape[0] // width
    grid = table.reshape(groups, width)
    digits = jnp.concatenate([grid >> 8, grid & 255], 1).astype(jnp.bfloat16)
    pick = ((ids // width)[..., None] == jnp.arange(groups, dtype=jnp.int32)).astype(jnp.bfloat16)
    rows = jnp.dot(pick, digits, preferred_element_type=jnp.float32)
    here = (ids % width)[..., None] == jnp.arange(width, dtype=jnp.int32)
    both = jnp.where(here, rows[..., :width] * 256.0 + rows[..., width:], 0.0)
    return jnp.sum(both, -1).astype(jnp.int32)


def sum_everywhere(gradients, loss_local, count_local, devices):
    g_self, g_nbr, g_embed, g_dec1, g_bias1, g_dec2, g_bias2 = gradients
    width = g_self.shape[1]
    scalars = jnp.concatenate([g_bias2, loss_local[None], count_local[None]])
    scalars = jnp.pad(scalars, (0, width - scalars.shape[0]))
    table = jnp.concatenate(
        [g_self, g_nbr, g_dec1, jnp.stack([g_embed, g_bias1, g_dec2, scalars])], 0
    )
    used = table.shape[0]
    share = -(-used // (devices * 8)) * 8
    table = jnp.pad(table, ((0, share * devices - used), (0, 0))).reshape(devices, share, width)
    parts = lax.all_to_all(table, ("mem", "rep"), split_axis=0, concat_axis=0, tiled=True)
    total = lax.all_gather(jnp.sum(parts, 0), ("mem", "rep"), axis=0, tiled=True)
    n_self, n_nbr, n_dec1 = g_self.shape[0], g_nbr.shape[0], g_dec1.shape[0]
    at = n_self + n_nbr + n_dec1
    return (
        (
            total[:n_self],
            total[n_self : n_self + n_nbr],
            total[at],
            total[n_self + n_nbr : at],
            total[at + 1],
            total[at + 2],
            total[at + 3, :1],
        ),
        total[at + 3, 1],
        total[at + 3, 2],
    )


def place_rows(owner_ids, owners, stride, offset):
    length = owner_ids.shape[0]
    width = 128
    groups = -(-length // width)
    padded_ids = owner_ids.reshape(groups, width)
    one_hot = (padded_ids[:, :, None] == jnp.arange(owners, dtype=jnp.int32)[None, None, :]).astype(
        jnp.float32
    )
    lower = (
        jnp.arange(width, dtype=jnp.int32)[:, None] > jnp.arange(width, dtype=jnp.int32)[None, :]
    ).astype(jnp.float32)
    within = jnp.einsum("ij,gjo->gio", lower, one_hot, precision=lax.Precision.HIGHEST)
    totals = jnp.sum(one_hot, 1)
    starts = jnp.cumsum(totals, 0) - totals
    before = jnp.sum((within + starts[:, None, :]) * one_hot, 2).reshape(-1)
    return owner_ids * stride + offset + before.astype(jnp.int32)


def body(
    memory,
    node_slot,
    event_nodes,
    event_times,
    valid_mask,
    time_freq,
    time_phase,
    gru_input,
    gru_hidden,
    gru_in_bias,
    gru_hid_bias,
    w_self,
    w_nbr,
    b_embed,
    w_dec1,
    b_dec1,
    w_dec2,
    b_dec2,
):
    owners = lax.axis_size("mem")
    devices = owners * lax.axis_size("rep")
    node_dev, row_width = memory.shape
    batches, events, columns = event_nodes.shape
    neighbours = (columns - 3) // 3
    cap_pair = 2 * events // owners * 2
    params = (w_self, w_nbr, b_embed, w_dec1, b_dec1, w_dec2, b_dec2)
    losses = []
    all_slots = look_up(node_slot, event_nodes.transpose(0, 2, 1))
    for batch_index in range(batches):
        slot_ids = all_slots[batch_index]
        memory_bf = memory.astype(jnp.bfloat16)
        whole_bf = lax.all_gather(memory_bf, "mem", axis=0, tiled=True)
        fetched = jnp.take(whole_bf, slot_ids.reshape(-1), axis=0, mode="clip")
        own_rows = fetched[: 3 * events]
        beside = fetched[3 * events :].reshape(3, neighbours, events, row_width)
        beside_sum = jnp.sum(beside.astype(jnp.float32), 1).reshape(3 * events, row_width)

        pair_slots = slot_ids[:2].reshape(-1)
        pair_at = place_rows(pair_slots // node_dev, owners, cap_pair, 0)
        offsets = (pair_slots % node_dev).astype(jnp.int32)
        time_code = jnp.cos(
            event_times[batch_index].astype(jnp.float32)[:, None] * time_freq + time_phase
        ).astype(jnp.bfloat16)
        marks = jnp.stack([jnp.ones_like(offsets), offsets // 128, offsets % 128], 1)
        partners = jnp.concatenate([own_rows[events : 2 * events], own_rows[:events]], 0)
        letters = jnp.concatenate(
            [partners, jnp.concatenate([time_code, time_code], 0), marks.astype(jnp.bfloat16)], 1
        )
        seats = jnp.arange(owners * cap_pair, dtype=jnp.int32)[:, None] == pair_at[None, :]
        parcel = jnp.dot(
            seats.astype(jnp.bfloat16), letters, preferred_element_type=jnp.float32
        ).astype(jnp.bfloat16)
        parcel = parcel.reshape(owners, cap_pair, letters.shape[1])
        parcel = lax.all_to_all(parcel, "mem", split_axis=0, concat_axis=0, tiled=True)
        every_parcel = lax.all_gather(parcel, "rep", axis=0, tiled=True)
        every_parcel = every_parcel.reshape(-1, letters.shape[1])
        digits = every_parcel[:, -2:].astype(jnp.int32)
        target = digits[:, 0] * 128 + digits[:, 1]
        matches = jnp.arange(node_dev, dtype=jnp.int32)[:, None] == target[None, :]
        summed = jnp.dot(
            matches.astype(jnp.bfloat16), every_parcel, preferred_element_type=jnp.float32
        )
        counts = summed[:, -3:-2]
        mean_rest = (summed[:, :-3] / jnp.maximum(counts, 1.0)).astype(jnp.bfloat16)
        fresh = memory_update(
            mean_rest, memory_bf, memory, gru_input, gru_hidden, gru_in_bias, gru_hid_bias
        )
        memory = jnp.where(counts > 0, fresh, memory)

        valid_part = valid_mask[batch_index]
        loss_local, pullback = jax.vjp(
            lambda current: block_loss(current, own_rows, beside_sum, neighbours, valid_part),
            params,
        )
        gradients = pullback(jnp.ones_like(loss_local))[0]
        count_local = jnp.sum(valid_part.astype(jnp.float32))
        gradients, loss_total, count_total = sum_everywhere(
            gradients, loss_local, count_local, devices
        )
        params = normalized_step(params, gradients)
        losses.append(loss_total / jnp.maximum(count_total, 1.0))
    return (
        memory,
        jnp.stack(losses),
        params[0],
        params[1],
        params[2],
        params[3],
        params[4],
        params[5],
        params[6],
    )


def solution(mesh):
    owners, reps = mesh.shape["mem"], mesh.shape["rep"]
    in_specs = (
        P("mem", None),
        P(),
        P(None, ("mem", "rep"), None),
        P(None, ("mem", "rep")),
        P(None, ("mem", "rep")),
    ) + (P(),) * 13
    out_specs = (P("mem", None),) + (P(),) * 8

    def choose(*args):
        memory, node_slot, event_nodes = args[:3]
        node_dev, width = memory.shape
        batches, events, _ = event_nodes.shape
        cap = 2 * events // owners * 2
        pack = Pack(width, args[11].shape[1], owners * reps)
        small = node_slot.shape[0] * 2 * LANES * 4 <= 16 * 1024 * 1024
        shaped = (
            reps == 4
            and owners % 2 == 0
            and owners > 4
            and batches == 2
            and 2 * cap == LANES
            and events == LANES
            and node_dev % (4 * LANES) == 0
            and LANES < width <= LANES + LANES // 2
            and args[5].shape[0] < LANES
            and pack.fits()
        )
        if small and shaped:
            return quick_body(owners, reps, cap, *args)
        return body(*args)

    return jax.shard_map(choose, mesh=mesh, in_specs=in_specs, out_specs=out_specs, check_vma=False)
```

```python
import functools

import jax
import jax.numpy as jnp
from jax import lax
from jax.experimental import pallas as pl
from jax.experimental.pallas import tpu as pltpu
from jax.sharding import PartitionSpec as P

step_size = 4.0
LANES = 128
TIMES = 1000
MESH_ID = pl.DeviceIdType.MESH
BF = jnp.bfloat16
F32 = jnp.float32
HI = lax.Precision.HIGHEST


def vmem(count):
    return [pl.BlockSpec(memory_space=pltpu.VMEM)] * count


def dot(a, b, precision=None):
    return lax.dot_general(
        a, b, (((1,), (0,)), ((), ())), precision=precision, preferred_element_type=F32
    )


def dot_tn(a, b, precision=None):
    return lax.dot_general(
        a, b, (((0,), (0,)), ((), ())), precision=precision, preferred_element_type=F32
    )


def dot_nt(a, b, precision=None):
    return lax.dot_general(
        a, b, (((1,), (1,)), ((), ())), precision=precision, preferred_element_type=F32
    )


def iota(shape, axis):
    return lax.broadcasted_iota(jnp.int32, shape, axis)


def pad_lanes(x):
    return jnp.concatenate([x, jnp.zeros((x.shape[0], LANES - x.shape[1]), x.dtype)], 1)


def pad_rows(x, rows):
    return jnp.concatenate([x, jnp.zeros((rows - x.shape[0], x.shape[1]), x.dtype)], 0)


def make_lists(owners, node_dev, cap, slot_ref, nodes_ref, time_ref, lists_ref):
    groups = slot_ref.shape[0]
    ids = []
    for b in range(2):
        ids += [nodes_ref[0, b : b + 1], nodes_ref[1, b : b + 1]]
    ids = jnp.concatenate(ids, 1)
    letters = ids.shape[1]
    per_batch = letters // 2
    grid = slot_ref[...]
    digits = jnp.concatenate([grid >> 8, grid & 255], 1).astype(F32).astype(BF)
    group_hot = jnp.where(iota((groups, letters), 0) == (ids >> 7), 1.0, 0.0).astype(BF)
    found = dot_tn(digits, group_hot)
    here = iota((LANES, letters), 0) == (ids & 127)
    slots_f = jnp.sum(jnp.where(here, found[:LANES] * 256.0 + found[LANES:], 0.0), 0, keepdims=True)
    slots = slots_f.astype(jnp.int32)
    events = per_batch // 2
    partners = jnp.concatenate(
        [
            slots[:, events : 2 * events],
            slots[:, :events],
            slots[:, 3 * events :],
            slots[:, 2 * events : 3 * events],
        ],
        1,
    )
    owner = slots // node_dev
    offset = slots - owner * node_dev
    owner_hot = jnp.where(iota((owners, letters), 0) == owner, 1.0, 0.0)
    earlier = jnp.where(
        iota((per_batch, per_batch), 0) < iota((per_batch, per_batch), 1), 1.0, 0.0
    ).astype(BF)
    hot_bf = owner_hot.astype(BF)
    before = jnp.concatenate(
        [dot(hot_bf[:, :per_batch], earlier), dot(hot_bf[:, per_batch:], earlier)], 1
    )
    rank = jnp.sum(before * owner_hot, 0, keepdims=True).astype(jnp.int32)
    batch = iota((1, letters), 1) // per_batch
    seat = owner * (2 * cap) + batch * cap + rank
    times = jnp.concatenate([time_ref[0:1], time_ref[0:1], time_ref[1:2], time_ref[1:2]], 1)
    values = jnp.concatenate(
        [
            offset >> 8, offset & 255, partners >> 8, partners & 255,
            times >> 8, times & 255, jnp.ones_like(times), jnp.zeros_like(times),
        ],
        0,
    ).astype(F32).astype(BF)
    for o in range(owners):
        seats = jnp.where(iota((2 * cap, letters), 0) + o * 2 * cap == seat, 1.0, 0.0).astype(BF)
        placed = dot_nt(values, seats)
        taken = placed[6:7] > 0.5
        rows = [
            jnp.where(taken, placed[0:1] * 256.0 + placed[1:2], float(node_dev)),
            placed[2:3] * 256.0 + placed[3:4],
            placed[4:5] * 256.0 + placed[5:6],
        ]
        lists_ref[o] = jnp.concatenate(rows + [jnp.zeros((5, 2 * cap), F32)], 0).astype(jnp.int32)


def make_codes(width, pad_ref, codes_ref):
    stamps = iota(codes_ref.shape, 0).astype(F32)
    lane = iota(codes_ref.shape, 1)
    code = jnp.cos(stamps * pad_ref[0:1] + pad_ref[1:2])
    code = jnp.where(lane < width, code, jnp.where(lane == width, 1.0, 0.0))
    codes_ref[...] = code.astype(BF)


def peer(index, reps):
    return (index // reps, lax.rem(index, reps))


BLOCKS = 6


class Gather:
    def __init__(self, owners, own_ref, table_ref, send_sem, recv_sem, local_sem):
        self.outer = owners // 2
        mem = lax.axis_index("mem")
        rep = lax.axis_index("rep")
        self.a, self.b = mem // 2, lax.rem(mem, 2)
        self.u, self.c = rep // 2, lax.rem(rep, 2)
        self.mem, self.rep = mem, rep
        self.own, self.table = own_ref, table_ref
        self.send_sem, self.recv_sem = send_sem, recv_sem
        self.local = pltpu.make_async_copy(own_ref, table_ref.at[mem], local_sem)
        self.sent = 0
        base = BLOCKS * self.c
        self.line_first = [base + 2 * self.u, base + 2 * self.u + 1, base + 4]
        self.pair_first = base + 5
        self.planes = [base + 2 * (1 - self.u), base + 2 * (1 - self.u) + 1]
        self.ahead = (jnp.minimum(mem + 2, owners - 1), rep)
        self.behind = (jnp.maximum(mem - 2, 0), rep)
        self.beside = (2 * self.a + 1 - self.b, rep)
        self.plane = (mem, 2 * (1 - self.u) + self.c)
        self.core = (mem, 2 * self.u + 1 - self.c)
        self.checks = []

    def push(self, shard, block, target, from_own=False, when=None):
        index = self.sent
        self.sent += 1
        src = self.own.at[block] if from_own else self.table.at[shard, block]

        def go():
            pltpu.make_async_remote_copy(
                src_ref=src,
                dst_ref=self.table.at[shard, block],
                send_sem=self.send_sem.at[index],
                recv_sem=self.recv_sem.at[shard, block],
                device_id=target,
                device_id_type=MESH_ID,
            ).start()

        self.guard(when, go)
        self.checks.append((index, when))

    def guard(self, when, go):
        if when is None:
            go()
        else:
            pl.when(when)(go)

    def arrived(self, shard, block):
        ref = self.table.at[shard, block]
        pltpu.make_async_copy(ref, ref, self.recv_sem.at[shard, block]).wait()

    def along(self, shard, block, from_own=False):
        self.push(shard, block, self.ahead, from_own, self.a < self.outer - 1)
        self.push(shard, block, self.behind, from_own, self.a > 0)

    def begin(self):
        self.local.start()
        self.push(self.mem, self.pair_first, self.beside, True)
        for block in self.line_first:
            self.along(self.mem, block, True)
            self.push(self.mem, block, self.beside, True)
        self.along(self.mem, self.pair_first, True)

    def shard(self, t, other):
        at = jnp.clip(self.a + t, 0, self.outer - 1)
        return 2 * at + (1 - self.b if other else self.b)

    def take(self, t, other, k):
        shard = self.shard(t, other)
        block = self.line_first[k] if k < 3 else self.pair_first
        onward = (t != 0) and not (other and k < 3)

        there = None
        if t < 0:
            there = self.a >= -t
        if t > 0:
            there = self.a < self.outer - t

        def also(extra):
            return extra if there is None else there & extra

        self.guard(there, lambda: self.arrived(shard, block))
        if t == 0 and k == 3:
            self.along(shard, block)
        if onward and t < 0:
            self.push(shard, block, self.ahead, when=also(self.a < self.outer - 1))
        if onward and t > 0:
            self.push(shard, block, self.behind, when=also(self.a > 0))
        if not other and k < 3:
            self.push(shard, block, self.beside, when=there)
        if k < 2:
            self.push(shard, block, self.plane, when=there)
        self.push(shard, block, self.core, when=there)

    def from_plane(self, t, other, k):
        shard, block = self.shard(t, other), self.planes[k]
        there = None
        if t < 0:
            there = self.a >= -t
        if t > 0:
            there = self.a < self.outer - t
        self.guard(there, lambda: self.arrived(shard, block))
        self.push(shard, block, self.core, when=there)

    def from_core(self, t, other):
        shard = self.shard(t, other)
        there = None
        if t < 0:
            there = self.a >= -t
        if t > 0:
            there = self.a < self.outer - t

        def go():
            for k in range(BLOCKS):
                self.arrived(shard, BLOCKS * (1 - self.c) + k)

        self.guard(there, go)

    def steps(self):
        far = self.outer - 1
        self.take(0, True, 3)
        for k in range(3):
            for t in (-1, 1):
                self.take(t, False, k)
            self.take(0, True, k)
            yield
        for t in range(1, far + 1):
            for k in range(3):
                for s in (-t, t):
                    self.take(s, True, k)
                    if t < far:
                        self.take(s + (1 if s > 0 else -1), False, k)
                yield
            for s in (-t, t):
                self.take(s, False, 3)
                self.take(s, True, 3)
            if t == 1:
                self.from_plane(0, True, 0)
                self.from_plane(0, True, 1)
            yield
            for s in (-t, t):
                for k in range(2):
                    self.from_plane(s, False, k)
                    self.from_plane(s, True, k)
            yield
        self.local.wait()
        self.from_core(0, True)
        for t in range(1, far + 1):
            for s in (-t, t):
                self.from_core(s, False)
                self.from_core(s, True)

    def finish(self):
        for index, when in self.checks:
            ref = self.own.at[0]
            copy = pltpu.make_async_copy(ref, ref, self.send_sem.at[index])
            self.guard(when, copy.wait)


def gather_sends(owners):
    outer = owners // 2
    return 12 + 16 * outer + 4 * BLOCKS * owners


class Exchange:
    def __init__(self, devices, reps, me, source, target, send_sem, recv_sem):
        self.devices, self.reps, self.me = devices, reps, me
        self.source, self.target = source, target
        self.send_sem, self.recv_sem = send_sem, recv_sem

    def copy(self, k):
        to = lax.rem(self.me + k, self.devices)
        return pltpu.make_async_remote_copy(
            src_ref=self.source(to),
            dst_ref=self.target(self.me),
            send_sem=self.send_sem.at[k],
            recv_sem=self.recv_sem.at[k],
            device_id=peer(to, self.reps),
            device_id_type=MESH_ID,
        )

    def start(self):
        def one(k, carry):
            self.copy(k).start()
            return carry

        lax.fori_loop(1, self.devices, one, 0)

    def wait_recv(self):
        def one(k, carry):
            come = lax.rem(self.me + self.devices - k, self.devices)
            ref = self.target(come)
            pltpu.make_async_copy(ref, ref, self.recv_sem.at[k]).wait()
            return carry

        lax.fori_loop(1, self.devices, one, 0)

    def wait_send(self):
        def one(k, carry):
            self.copy(k).wait_send()
            return carry

        lax.fori_loop(1, self.devices, one, 0)


def reduce_parts(devices, reps, me, grads_ref, parts_ref, sum_ref, total_ref, sems):
    scatter = Exchange(
        devices, reps, me, lambda to: grads_ref.at[to], lambda come: parts_ref.at[come],
        sems[0], sems[1],
    )
    share = Exchange(
        devices, reps, me, lambda to: sum_ref, lambda come: total_ref.at[come], sems[2], sems[3]
    )
    return scatter, share


def reduce_middle(me, grads_ref, parts_ref, sum_ref, total_ref):
    parts_ref[me] = grads_ref[me]
    total = jnp.sum(parts_ref[...].astype(F32), 0)
    sum_ref[...] = total
    total_ref[me] = total


def up8(n):
    return -(-n // 8) * 8


class Pack:
    def __init__(self, width, embed, devices):
        self.width, self.embed, self.devices = width, embed, devices
        self.high = up8(width - LANES)
        self.side = up8(embed)
        self.main = 16 * devices
        self.nbr = 2 * LANES
        self.top = 4 * LANES
        self.bottom = 5 * LANES
        self.vectors = 6 * LANES
        self.rows = 6 * LANES + 8
        self.at_top = 2 * LANES + 2 * self.high
        self.at_bottom = self.at_top + self.side
        self.extra = self.at_bottom + self.side - self.main
        self.spare = LANES - embed
        self.chunks = -(-embed // self.spare) if self.spare > 0 else 0

    def fits(self):
        return (
            self.spare > 0
            and 0 <= self.extra < self.side
            and self.chunks * (self.extra + 8) <= self.main
        )


def pack_params(pack, refs, out_ref):
    w_self, w_nbr, b_embed, w_dec1, b_dec1, w_dec2, b_dec2 = refs
    width, embed = pack.width, pack.embed
    out_ref[...] = jnp.zeros_like(out_ref)
    out_ref[0:width, 0:embed] = w_self[...]
    out_ref[pack.nbr : pack.nbr + width, 0:embed] = w_nbr[...]
    out_ref[pack.top : pack.top + embed, 0:embed] = w_dec1[0:embed, :]
    out_ref[pack.bottom : pack.bottom + embed, 0:embed] = w_dec1[embed : 2 * embed, :]
    v = pack.vectors
    out_ref[v : v + 1, 0:embed] = b_embed[...]
    out_ref[v + 1 : v + 2, 0:embed] = b_dec1[...]
    out_ref[v + 2 : v + 3, 0:embed] = w_dec2[...]
    out_ref[v + 3 : v + 4, 0:1] = b_dec2[...]


def pack_grads(pack, grads, small, table_ref, out_ref):
    s_lo, s_hi, n_lo, n_hi, top, bottom = grads
    high, side, extra = pack.high, pack.side, pack.extra
    table_ref[0:LANES] = s_lo
    table_ref[LANES : 2 * LANES] = n_lo
    table_ref[2 * LANES : 2 * LANES + high] = s_hi[:high]
    table_ref[2 * LANES + high : pack.at_top] = n_hi[:high]
    table_ref[pack.at_top : pack.at_bottom] = top[:side]
    table_ref[pack.at_bottom : pack.main] = bottom[: side - extra]
    coarse = small.astype(BF).astype(F32)
    pieces = [(0, bottom[side - extra : side])] if extra else []
    pieces.append((pack.chunks * extra, jnp.concatenate([coarse, small - coarse], 0)))
    for start, piece in pieces:
        size = piece.shape[0]
        lane = iota((size, LANES), 1)
        for k in range(pack.chunks):
            moved = pltpu.roll(piece, (pack.embed - k * pack.spare) % LANES, 1)
            rows = slice(start + k * size, start + (k + 1) * size)
            table_ref[rows] = jnp.where(lane >= pack.embed, moved, table_ref[rows])
    out_ref[...] = table_ref[...].reshape(out_ref.shape).astype(BF)


def update_params(pack, total_ref, old_ref, new_ref):
    high, side, extra = pack.high, pack.side, pack.extra
    table = total_ref[...].reshape(pack.main, LANES)

    def clean(x):
        return jnp.where(iota(x.shape, 1) < pack.embed, x, 0.0)

    def collect(start, size):
        out = jnp.zeros((size, LANES), F32)
        lane = iota((size, LANES), 1)
        for k in range(pack.chunks):
            part = table[start + k * size : start + (k + 1) * size]
            part = jnp.where(lane >= pack.embed, part, 0.0)
            out = out + pltpu.roll(part, (k * pack.spare - pack.embed) % LANES, 1)
        return out

    small = collect(pack.chunks * extra, 8)
    small = small[0:4] + small[4:8]
    lane4 = iota((4, LANES), 1)
    row4 = iota((4, LANES), 0)
    loss = jnp.sum(jnp.where((row4 == 3) & (lane4 == 1), small, 0.0))
    count = jnp.sum(jnp.where((row4 == 3) & (lane4 == 2), small, 0.0))
    small = jnp.where((row4 < 3) | (lane4 == 0), small, 0.0)
    parts = [
        (0, clean(table[0:LANES])),
        (LANES, clean(table[2 * LANES : 2 * LANES + high])),
        (pack.nbr, clean(table[LANES : 2 * LANES])),
        (pack.nbr + LANES, clean(table[2 * LANES + high : pack.at_top])),
        (pack.top, clean(table[pack.at_top : pack.at_bottom])),
        (pack.bottom, clean(table[pack.at_bottom : pack.main])),
    ]
    if extra:
        parts.append((pack.bottom + side - extra, collect(0, extra)))
    total = jnp.sum(small * small)
    for _, part in parts:
        total = total + jnp.sum(part * part)
    total = jnp.zeros((1, LANES), F32) + total
    factor = step_size / (jnp.sqrt(total) + 1e-06)
    new_ref[...] = old_ref[...]
    for start, part in parts:
        rows = slice(start, start + part.shape[0])
        new_ref[rows] = old_ref[rows] - factor * part
    rows = slice(pack.vectors, pack.vectors + 4)
    new_ref[rows] = old_ref[rows] - factor * small
    return loss / jnp.maximum(jnp.zeros((1, LANES), F32) + count, 1.0)


def unpack_params(pack, packed_ref, refs):
    w_self, w_nbr, b_embed, w_dec1, b_dec1, w_dec2, b_dec2 = refs
    width, embed = pack.width, pack.embed
    w_self[...] = packed_ref[0:width, 0:embed]
    w_nbr[...] = packed_ref[pack.nbr : pack.nbr + width, 0:embed]
    w_dec1[0:embed, :] = packed_ref[pack.top : pack.top + embed, 0:embed]
    w_dec1[embed : 2 * embed, :] = packed_ref[pack.bottom : pack.bottom + embed, 0:embed]
    v = pack.vectors
    b_embed[...] = packed_ref[v : v + 1, 0:embed]
    b_dec1[...] = packed_ref[v + 1 : v + 2, 0:embed]
    w_dec2[...] = packed_ref[v + 2 : v + 3, 0:embed]
    b_dec2[...] = packed_ref[v + 3 : v + 4, 0:1]


def expand(table_ref, low_ref, high_ref, shard, quarter):
    base = shard * 4 * quarter
    lane = iota((quarter, LANES), 1)
    for c in range(2):
        at = pl.multiple_of(base + 2 * c * quarter, quarter)
        low = table_ref[shard, BLOCKS * c : BLOCKS * c + 4].astype(F32)
        low_ref[pl.ds(at, 2 * quarter), :] = low.reshape(2 * quarter, LANES)
        both = table_ref[shard, BLOCKS * c + 4 : BLOCKS * c + 6].astype(F32).reshape(quarter, LANES)
        at = pl.multiple_of(base + 2 * c * quarter, quarter)
        high_ref[pl.ds(at, quarter), :] = jnp.where(lane < LANES // 2, both, 0.0)
        at = pl.multiple_of(base + (2 * c + 1) * quarter, quarter)
        high_ref[pl.ds(at, quarter), :] = jnp.where(
            lane < LANES // 2, pltpu.roll(both, LANES // 2, 1), 0.0
        )


def partner_rows(batch, cap, lists_smem, low_ref, high_ref, out_low, out_high):
    slots = low_ref.shape[0]

    def one(d, carry):
        for j in range(cap):
            p = lists_smem[d, 1, batch * cap + j]
            p = p & (slots - 1) if slots & (slots - 1) == 0 else jnp.clip(p, 0, slots - 1)
            at = d * cap + j
            out_low[pl.ds(at, 1), :] = low_ref[pl.ds(p, 1), :]
            out_high[pl.ds(at, 1), :] = high_ref[pl.ds(p, 1), :]
        return carry

    lax.fori_loop(0, lists_smem.shape[0], one, 0)


def event_rows(batch, first, count, nodes_smem, slot_smem, low_ref, high_ref, own_low, own_high, nbr_low, nbr_high):
    neighbours = (nodes_smem.shape[0] - 3) // 3
    events = nodes_smem.shape[2]

    def one(e, carry):
        def row(col):
            slot = slot_smem[nodes_smem[col, batch, e]]
            return low_ref[pl.ds(slot, 1), :], high_ref[pl.ds(slot, 1), :]

        for r in range(3):
            at = pl.ds(r * events + e, 1)
            low, high = row(r)
            own_low[at, :] = low
            own_high[at, :] = high
            low, high = row(3 + r * neighbours)
            for k in range(1, neighbours):
                more, rest = row(3 + r * neighbours + k)
                low, high = low + more, high + rest
            nbr_low[at, :] = low
            nbr_high[at, :] = high
        return carry

    lax.fori_loop(first, first + count, one, 0)


def pair_row(batch, cap, lists_ref, i, row):
    first, second = lists_ref[2 * i], lists_ref[2 * i + 1]
    lane = iota(first.shape, 1)
    if batch == 0:
        both = jnp.where(lane < cap, first, pltpu.roll(second, cap, 1))
    else:
        both = jnp.where(lane < cap, pltpu.roll(first, cap, 1), second)
    return both[row : row + 1]


def letter_codes(batch, cap, lists_ref, codes_ref, letters_ref):
    times = codes_ref.shape[0]
    codes = codes_ref[...]
    for i in range(lists_ref.shape[0] // 2):
        stamp = pair_row(batch, cap, lists_ref, i, 2)
        hot = jnp.where(iota((times, LANES), 0) == stamp, 1.0, 0.0).astype(BF)
        letters_ref[i * LANES : (i + 1) * LANES, 2 * LANES :] = dot_tn(hot, codes).astype(BF)


def split2(x):
    coarse = x.astype(BF)
    return coarse, (x - coarse.astype(F32)).astype(BF)


def memory_step(batch, cap, width, code, lists_ref, letters_ref, memory_ref, gi_ref, gh_ref, bias_ref, hot_ref, out_ref, blocks_ref):
    slots = memory_ref.shape[0]
    quarter = slots // 4
    pairs = lists_ref.shape[0] // 2
    lane = iota((quarter, LANES), 1)
    rest = width - LANES
    held = None
    for q in range(4):
        rows = slice(q * quarter, (q + 1) * quarter)
        for i in range(pairs):
            target = pair_row(batch, cap, lists_ref, i, 0)
            hot = jnp.where(iota((quarter, LANES), 0) + q * quarter == target, 1.0, 0.0)
            hot_ref[:, i * LANES : (i + 1) * LANES] = hot.astype(BF)
        summed = dot(hot_ref[...], letters_ref[...])
        counts = jnp.sum(
            jnp.where(lane == code, summed[:, 2 * LANES :], 0.0), 1, keepdims=True
        )
        mean = (summed / jnp.maximum(counts, 1.0)).astype(BF)
        low = memory_ref[rows, 0:LANES]
        high = memory_ref[rows, LANES : 2 * LANES]
        old = jnp.concatenate([low, high], 1)
        state = old.astype(BF)
        joined = jnp.concatenate([state, mean], 1)
        inner = [dot(joined, gi_ref[j]) + bias_ref[j : j + 1] for j in range(3)]
        outer = [dot(state, gh_ref[j]) + bias_ref[j + 3 : j + 4] for j in range(3)]
        reset = jax.nn.sigmoid(inner[0] + outer[0])
        update = jax.nn.sigmoid(inner[1] + outer[1])
        candidate = jnp.tanh(inner[2] + reset * outer[2])
        fresh = (1.0 - update) * candidate + update * old
        new = jnp.where(counts > 0.5, fresh, old)
        new_low, new_high = new[:, :LANES], new[:, LANES:]
        if blocks_ref is None:
            out_ref[0:LANES, rows] = new_low.T
            out_ref[LANES:width, rows] = new_high.T[:rest]
        else:
            out_ref[rows, 0:LANES] = new_low
            out_ref[rows, LANES : 2 * LANES] = new_high
            c, u = q // 2, q % 2
            at = BLOCKS * c + 2 * u
            blocks_ref[at : at + 2] = new_low.astype(BF).reshape(2, quarter // 2, LANES)
            masked = jnp.where(lane < rest, new_high, 0.0)
            if u == 0:
                held = masked
            else:
                both = (held + pltpu.roll(masked, LANES // 2, 1)).astype(BF)
                blocks_ref[BLOCKS * c + 4 : BLOCKS * c + 6] = both.reshape(2, quarter // 2, LANES)


def loss_step(pack, batch, neighbours, params_ref, valid_ref, own_low, own_high, nbr_low, nbr_high, table_ref, out_ref):
    events = valid_ref.shape[1]
    v = pack.vectors

    def weight(start):
        return params_ref[start : start + LANES].astype(BF)

    b_embed = params_ref[v : v + 1]
    yield
    b_dec1 = params_ref[v + 1 : v + 2]
    w_dec2 = params_ref[v + 2 : v + 3]
    b_dec2 = jnp.sum(params_ref[v + 3 : v + 4])
    x_low, x_high = own_low[...].astype(BF), own_high[...].astype(BF)
    n_low, n_high = split2(nbr_low[...]), split2(nbr_high[...])
    direct = dot(x_low, weight(0)) + dot(x_high, weight(LANES))
    w_low, w_high = weight(pack.nbr), weight(pack.nbr + LANES)
    spread = (
        dot(n_low[0], w_low) + dot(n_low[1], w_low) + dot(n_high[0], w_high) + dot(n_high[1], w_high)
    )
    act = jnp.tanh(direct + spread * (1.0 / neighbours) + b_embed)
    hidden = act.astype(BF)
    yield
    h0, h1, h2 = (hidden[r * events : (r + 1) * events] for r in range(3))
    top, bottom = weight(pack.top), weight(pack.bottom)
    shared = dot(h0, top)
    pre = [shared + dot(h, bottom) + b_dec1 for h in (h1, h2)]
    eye = iota((events, events), 0) == iota((events, events), 1)
    valid = jnp.where(eye, valid_ref[batch : batch + 1].astype(F32), 0.0)
    valid = jnp.sum(valid, 1, keepdims=True)
    loss = jnp.zeros((1, 1), F32)
    d_pre, g_dec2, g_out = [], jnp.zeros((1, LANES), F32), jnp.zeros((1, 1), F32)
    for z, sign in zip(pre, (-1.0, 1.0)):
        inner = jnp.maximum(z, 0.0)
        logit = (jnp.sum(inner * w_dec2, 1, keepdims=True) + b_dec2) * sign
        soft = jnp.maximum(logit, 0.0) + jnp.log1p(jnp.exp(-jnp.abs(logit)))
        loss = loss + jnp.sum(soft * valid, 0, keepdims=True)
        d_logit = jax.nn.sigmoid(logit) * valid * sign
        g_dec2 = g_dec2 + jnp.sum(d_logit * inner, 0, keepdims=True)
        g_out = g_out + jnp.sum(d_logit, 0, keepdims=True)
        d_pre.append(jnp.where(z > 0.0, d_logit * w_dec2, 0.0))
    yield
    g_dec1 = jnp.sum(d_pre[0] + d_pre[1], 0, keepdims=True)
    both = split2(d_pre[0] + d_pre[1])
    parts = [split2(d) for d in d_pre]
    g_top = dot_tn(h0, both[0]) + dot_tn(h0, both[1])
    g_bottom = (
        dot_tn(h1, parts[0][0]) + dot_tn(h1, parts[0][1])
        + dot_tn(h2, parts[1][0]) + dot_tn(h2, parts[1][1])
    )
    yield
    back = []
    for w in (top, bottom):
        back.append([(dot_nt(p[0], w) + dot_nt(p[1], w)).astype(BF) for p in parts])
    d0 = (back[0][0].astype(F32) + back[0][1].astype(F32)).astype(BF)
    d_hidden = jnp.concatenate([d0, back[1][0], back[1][1]], 0).astype(F32)
    d_act = d_hidden * (1.0 - act * act)
    g_embed = jnp.sum(d_act, 0, keepdims=True)
    d_own = split2(d_act)
    d_nbr = split2(d_act * (1.0 / neighbours))
    yield
    g_s = [dot_tn(x, d_own[0]) + dot_tn(x, d_own[1]) for x in (x_low, x_high)]
    yield
    g_n = [
        dot_tn(n[0], d_nbr[0]) + dot_tn(n[0], d_nbr[1]) + dot_tn(n[1], d_nbr[0])
        for n in (n_low, n_high)
    ]
    yield
    count = jnp.sum(valid, 0, keepdims=True)
    lane = iota((1, LANES), 1)
    scalars = jnp.where(lane == 0, g_out, jnp.where(lane == 1, loss, jnp.where(lane == 2, count, 0.0)))
    small = jnp.concatenate([g_embed, g_dec1, g_dec2, scalars], 0)
    pack_grads(pack, (g_s[0], g_s[1], g_n[0], g_n[1], g_top, g_bottom), small, table_ref, out_ref)


def turn_memory(turned_ref, memory_ref, blocks_ref):
    width, node_dev = turned_ref.shape
    quarter = node_dev // 4
    rest = width - LANES
    held = None
    for q in range(4):
        rows = slice(q * quarter, (q + 1) * quarter)
        c, u = q // 2, q % 2
        low = turned_ref[0:LANES, rows].T
        memory_ref[rows, 0:LANES] = low
        at = BLOCKS * c + 2 * u
        blocks_ref[at : at + 2] = low.astype(BF).reshape(2, quarter // 2, LANES)
        pad = jnp.zeros((LANES - up8(rest), quarter), F32)
        high = turned_ref[LANES:width, rows]
        if up8(rest) != rest:
            high = jnp.concatenate([high, jnp.zeros((up8(rest) - rest, quarter), F32)], 0)
        high = jnp.concatenate([high, pad], 0).T
        memory_ref[rows, LANES : 2 * LANES] = high
        if u == 0:
            held = high
        else:
            both = (held + pltpu.roll(high, LANES // 2, 1)).astype(BF)
            blocks_ref[BLOCKS * c + 4 : BLOCKS * c + 6] = both.reshape(2, quarter // 2, LANES)


def pack_turned(width, source_ref, spans, wide_ref, out_ref):
    rows, columns = source_ref.shape
    wide_ref[...] = jnp.zeros_like(wide_ref)
    wide_ref[0:rows, 0:columns] = source_ref[...].astype(F32)
    total = wide_ref.shape[1]
    keep = 2 * LANES
    for j in range(3):
        part = wide_ref[j * width : j * width + keep, :]
        for start, size, to in spans:
            span = -(-size // LANES) * LANES
            moved = part if start == 0 else pltpu.roll(part, total - start, 1)
            moved = moved[:, :span]
            inside = (iota(moved.shape, 1) < size) & (iota(moved.shape, 0) < width)
            out_ref[j, to : to + span, :] = jnp.where(inside, moved, 0.0).T.astype(BF)


def pack_gates(width, source_ref, spans, wide_ref, out_ref):
    rows, columns = source_ref.shape
    wide_ref[...] = jnp.zeros_like(wide_ref)
    wide_ref[0:rows, 0:columns] = source_ref[...].astype(F32)
    total = wide_ref.shape[1]
    out_ref[...] = jnp.zeros_like(out_ref)
    for start, size, to in spans:
        part = wide_ref[start : start + size, :]
        for j in range(3):
            moved = part if j == 0 else pltpu.roll(part, total - j * width, 1)
            moved = moved[:, : 2 * LANES]
            moved = jnp.where(iota(moved.shape, 1) < width, moved, 0.0)
            out_ref[j, to : to + size, :] = moved.astype(BF)


def pack_bias(width, in_ref, hid_ref, wide_ref, out_ref):
    total = wide_ref.shape[1]
    columns = in_ref.shape[0]
    wide_ref[0:8, :] = jnp.zeros((8, total), F32)
    wide_ref[0:1, 0:columns] = in_ref[...].reshape(1, columns)
    wide_ref[1:2, 0:columns] = hid_ref[...].reshape(1, columns)
    part = wide_ref[0:8, :]
    for j in range(3):
        moved = part if j == 0 else pltpu.roll(part, total - j * width, 1)
        moved = jnp.where(iota((8, 2 * LANES), 1) < width, moved[:, : 2 * LANES], 0.0)
        out_ref[j : j + 1] = moved[0:1]
        out_ref[j + 3 : j + 4] = moved[1:2]


def window_kernel(owners, reps, cap, code, pack, *refs):
    (
        nodes_smem, slot_smem, nodes_ref, slot_ref, time_ref, valid_ref, freq_ref, phase_ref,
        turned_ref, gru_in_ref, gru_hid_ref, in_bias_ref, hid_bias_ref,
    ) = refs[:13]
    params = refs[13:20]
    memory_out, loss_ref, packed_out = refs[20:23]
    (
        memory_ref, blocks, table, low, high, p_low, p_high, letters, hot, own_low, own_high, nbr_low, nbr_high,
        flat, middle, lists_ref, all_lists, lists_smem, codes, packed, gi, gh, bias, wide, pad_ref,
        grads, parts, sums, totals,
        send_sems, recv_sems, local_sem, list_sems, reduce_sems,
    ) = refs[23:]
    me = lax.axis_index("mem") * reps + lax.axis_index("rep")
    devices = owners * reps
    width, node_dev = turned_ref.shape
    quarter = node_dev // 4
    columns, _, events = nodes_ref.shape
    neighbours = (columns - 3) // 3

    barrier = pltpu.get_barrier_semaphore()

    def greet(k, carry):
        pl.semaphore_signal(
            barrier, inc=1, device_id=peer(lax.rem(me + k, devices), reps), device_id_type=MESH_ID
        )
        return carry

    lax.fori_loop(1, devices, greet, 0)
    turn_memory(turned_ref, memory_ref, blocks.at[0])
    make_lists(owners, node_dev, cap, slot_ref, nodes_ref, time_ref, lists_ref)
    pack_bias(width, in_bias_ref, hid_bias_ref, wide, bias)
    pack_params(pack, params, packed.at[0])
    pack_gates(width, gru_hid_ref, [(0, width, 0)], wide, gh)
    pl.semaphore_wait(barrier, devices - 1)

    gathers = [
        Gather(owners, blocks.at[b], table.at[b], send_sems.at[b], recv_sems.at[b], local_sem.at[b])
        for b in range(2)
    ]
    exchange = Exchange(
        devices, reps, me,
        lambda to: lists_ref.at[to // reps], lambda come: all_lists.at[come],
        list_sems.at[0], list_sems.at[1],
    )
    mine = pltpu.make_async_copy(
        lists_ref.at[lax.axis_index("mem")], all_lists.at[me], local_sem.at[2]
    )
    to_smem = pltpu.make_async_copy(all_lists, lists_smem, local_sem.at[3])
    reduces = [
        reduce_parts(
            devices, reps, me, grads.at[b], parts.at[b], sums.at[b], totals.at[b],
            [reduce_sems.at[4 * b + i] for i in range(4)],
        )
        for b in range(2)
    ]

    gathers[0].begin()
    exchange.start()
    mine.start()

    def time_table():
        pad_ref[...] = jnp.zeros_like(pad_ref)
        pad_ref[0:1, 0:code] = freq_ref[...]
        pad_ref[1:2, 0:code] = phase_ref[...]
        make_codes(code, pad_ref, codes)

    def lists_in():
        exchange.wait_recv()
        mine.wait()
        to_smem.start()

    def codes_of(batch):
        return lambda: letter_codes(batch, cap, all_lists, codes, letters.at[batch])

    shadow = [
        lambda: pack_turned(
            width, gru_in_ref,
            [(0, width, 0), (width, width, 2 * LANES), (2 * width, code, 4 * LANES)],
            wide, gi,
        ),
        time_table,
        lists_in,
        codes_of(0),
        codes_of(1),
    ]
    for _ in gathers[0].steps():
        if shadow:
            shadow.pop(0)()
    for task in shadow:
        task()
    to_smem.wait()

    def spread(b):
        def one(s, carry):
            expand(table.at[b], low, high, s, quarter)
            return carry

        lax.fori_loop(0, owners, one, 0)

    def partners(b):
        partner_rows(b, cap, lists_smem, low, high, p_low, p_high)
        letters[b, :, 0:LANES] = p_low[...].astype(BF)
        letters[b, :, LANES : 2 * LANES] = p_high[...].astype(BF)

    def remember(b, old_ref, new_ref, blocks_ref):
        memory_step(
            b, cap, width, code, all_lists, letters.at[b], old_ref, gi, gh, bias, hot, new_ref, blocks_ref
        )

    def rows_of(b, first, count):
        event_rows(
            b, first, count, nodes_smem, slot_smem, low, high, own_low, own_high, nbr_low, nbr_high
        )

    def loss_of(b):
        return loss_step(
            pack, b, neighbours, packed.at[b], valid_ref, own_low, own_high, nbr_low, nbr_high, flat,
            grads.at[b],
        )

    spread(0)
    partners(0)
    remember(0, memory_ref, middle, blocks.at[1])
    gathers[1].begin()
    pieces = 16
    size = events // pieces
    tasks = [functools.partial(rows_of, 0, i * size, size) for i in range(pieces)]

    def send_grads():
        for _ in loss_of(0):
            pass
        reduces[0][0].start()

    tasks.append(send_grads)
    for _ in gathers[1].steps():
        if tasks:
            tasks.pop(0)()
    for task in tasks:
        task()
    spread(1)
    rows_of(1, 0, events // 2)
    reduces[0][0].wait_recv()
    reduce_middle(me, grads.at[0], parts.at[0], sums.at[0], totals.at[0])
    reduces[0][1].start()
    rows_of(1, events // 2, events // 2)
    partners(1)
    reduces[0][1].wait_recv()
    loss0 = update_params(pack, totals.at[0], packed.at[0], packed.at[1])
    for _ in loss_of(1):
        pass
    reduces[1][0].start()
    reduces[1][0].wait_recv()
    reduce_middle(me, grads.at[1], parts.at[1], sums.at[1], totals.at[1])
    reduces[1][1].start()
    remember(1, middle, memory_out, None)
    reduces[1][1].wait_recv()
    loss1 = update_params(pack, totals.at[1], packed.at[1], packed_out)
    loss_ref[...] = jnp.where(iota((1, LANES), 1) == 0, loss0, loss1)

    exchange.wait_send()
    for scatter, share in reduces:
        scatter.wait_send()
        share.wait_send()
    for gather in gathers:
        gather.finish()


def final_kernel(pack, memory_ref, loss_ref, packed_ref, memory_out, loss_out, *outs):
    memory_out[...] = memory_ref[...]
    loss_out[...] = loss_ref[0, 0:2]
    unpack_params(pack, packed_ref, outs)


def quick_body(owners, reps, cap, memory, node_slot, event_nodes, event_times, valid_mask, time_freq, time_phase, gru_input, gru_hidden, gru_in_bias, gru_hid_bias, *params):
    node_dev, width = memory.shape
    batches, events, columns = event_nodes.shape
    code = time_freq.shape[0]
    devices = owners * reps
    pack = Pack(width, params[0].shape[1], devices)
    quarter = node_dev // 4
    slots = node_slot.shape[0]
    letters = devices * cap
    sends = gather_sends(owners)
    stamps = -(-TIMES // LANES) * LANES
    wide_rows = up8(2 * width + 2 * LANES)
    wide_lanes = -(-3 * width // LANES) * LANES + LANES
    sds = jax.ShapeDtypeStruct
    dma = pltpu.SemaphoreType.DMA
    rows = [p[None, :] if p.ndim == 1 else p for p in params]
    smem = [pl.BlockSpec(memory_space=pltpu.SMEM)]
    nodes = event_nodes.transpose(2, 0, 1)
    made = pl.pallas_call(
        functools.partial(window_kernel, owners, reps, cap, code, pack),
        out_shape=(sds((width, node_dev), F32), sds((1, LANES), F32), sds((pack.rows, LANES), F32)),
        in_specs=smem * 2 + vmem(18),
        out_specs=tuple(vmem(3)),
        scratch_shapes=[
            pltpu.VMEM((node_dev, 2 * LANES), F32),
            pltpu.VMEM((2, 2 * BLOCKS, quarter // 2, LANES), BF),
            pltpu.VMEM((2, owners, 2 * BLOCKS, quarter // 2, LANES), BF),
            pltpu.VMEM((slots, LANES), F32),
            pltpu.VMEM((slots, LANES), F32),
            pltpu.VMEM((letters, LANES), F32),
            pltpu.VMEM((letters, LANES), F32),
            pltpu.VMEM((2, letters, 3 * LANES), BF),
            pltpu.VMEM((quarter, letters), BF),
            pltpu.VMEM((3 * events, LANES), F32),
            pltpu.VMEM((3 * events, LANES), F32),
            pltpu.VMEM((3 * events, LANES), F32),
            pltpu.VMEM((3 * events, LANES), F32),
            pltpu.VMEM((pack.main, LANES), F32),
            pltpu.VMEM((node_dev, 2 * LANES), F32),
            pltpu.VMEM((owners, 8, 2 * cap), jnp.int32),
            pltpu.VMEM((devices, 8, 2 * cap), jnp.int32),
            pltpu.SMEM((devices, 8, 2 * cap), jnp.int32),
            pltpu.VMEM((stamps, LANES), BF),
            pltpu.VMEM((2, pack.rows, LANES), F32),
            pltpu.VMEM((3, 5 * LANES, 2 * LANES), BF),
            pltpu.VMEM((3, 2 * LANES, 2 * LANES), BF),
            pltpu.VMEM((8, 2 * LANES), F32),
            pltpu.VMEM((wide_rows, wide_lanes), F32),
            pltpu.VMEM((8, LANES), F32),
            pltpu.VMEM((2, devices, 16, LANES), BF),
            pltpu.VMEM((2, devices, 16, LANES), BF),
            pltpu.VMEM((2, 16, LANES), F32),
            pltpu.VMEM((2, devices, 16, LANES), F32),
            dma((2, sends)),
            dma((2, owners, 2 * BLOCKS)),
            dma((4,)),
            dma((2, devices)),
            dma((8, devices)),
        ],
        compiler_params=pltpu.CompilerParams(
            collective_id=0, has_side_effects=True, vmem_limit_bytes=56 * 1024 * 1024
        ),
        name="window",
    )(
        nodes, node_slot, nodes, node_slot.reshape(-1, LANES), event_times, valid_mask,
        time_freq[None, :], time_phase[None, :], memory.T, gru_input.T, gru_hidden,
        gru_in_bias, gru_hid_bias, *rows,
    )
    outs = pl.pallas_call(
        functools.partial(final_kernel, pack),
        out_shape=(sds((width, node_dev), F32), sds((batches,), F32))
        + tuple(sds(p.shape, F32) for p in rows),
        in_specs=vmem(3),
        out_specs=tuple(vmem(9)),
        name="final",
    )(*made)
    new = [o.reshape(p.shape) for o, p in zip(outs[2:], params)]
    return (outs[0].T, outs[1], *new)


def block_loss(current, own_rows, beside_sum, neighbours, valid_part):
    w_self, w_nbr, b_embed, w_dec1, b_dec1, w_dec2, b_dec2 = current
    num_events = own_rows.shape[0] // 3
    direct = jnp.dot(own_rows, w_self.astype(jnp.bfloat16), preferred_element_type=jnp.float32)
    spread = jnp.dot(
        beside_sum,
        w_nbr.astype(jnp.bfloat16).astype(jnp.float32),
        precision=lax.Precision.HIGHEST,
    )
    hidden = jnp.tanh(direct + spread * (1.0 / neighbours) + b_embed).astype(jnp.bfloat16)
    first = hidden[:num_events]
    paired = jnp.concatenate(
        [jnp.concatenate([first, first], 0), hidden[num_events:]],
        1,
    )
    inner_act = jax.nn.relu(
        jnp.dot(paired, w_dec1.astype(jnp.bfloat16), preferred_element_type=jnp.float32) + b_dec1
    )
    logits = jnp.sum(inner_act * w_dec2, 1) + b_dec2[0]
    weights = valid_part.astype(jnp.float32)
    sign_flip = jnp.concatenate(
        [-jnp.ones((num_events,), jnp.float32), jnp.ones((num_events,), jnp.float32)]
    )
    return jnp.sum(jax.nn.softplus(sign_flip * logits) * jnp.concatenate([weights, weights]))


def normalized_step(params, gradients):
    total = jnp.zeros((), jnp.float32)
    for grad_part in gradients:
        total = total + jnp.sum(grad_part * grad_part)
    factor = step_size / (jnp.sqrt(total) + 1e-06)
    return tuple((value - factor * grad_part for value, grad_part in zip(params, gradients)))


def memory_update(
    mean_rest, state_bf, old_state, gru_input, gru_hidden, gru_in_bias, gru_hid_bias
):
    row_width = old_state.shape[1]
    from_input = (
        jnp.dot(state_bf, gru_input[:row_width], preferred_element_type=jnp.float32)
        + jnp.dot(mean_rest, gru_input[row_width:], preferred_element_type=jnp.float32)
        + gru_in_bias
    )
    from_state = jnp.dot(state_bf, gru_hidden, preferred_element_type=jnp.float32) + gru_hid_bias
    reset = jax.nn.sigmoid(from_input[:, :row_width] + from_state[:, :row_width])
    update = jax.nn.sigmoid(
        from_input[:, row_width : 2 * row_width] + from_state[:, row_width : 2 * row_width]
    )
    candidate = jnp.tanh(from_input[:, 2 * row_width :] + reset * from_state[:, 2 * row_width :])
    return (1.0 - update) * candidate + update * old_state


def look_up(table, ids):
    width = 128
    groups = table.shape[0] // width
    grid = table.reshape(groups, width)
    digits = jnp.concatenate([grid >> 8, grid & 255], 1).astype(jnp.bfloat16)
    pick = ((ids // width)[..., None] == jnp.arange(groups, dtype=jnp.int32)).astype(jnp.bfloat16)
    rows = jnp.dot(pick, digits, preferred_element_type=jnp.float32)
    here = (ids % width)[..., None] == jnp.arange(width, dtype=jnp.int32)
    both = jnp.where(here, rows[..., :width] * 256.0 + rows[..., width:], 0.0)
    return jnp.sum(both, -1).astype(jnp.int32)


def sum_everywhere(gradients, loss_local, count_local, devices):
    g_self, g_nbr, g_embed, g_dec1, g_bias1, g_dec2, g_bias2 = gradients
    width = g_self.shape[1]
    scalars = jnp.concatenate([g_bias2, loss_local[None], count_local[None]])
    scalars = jnp.pad(scalars, (0, width - scalars.shape[0]))
    table = jnp.concatenate(
        [g_self, g_nbr, g_dec1, jnp.stack([g_embed, g_bias1, g_dec2, scalars])], 0
    )
    used = table.shape[0]
    share = -(-used // (devices * 8)) * 8
    table = jnp.pad(table, ((0, share * devices - used), (0, 0))).reshape(devices, share, width)
    parts = lax.all_to_all(table, ("mem", "rep"), split_axis=0, concat_axis=0, tiled=True)
    total = lax.all_gather(jnp.sum(parts, 0), ("mem", "rep"), axis=0, tiled=True)
    n_self, n_nbr, n_dec1 = g_self.shape[0], g_nbr.shape[0], g_dec1.shape[0]
    at = n_self + n_nbr + n_dec1
    return (
        (
            total[:n_self],
            total[n_self : n_self + n_nbr],
            total[at],
            total[n_self + n_nbr : at],
            total[at + 1],
            total[at + 2],
            total[at + 3, :1],
        ),
        total[at + 3, 1],
        total[at + 3, 2],
    )


def place_rows(owner_ids, owners, stride, offset):
    length = owner_ids.shape[0]
    width = 128
    groups = -(-length // width)
    padded_ids = owner_ids.reshape(groups, width)
    one_hot = (padded_ids[:, :, None] == jnp.arange(owners, dtype=jnp.int32)[None, None, :]).astype(
        jnp.float32
    )
    lower = (
        jnp.arange(width, dtype=jnp.int32)[:, None] > jnp.arange(width, dtype=jnp.int32)[None, :]
    ).astype(jnp.float32)
    within = jnp.einsum("ij,gjo->gio", lower, one_hot, precision=lax.Precision.HIGHEST)
    totals = jnp.sum(one_hot, 1)
    starts = jnp.cumsum(totals, 0) - totals
    before = jnp.sum((within + starts[:, None, :]) * one_hot, 2).reshape(-1)
    return owner_ids * stride + offset + before.astype(jnp.int32)


def body(
    memory,
    node_slot,
    event_nodes,
    event_times,
    valid_mask,
    time_freq,
    time_phase,
    gru_input,
    gru_hidden,
    gru_in_bias,
    gru_hid_bias,
    w_self,
    w_nbr,
    b_embed,
    w_dec1,
    b_dec1,
    w_dec2,
    b_dec2,
):
    owners = lax.axis_size("mem")
    devices = owners * lax.axis_size("rep")
    node_dev, row_width = memory.shape
    batches, events, columns = event_nodes.shape
    neighbours = (columns - 3) // 3
    cap_pair = 2 * events // owners * 2
    params = (w_self, w_nbr, b_embed, w_dec1, b_dec1, w_dec2, b_dec2)
    losses = []
    all_slots = look_up(node_slot, event_nodes.transpose(0, 2, 1))
    for batch_index in range(batches):
        slot_ids = all_slots[batch_index]
        memory_bf = memory.astype(jnp.bfloat16)
        whole_bf = lax.all_gather(memory_bf, "mem", axis=0, tiled=True)
        fetched = jnp.take(whole_bf, slot_ids.reshape(-1), axis=0, mode="clip")
        own_rows = fetched[: 3 * events]
        beside = fetched[3 * events :].reshape(3, neighbours, events, row_width)
        beside_sum = jnp.sum(beside.astype(jnp.float32), 1).reshape(3 * events, row_width)

        pair_slots = slot_ids[:2].reshape(-1)
        pair_at = place_rows(pair_slots // node_dev, owners, cap_pair, 0)
        offsets = (pair_slots % node_dev).astype(jnp.int32)
        time_code = jnp.cos(
            event_times[batch_index].astype(jnp.float32)[:, None] * time_freq + time_phase
        ).astype(jnp.bfloat16)
        marks = jnp.stack([jnp.ones_like(offsets), offsets // 128, offsets % 128], 1)
        partners = jnp.concatenate([own_rows[events : 2 * events], own_rows[:events]], 0)
        letters = jnp.concatenate(
            [partners, jnp.concatenate([time_code, time_code], 0), marks.astype(jnp.bfloat16)], 1
        )
        seats = jnp.arange(owners * cap_pair, dtype=jnp.int32)[:, None] == pair_at[None, :]
        parcel = jnp.dot(
            seats.astype(jnp.bfloat16), letters, preferred_element_type=jnp.float32
        ).astype(jnp.bfloat16)
        parcel = parcel.reshape(owners, cap_pair, letters.shape[1])
        parcel = lax.all_to_all(parcel, "mem", split_axis=0, concat_axis=0, tiled=True)
        every_parcel = lax.all_gather(parcel, "rep", axis=0, tiled=True)
        every_parcel = every_parcel.reshape(-1, letters.shape[1])
        digits = every_parcel[:, -2:].astype(jnp.int32)
        target = digits[:, 0] * 128 + digits[:, 1]
        matches = jnp.arange(node_dev, dtype=jnp.int32)[:, None] == target[None, :]
        summed = jnp.dot(
            matches.astype(jnp.bfloat16), every_parcel, preferred_element_type=jnp.float32
        )
        counts = summed[:, -3:-2]
        mean_rest = (summed[:, :-3] / jnp.maximum(counts, 1.0)).astype(jnp.bfloat16)
        fresh = memory_update(
            mean_rest, memory_bf, memory, gru_input, gru_hidden, gru_in_bias, gru_hid_bias
        )
        memory = jnp.where(counts > 0, fresh, memory)

        valid_part = valid_mask[batch_index]
        loss_local, pullback = jax.vjp(
            lambda current: block_loss(current, own_rows, beside_sum, neighbours, valid_part),
            params,
        )
        gradients = pullback(jnp.ones_like(loss_local))[0]
        count_local = jnp.sum(valid_part.astype(jnp.float32))
        gradients, loss_total, count_total = sum_everywhere(
            gradients, loss_local, count_local, devices
        )
        params = normalized_step(params, gradients)
        losses.append(loss_total / jnp.maximum(count_total, 1.0))
    return (
        memory,
        jnp.stack(losses),
        params[0],
        params[1],
        params[2],
        params[3],
        params[4],
        params[5],
        params[6],
    )


def solution(mesh):
    owners, reps = mesh.shape["mem"], mesh.shape["rep"]
    in_specs = (
        P("mem", None),
        P(),
        P(None, ("mem", "rep"), None),
        P(None, ("mem", "rep")),
        P(None, ("mem", "rep")),
    ) + (P(),) * 13
    out_specs = (P("mem", None),) + (P(),) * 8

    def choose(*args):
        memory, node_slot, event_nodes = args[:3]
        node_dev, width = memory.shape
        batches, events, _ = event_nodes.shape
        cap = 2 * events // owners * 2
        pack = Pack(width, args[11].shape[1], owners * reps)
        small = node_slot.shape[0] * 2 * LANES * 4 <= 16 * 1024 * 1024
        shaped = (
            reps == 4
            and owners % 2 == 0
            and owners > 4
            and batches == 2
            and 2 * cap == LANES
            and events == LANES
            and node_dev % (4 * LANES) == 0
            and LANES < width <= LANES + LANES // 2
            and args[5].shape[0] < LANES
            and pack.fits()
        )
        if small and shaped:
            return quick_body(owners, reps, cap, *args)
        return body(*args)

    return jax.shard_map(choose, mesh=mesh, in_specs=in_specs, out_specs=out_specs, check_vma=False)
```
